8 devices in a mesh: dp: 1 (over z), tp: 2 (over y), ep: 4 (over x, core).
Axes of the slice: x: 2, y: 2, z: 1, core: 2. Of those that a mesh axis runs over, the one named last changes fastest.
Arguments:
- hidden_in: bfloat16 [4, 1024, 2048], P(('dp', 'ep'))
- expert_ids: int32 [4, 1024, 8], P(('dp', 'ep'))
- slot_ids: int32 [4, 1024, 8], P(('dp', 'ep'))
- attn_gain: bfloat16 [2048], replicated
- w_query: bfloat16 [2048, 16, 128], P(None, 'tp')
- w_key: bfloat16 [2048, 16, 128], P(None, 'tp')
- w_value: bfloat16 [2048, 16, 128], P(None, 'tp')
- w_out: bfloat16 [16, 128, 2048], P('tp')
- ffn_gain: bfloat16 [2048], replicated
- w_gate: bfloat16 [2048, 8192], P(None, 'tp')
- w_up: bfloat16 [2048, 8192], P(None, 'tp')
- w_down: bfloat16 [8192, 2048], P('tp')
- moe_gain: bfloat16 [2048], replicated
- w_router: bfloat16 [2048, 64], replicated
- exp_gate: bfloat16 [64, 2048, 1024], P('ep')
- exp_up: bfloat16 [64, 2048, 1024], P('ep')
- exp_down: bfloat16 [64, 1024, 2048], P('ep')
Outputs:
- output: bfloat16 [4, 1024, 2048], P(('dp', 'ep'))
All inputs are finite; a program needn't handle non-finite values.
Results may differ from the reference program's by a relative error of at most 0.00923202.
Values are sent between devices in bfloat16 or wider.
A program may use at most 1.25 GiB of HBM per device.

```python
import math
import jax
import jax.numpy as jnp
from jax import lax

D = 2048
HEADS = 16
HEAD = 128
FF = 8192
EXPERTS = 64
TOP = 8
FE = 1024
SEQ = 1024
SEQS_DEV = 1
GROUP = 4
TOK_DEV = SEQS_DEV * SEQ
TOKENS = GROUP * TOK_DEV
MEAN_LOAD = TOK_DEV * TOP // EXPERTS
CAP = 3 * MEAN_LOAD // 2
EPS = 1e-6
ROPE_BASE = 10000.0


def rms_norm(x_val, gain):
    x_f32 = x_val.astype(jnp.float32)
    inv_rms = lax.rsqrt(jnp.mean(x_f32 * x_f32, axis=-1, keepdims=True) + EPS)
    return (x_f32 * inv_rms * gain.astype(jnp.float32)).astype(jnp.bfloat16)


def rope_tables():
    inv_freq = ROPE_BASE ** (-jnp.arange(HEAD // 2, dtype=jnp.float32) * (2.0 / HEAD))
    angle = jnp.arange(SEQ, dtype=jnp.float32)[:, None] * inv_freq[None, :]
    return jnp.cos(angle), jnp.sin(angle)


def apply_rope(x_val, cos_tab, sin_tab):
    half_dim = x_val.shape[-1] // 2
    lower = x_val[..., :half_dim]
    upper = x_val[..., half_dim:]
    cos_b = cos_tab[:, None, :]
    sin_b = sin_tab[:, None, :]
    return jnp.concatenate([lower * cos_b - upper * sin_b, upper * cos_b + lower * sin_b], axis=-1)


def dense_sequence(h_seq, attn_gain, w_query, w_key, w_value, w_out, ffn_gain, w_gate, w_up, w_down):
    width = HEADS * HEAD
    cos_tab, sin_tab = rope_tables()
    x_norm = rms_norm(h_seq, attn_gain)
    q_f32 = jnp.dot(x_norm, w_query.reshape(D, width), preferred_element_type=jnp.float32).reshape(SEQ, HEADS, HEAD)
    k_f32 = jnp.dot(x_norm, w_key.reshape(D, width), preferred_element_type=jnp.float32).reshape(SEQ, HEADS, HEAD)
    query = apply_rope(q_f32, cos_tab, sin_tab).astype(jnp.bfloat16)
    key_proj = apply_rope(k_f32, cos_tab, sin_tab).astype(jnp.bfloat16)
    value_proj = jnp.dot(x_norm, w_value.reshape(D, width), preferred_element_type=jnp.float32).astype(jnp.bfloat16).reshape(SEQ, HEADS, HEAD)
    scores = jnp.einsum('qhe,khe->hqk', query.astype(jnp.float32), key_proj.astype(jnp.float32)) * HEAD ** -0.5
    causal = jnp.arange(SEQ)[:, None] >= jnp.arange(SEQ)[None, :]
    attn_prob = jax.nn.softmax(jnp.where(causal[None], scores, -1e30), axis=-1).astype(jnp.bfloat16)
    context = jnp.einsum('hqk,khe->qhe', attn_prob.astype(jnp.float32), value_proj.astype(jnp.float32)).astype(jnp.bfloat16)
    attn_out = jnp.dot(context.reshape(SEQ, width), w_out.reshape(width, D), preferred_element_type=jnp.float32)
    after_attn = (h_seq.astype(jnp.float32) + attn_out).astype(jnp.bfloat16)
    f_norm = rms_norm(after_attn, ffn_gain)
    gate_pre = jnp.dot(f_norm, w_gate, preferred_element_type=jnp.float32)
    up_pre = jnp.dot(f_norm, w_up, preferred_element_type=jnp.float32)
    hidden_act = (jax.nn.silu(gate_pre) * up_pre).astype(jnp.bfloat16)
    ffn_out = jnp.dot(hidden_act, w_down, preferred_element_type=jnp.float32)
    return after_attn.astype(jnp.float32) + ffn_out


def source_routing(key):
    key_shift, key_label, key_token = jax.random.split(key, 3)
    shift = jax.random.randint(key_shift, (EXPERTS // 2,), 0, MEAN_LOAD // 2 + 1)
    shift = shift.at[0].set(MEAN_LOAD // 2)
    paired = jnp.stack([MEAN_LOAD + shift, MEAN_LOAD - shift], axis=1).reshape(EXPERTS)
    counts = paired[jax.random.permutation(key_label, EXPERTS)]
    ends = jnp.cumsum(counts)
    starts = ends - counts
    position = jnp.arange(TOK_DEV * TOP, dtype=jnp.int32)
    owner = jnp.sum((position[:, None] >= ends[None, :]).astype(jnp.int32), axis=1)
    slot_row = position - starts[owner]
    column = jax.random.permutation(key_token, TOK_DEV)
    expert_col = owner.reshape(TOP, TOK_DEV)[:, column].T
    slot_col = slot_row.reshape(TOP, TOK_DEV)[:, column].T
    return expert_col.astype(jnp.int32), slot_col.astype(jnp.int32)


def draw_routing(key):
    expert_all, slot_all = lax.map(source_routing, jax.random.split(key, GROUP))
    out_shape = (GROUP * SEQS_DEV, SEQ, TOP)
    return expert_all.reshape(out_shape), slot_all.reshape(out_shape)


def normal_weight(key, shape, scale):
    return (jax.random.normal(key, shape, jnp.float32) * scale).astype(jnp.bfloat16)


def gain_vector(key):
    return (1.0 + 0.3 * jax.random.normal(key, (D,), jnp.float32)).astype(jnp.bfloat16)


def setup_inputs(seed: int = 0, part: int = 0) -> dict:
    root = jax.random.key(seed)
    part_key = jax.random.fold_in(root, part)
    key_hidden, key_route = jax.random.split(part_key, 2)
    weight_keys = jax.random.split(root, 14)
    width = HEADS * HEAD
    query_scale = math.sqrt(math.log(SEQ) / 2.0) * D ** -0.5
    expert_ids, slot_ids = draw_routing(key_route)
    return {
        'hidden_in': normal_weight(key_hidden, (GROUP * SEQS_DEV, SEQ, D), 1.0),
        'expert_ids': expert_ids,
        'slot_ids': slot_ids,
        'attn_gain': gain_vector(weight_keys[0]),
        'w_query': normal_weight(weight_keys[1], (D, HEADS, HEAD), query_scale),
        'w_key': normal_weight(weight_keys[2], (D, HEADS, HEAD), D ** -0.5),
        'w_value': normal_weight(weight_keys[3], (D, HEADS, HEAD), D ** -0.5),
        'w_out': normal_weight(weight_keys[4], (HEADS, HEAD, D), 2.0 * width ** -0.5),
        'ffn_gain': gain_vector(weight_keys[5]),
        'w_gate': normal_weight(weight_keys[6], (D, FF), D ** -0.5),
        'w_up': normal_weight(weight_keys[7], (D, FF), D ** -0.5),
        'w_down': normal_weight(weight_keys[8], (FF, D), FF ** -0.5),
        'moe_gain': gain_vector(weight_keys[9]),
        'w_router': normal_weight(weight_keys[10], (D, EXPERTS), 2.0 * D ** -0.5),
        'exp_gate': normal_weight(weight_keys[11], (EXPERTS, D, FE), D ** -0.5),
        'exp_up': normal_weight(weight_keys[12], (EXPERTS, D, FE), D ** -0.5),
        'exp_down': normal_weight(weight_keys[13], (EXPERTS, FE, D), 2.0 * FE ** -0.5),
    }


def reference(hidden_in, expert_ids, slot_ids, attn_gain, w_query, w_key, w_value, w_out, ffn_gain, w_gate, w_up, w_down, moe_gain, w_router, exp_gate, exp_up, exp_down):
    tokens = hidden_in.reshape(TOKENS, D)
    route_ids = expert_ids.reshape(TOKENS, TOP)
    slots = slot_ids.reshape(TOKENS, TOP)
    u_norm = rms_norm(tokens, moe_gain)
    logits = jnp.dot(u_norm, w_router, preferred_element_type=jnp.float32)
    gates = jax.nn.softmax(jnp.take_along_axis(logits, route_ids, axis=1), axis=-1)
    token_of = jnp.broadcast_to(jnp.arange(TOKENS, dtype=jnp.int32)[:, None], (TOKENS, TOP))
    flat_pos = (((token_of // TOK_DEV) * EXPERTS + route_ids) * CAP + slots).reshape(-1)
    row_token = jnp.full((GROUP * EXPERTS * CAP,), TOKENS, jnp.int32).at[flat_pos].set(token_of.reshape(-1))
    row_gate = jnp.zeros((GROUP * EXPERTS * CAP,), jnp.float32).at[flat_pos].set(gates.reshape(-1))
    row_token = row_token.reshape(GROUP, EXPERTS, CAP).transpose(1, 0, 2).reshape(EXPERTS, GROUP * CAP)
    row_gate = row_gate.reshape(GROUP, EXPERTS, CAP).transpose(1, 0, 2).reshape(EXPERTS, GROUP * CAP)

    def expert_step(moe_acc, slab):
        rows, gate_rows, w_one, w_three, w_two = slab
        x_rows = jnp.take(u_norm, rows, axis=0, mode='fill', fill_value=0)
        gate_pre = jnp.dot(x_rows, w_one, preferred_element_type=jnp.float32)
        up_pre = jnp.dot(x_rows, w_three, preferred_element_type=jnp.float32)
        hidden_act = (jax.nn.silu(gate_pre) * up_pre).astype(jnp.bfloat16)
        expert_out = jnp.dot(hidden_act, w_two, preferred_element_type=jnp.float32).astype(jnp.bfloat16)
        return moe_acc.at[rows].add(gate_rows[:, None] * expert_out.astype(jnp.float32), mode='drop'), None

    moe_sum = lax.scan(expert_step, jnp.zeros((TOKENS, D), jnp.float32), (row_token, row_gate, exp_gate, exp_up, exp_down))[0]
    dense_out = lax.map(lambda h_seq: dense_sequence(h_seq, attn_gain, w_query, w_key, w_value, w_out, ffn_gain, w_gate, w_up, w_down), hidden_in)
    return (dense_out.reshape(TOKENS, D) + moe_sum).reshape(GROUP * SEQS_DEV, SEQ, D).astype(jnp.bfloat16)
```

```python
import functools
import jax
import jax.numpy as jnp
from jax import lax
from jax.experimental import pallas as pl
from jax.experimental.pallas import tpu as pltpu
from jax.sharding import PartitionSpec as P

EPS = 1e-6
ROPE_BASE = 10000.0
F32 = jnp.float32
BF16 = jnp.bfloat16
SEG = 16
GT = 128
CT = 256
VMEM_BIG = 60 * 1024 * 1024


def inv_rms_of(x_f32):
    return lax.rsqrt(jnp.mean(x_f32 * x_f32, axis=-1, keepdims=True) + EPS)


def rms_norm(x_val, gain):
    x_f32 = x_val.astype(F32)
    return (x_f32 * inv_rms_of(x_f32) * gain.astype(F32)).astype(BF16)


def rope_tables(seq_len, head_dim):
    inv_freq = ROPE_BASE ** (-jnp.arange(head_dim // 2, dtype=F32) * (2.0 / head_dim))
    angle = jnp.arange(seq_len, dtype=F32)[:, None] * inv_freq[None, :]
    cos_tab, sin_tab = jnp.cos(angle), jnp.sin(angle)
    return jnp.concatenate([cos_tab, cos_tab], axis=1), jnp.concatenate([-sin_tab, sin_tab], axis=1)


def attn_kernel(q_ref, k_ref, v_ref, cos_ref, sin_ref, o_ref, k_scr):
    seq, hd = q_ref.shape
    blk = 256
    cos_t, sin_t = cos_ref[...], sin_ref[...]
    k_f = k_ref[...]
    k_scr[...] = (k_f * cos_t + pltpu.roll(k_f, hd // 2, 1) * sin_t).astype(BF16)
    for i in range(seq // blk):
        rows = slice(i * blk, (i + 1) * blk)
        q_f = q_ref[rows, :]
        q_b = (q_f * cos_t[rows] + pltpu.roll(q_f, hd // 2, 1) * sin_t[rows]).astype(BF16)
        kv = (i + 1) * blk
        s = lax.dot_general(q_b, k_scr[:kv, :], (((1,), (1,)), ((), ())), preferred_element_type=F32) * hd ** -0.5
        r_id = lax.broadcasted_iota(jnp.int32, (blk, kv), 0) + i * blk
        c_id = lax.broadcasted_iota(jnp.int32, (blk, kv), 1)
        s = jnp.where(r_id >= c_id, s, -1e30)
        p = jnp.exp(s - jnp.max(s, axis=1, keepdims=True))
        p = (p * (1.0 / jnp.sum(p, axis=1, keepdims=True))).astype(BF16)
        o_ref[rows, :] = jnp.dot(p, v_ref[:kv, :], preferred_element_type=F32).astype(BF16)


def attention(q, k, v, cos_t, sin_t, head_dim):
    seq, width = q.shape
    heads = width // head_dim
    col = pl.BlockSpec((seq, head_dim), lambda h: (0, h))
    tab = pl.BlockSpec((seq, head_dim), lambda h: (0, 0))
    return pl.pallas_call(
        attn_kernel, grid=(heads,),
        in_specs=[col, col, col, tab, tab], out_specs=col,
        out_shape=jax.ShapeDtypeStruct((seq, width), BF16),
        scratch_shapes=[pltpu.VMEM((seq, head_dim), BF16)],
        cost_estimate=pl.CostEstimate(flops=heads * seq * seq * head_dim * 4, bytes_accessed=12 * seq * width, transcendentals=heads * seq * seq),
        name="attn",
    )(q, k, v, cos_t, sin_t)


def expert_kernel(n_ref, loc_ref, dst_ref, rank_ref, u_ref, wg_ref, wu_ref, wd_ref, y_hbm, x_scr, h_scr, y_scr, sem):
    e = pl.program_id(0)
    n_src, half, d = u_ref.shape
    fe = wg_ref.shape[2]

    for s in range(n_src):
        n = n_ref[s, e]
        base = loc_ref[s, e]
        rank_row = rank_ref[s, 0]
        for i in range(2):
            @pl.when(n > i * GT)
            def _():
                rid = lax.broadcasted_iota(jnp.int32, (GT, half), 0) + i * GT
                hot = (rank_row == rid).astype(F32).astype(BF16)
                for c in range(d // 1024):
                    cols = slice(c * 1024, (c + 1) * 1024)
                    x_scr[pl.ds(pl.multiple_of(base + i * GT, SEG), GT), cols] = jnp.dot(hot, u_ref[s, :, cols], preferred_element_type=F32).astype(BF16)

    total = loc_ref[n_src - 1, e] + lax.shift_right_logical(n_ref[n_src - 1, e] + (SEG - 1), 4) * SEG

    def copies(fn, ee):
        for s in range(n_src):
            base, dst = loc_ref[s, ee], dst_ref[s, ee]

            def body(i, carry):
                fn(pltpu.make_async_copy(
                    y_scr.at[pl.ds(pl.multiple_of(base + i * SEG, SEG), SEG), :],
                    y_hbm.at[s, pl.ds(pl.multiple_of(dst + i * SEG, SEG), SEG), :], sem))
                return carry
            lax.fori_loop(0, lax.shift_right_logical(n_ref[s, ee] + (SEG - 1), 4), body, 0)

    @pl.when(e > 0)
    def _():
        copies(lambda c: c.wait(), e - 1)

    def ffn(m0, rows):
        def up(c, carry):
            cols = pl.ds(pl.multiple_of(c * 512, 512), 512)
            x = x_scr[pl.ds(m0, rows), :]
            g = jnp.dot(x, wg_ref[0, :, cols], preferred_element_type=F32)
            v = jnp.dot(x, wu_ref[0, :, cols], preferred_element_type=F32)
            h_scr[pl.ds(0, rows), cols] = (g * jax.nn.sigmoid(g) * v).astype(BF16)
            return carry
        lax.fori_loop(0, fe // 512, up, 0)

        def down(c, carry):
            cols = pl.ds(pl.multiple_of(c * 1024, 1024), 1024)
            y_scr[pl.ds(m0, rows), cols] = jnp.dot(h_scr[pl.ds(0, rows), :], wd_ref[0, :, cols], preferred_element_type=F32).astype(BF16)
            return carry
        lax.fori_loop(0, d // 1024, down, 0)

    for lo, hi in ((0, 256), (256, 320), (320, 384)):
        @pl.when((total > lo) & (total <= hi))
        def _():
            ffn(0, hi)

    @pl.when(total > 384)
    def _():
        def body(i, carry):
            ffn(pl.multiple_of(i * 256, 256), 256)
            return carry
        lax.fori_loop(0, lax.shift_right_logical(total + 255, 8), body, 0)

    copies(lambda c: c.start(), e)

    @pl.when(e == pl.num_programs(0) - 1)
    def _():
        copies(lambda c: c.wait(), e)


def run_experts(n, loc, dst, rank_t, u_all, wg, wu, wd, cap_src):
    n_src, half, d = u_all.shape
    n_exp, _, fe = wg.shape
    grid_spec = pltpu.PrefetchScalarGridSpec(
        num_scalar_prefetch=3, grid=(n_exp,),
        in_specs=[
            pl.BlockSpec((n_src, 1, 1, half), lambda e, *_: (0, e, 0, 0)),
            pl.BlockSpec((n_src, half, d), lambda e, *_: (0, 0, 0), pipeline_mode=pl.Buffered(1)),
            pl.BlockSpec((1, d, fe), lambda e, *_: (e, 0, 0)),
            pl.BlockSpec((1, d, fe), lambda e, *_: (e, 0, 0)),
            pl.BlockSpec((1, fe, d), lambda e, *_: (e, 0, 0)),
        ],
        out_specs=pl.BlockSpec(memory_space=pl.ANY),
        scratch_shapes=[pltpu.VMEM((1024, d), BF16), pltpu.VMEM((384, fe), BF16), pltpu.VMEM((768, d), BF16), pltpu.SemaphoreType.DMA],
    )
    return pl.pallas_call(
        expert_kernel, grid_spec=grid_spec,
        out_shape=jax.ShapeDtypeStruct((n_src, cap_src, d), BF16),
        compiler_params=pltpu.CompilerParams(vmem_limit_bytes=VMEM_BIG),
        cost_estimate=pl.CostEstimate(flops=80_000_000_000, bytes_accessed=n_exp * d * fe * 6 + 40_000_000, transcendentals=0),
        name="experts",
    )(n, loc, dst, rank_t, u_all, wg, wu, wd)


def combine_kernel(srcs, rows_ref, pos_ref, gate_ref, y_hbm, o_ref, y_buf, sems):
    p = pl.program_id(0)
    src = jnp.where(p == 0, srcs[0], srcs[1])
    half, top_k = pos_ref.shape[1:]
    d = o_ref.shape[2]
    n_rows = rows_ref[src]
    n_tiles = lax.shift_right_logical(n_rows + (CT - 1), 8)

    def fetch(i, slot):
        return pltpu.make_async_copy(y_hbm.at[src, pl.ds(pl.multiple_of(i * CT, CT), CT), :], y_buf.at[slot], sems.at[slot])

    @pl.when(n_tiles > 0)
    def _():
        fetch(0, 0).start()

    o_ref[...] = jnp.zeros_like(o_ref)

    def body(i, carry):
        slot = lax.rem(i, 2)

        @pl.when(i + 1 < n_tiles)
        def _():
            fetch(i + 1, 1 - slot).start()

        rid = lax.broadcasted_iota(jnp.int32, (half, CT), 1) + i * CT
        g = jnp.zeros((half, CT), F32)
        for j in range(top_k):
            g = jnp.where(pos_ref[0, :, j:j + 1] == rid, gate_ref[0, :, j:j + 1], g)
        hi = g.astype(BF16)
        rest = g - hi.astype(F32)
        mid = rest.astype(BF16)
        low = (rest - mid.astype(F32)).astype(BF16)
        live = lax.broadcasted_iota(jnp.int32, (CT, 1), 0) + i * CT < n_rows
        fetch(i, slot).wait()
        for c in range(d // 512):
            cols = slice(c * 512, (c + 1) * 512)
            y = jnp.where(live, y_buf[slot, :, cols].astype(F32), 0.0).astype(BF16)
            acc = jnp.dot(low, y, preferred_element_type=F32)
            acc += jnp.dot(mid, y, preferred_element_type=F32)
            acc += jnp.dot(hi, y, preferred_element_type=F32)
            o_ref[0, :, cols] += acc
        return carry

    lax.fori_loop(0, n_tiles, body, 0)


def run_combine(srcs, rows, pos, gates, y_all):
    cap_src, d = y_all.shape[1:]
    half, top_k = pos.shape[1:]
    near = lambda p, r: (jnp.where(p == 0, srcs[0], srcs[1]), 0, 0)
    grid_spec = pltpu.PrefetchScalarGridSpec(
        num_scalar_prefetch=1, grid=(2,),
        in_specs=[
            pl.BlockSpec((1, half, top_k), near),
            pl.BlockSpec((1, half, top_k), near),
            pl.BlockSpec(memory_space=pl.ANY),
        ],
        out_specs=pl.BlockSpec((1, half, d), lambda p, r: (p, 0, 0)),
        scratch_shapes=[pltpu.VMEM((2, CT, d), BF16), pltpu.SemaphoreType.DMA((2,))],
    )
    return pl.pallas_call(
        functools.partial(combine_kernel, srcs), grid_spec=grid_spec,
        out_shape=jax.ShapeDtypeStruct((2, half, d), F32),
        compiler_params=pltpu.CompilerParams(vmem_limit_bytes=40 * 1024 * 1024),
        cost_estimate=pl.CostEstimate(flops=16_000_000_000, bytes_accessed=20_000_000, transcendentals=0),
        name="combine",
    )(rows, pos, gates, y_all)


def solution(mesh):
    tok_spec = P(('dp', 'ep'), None, None)
    col_spec = P(None, 'tp', None)
    exp_spec = P('ep', None, None)
    in_specs = (tok_spec, tok_spec, tok_spec, P(None), col_spec, col_spec, col_spec, P('tp', None, None), P(None), P(None, 'tp'), P(None, 'tp'), P('tp', None), P(None), P(None, None), exp_spec, exp_spec, exp_spec)
    n_ep, n_tp = mesh.shape['ep'], mesh.shape['tp']
    assert n_ep == 4 and n_tp == 2

    def over_x(v):
        return lax.ppermute(v, 'ep', [(i, i ^ 2) for i in range(4)])

    def over_core(v):
        return lax.ppermute(v, 'ep', [(i, i ^ 1) for i in range(4)])

    def over_tp(v):
        return lax.ppermute(v, 'tp', [(0, 1), (1, 0)])

    def layer_local(hidden_in, expert_ids, slot_ids, attn_gain, w_query, w_key, w_value, w_out, ffn_gain, w_gate, w_up, w_down, moe_gain, w_router, exp_gate, exp_up, exp_down):
        seq, d = hidden_in.shape[1:]
        top_k = expert_ids.shape[2]
        n_all = w_router.shape[1]
        n_exp = exp_gate.shape[0]
        half = seq // 2
        my_tp = lax.axis_index('tp')
        my_ep = lax.axis_index('ep')
        x2 = hidden_in.reshape(seq, d)
        ids = expert_ids.reshape(seq, top_k)

        x_half = lax.dynamic_slice(x2, (my_tp * half, 0), (half, d))
        ids_half = lax.dynamic_slice(ids, (my_tp * half, 0), (half, top_k))
        u_half = rms_norm(x_half, moe_gain)
        u_x = over_x(u_half)
        u_c = over_core(u_half)
        logits = jnp.dot(u_half, w_router, preferred_element_type=F32)
        is_e = ids_half[:, :, None] == jnp.arange(n_all, dtype=jnp.int32)[None, None, :]
        picked = jnp.sum(jnp.where(is_e, logits[:, None, :], 0.0), axis=2)
        gates = jax.nn.softmax(picked, axis=-1)
        meta = jnp.concatenate([ids_half.astype(F32), gates], axis=1)
        meta_x = over_x(meta)
        meta2 = jnp.stack([meta, meta_x])
        meta_all = jnp.concatenate([meta2, over_core(meta2)])
        u_d = over_core(u_x)
        u_all = jnp.stack([u_half, u_x, u_c, u_d])

        width = w_out.shape[0] * w_out.shape[1]
        w_o = w_out.reshape(width, d)
        quarter = width // 4
        w_q0 = over_tp(lax.dynamic_slice(w_o, (my_ep * quarter, 0), (quarter, d)))
        w_q1 = over_x(w_q0)
        w_q2 = over_core(w_q0)
        w_q3 = over_core(w_q1)
        w_peer = jnp.zeros((width, d), BF16)
        for r, piece in ((0, w_q0), (2, w_q1), (1, w_q2), (3, w_q3)):
            w_peer = lax.dynamic_update_slice(w_peer, piece, ((my_ep ^ r) * quarter, 0))

        ids_loc = meta_all[:, :, :top_k].astype(jnp.int32) - my_ep * n_exp
        gates_all = meta_all[:, :, top_k:]
        ids_t = jnp.swapaxes(ids_loc, 1, 2)
        e_ids = jnp.arange(n_exp, dtype=jnp.int32)
        sel_t = jnp.any(ids_t[:, None, :, :] == e_ids[None, :, None, None], axis=2)
        before = (jnp.arange(half)[:, None] < jnp.arange(half)[None, :]).astype(BF16)
        rank_f = jnp.dot(sel_t.reshape(-1, half).astype(BF16), before, preferred_element_type=F32).reshape(4, n_exp, half)
        n = jnp.sum(sel_t.astype(jnp.int32), axis=2)
        seg = (n + SEG - 1) // SEG * SEG
        lower4 = jnp.arange(4)[:, None] > jnp.arange(4)[None, :]
        loc = jnp.sum(jnp.where(lower4[:, :, None], seg[None], 0), axis=1)
        lower_e = jnp.arange(n_exp)[:, None] > jnp.arange(n_exp)[None, :]
        dst = jnp.sum(jnp.where(lower_e[None], seg[:, None, :], 0), axis=2)
        rows = jnp.sum(seg, axis=1)
        rank_i = rank_f.astype(jnp.int32)
        rank_t = jnp.where(sel_t, rank_i, -1)[:, :, None, :]
        pos_e = jnp.swapaxes(rank_i + dst[:, :, None], 1, 2)
        hit = ids_loc[..., None] == e_ids
        pos = jnp.sum(jnp.where(hit, pos_e[:, :, None, :] + 1, 0), axis=3) - 1

        x_norm = rms_norm(x2, attn_gain)
        hd = w_query.shape[2]
        q = jnp.dot(x_norm, w_query.reshape(d, width), preferred_element_type=F32)
        k = jnp.dot(x_norm, w_key.reshape(d, width), preferred_element_type=F32)
        v = jnp.dot(x_norm, w_value.reshape(d, width), preferred_element_type=F32).astype(BF16)
        cos_t, sin_t = rope_tables(seq, hd)
        ctx = attention(q, k, v, cos_t, sin_t, hd)
        ctx_peer = over_tp(ctx)

        cap_src = n_exp * (3 * seq * top_k // (2 * n_all))
        y_all = run_experts(n, loc, dst, rank_t, u_all, exp_gate, exp_up, exp_down, cap_src)
        m_far = run_combine((2, 3), rows, pos, gates_all, y_all)
        m_got = over_core(m_far)
        m_near = run_combine((0, 1), rows, pos, gates_all, y_all)
        m_x = over_x(m_near[1] + m_got[1])
        m_own = m_near[0] + m_got[0]

        o = jnp.dot(ctx, w_o, preferred_element_type=F32) + jnp.dot(ctx_peer, w_peer, preferred_element_type=F32)
        after = (x2.astype(F32) + o).astype(BF16)
        f_norm = rms_norm(after, ffn_gain)

        def ffn(rows_in):
            g = jnp.dot(rows_in, w_gate, preferred_element_type=F32)
            up = jnp.dot(rows_in, w_up, preferred_element_type=F32)
            h = (jax.nn.silu(g) * up).astype(BF16)
            return jnp.dot(h, w_down, preferred_element_type=F32)

        f_far = ffn(lax.dynamic_slice(f_norm, ((1 - my_tp) * half, 0), (half, d)))
        f_got = over_tp(f_far)
        f_own = ffn(lax.dynamic_slice(f_norm, (my_tp * half, 0), (half, d)))
        a_half = lax.dynamic_slice(after, (my_tp * half, 0), (half, d)).astype(F32)
        out_half = (a_half + (f_own + f_got) + (m_own + m_x)).astype(BF16)
        out_peer = over_tp(out_half)
        first = my_tp == 0
        out = jnp.concatenate([jnp.where(first, out_half, out_peer), jnp.where(first, out_peer, out_half)], axis=0)
        return out.reshape(1, seq, d)

    return jax.shard_map(layer_local, mesh=mesh, in_specs=in_specs, out_specs=tok_spec, check_vma=False)
```

```python
import functools
import jax
import jax.numpy as jnp
from jax import lax
from jax.experimental import pallas as pl
from jax.experimental.pallas import tpu as pltpu
from jax.sharding import PartitionSpec as P

EPS = 1e-6
ROPE_BASE = 10000.0
F32 = jnp.float32
BF16 = jnp.bfloat16
SEG = 16
GT = 128
OUT = 96
CHUNKS = 4
CT = 256
VMEM_BIG = 60 * 1024 * 1024


def inv_rms_of(x_f32):
    return lax.rsqrt(jnp.mean(x_f32 * x_f32, axis=-1, keepdims=True) + EPS)


def rms_norm(x_val, gain):
    x_f32 = x_val.astype(F32)
    return (x_f32 * inv_rms_of(x_f32) * gain.astype(F32)).astype(BF16)


def rope_tables(seq_len, head_dim):
    inv_freq = ROPE_BASE ** (-jnp.arange(head_dim // 2, dtype=F32) * (2.0 / head_dim))
    angle = jnp.arange(seq_len, dtype=F32)[:, None] * inv_freq[None, :]
    cos_tab, sin_tab = jnp.cos(angle), jnp.sin(angle)
    return jnp.concatenate([cos_tab, cos_tab], axis=1), jnp.concatenate([-sin_tab, sin_tab], axis=1)


def attn_kernel(q_ref, k_ref, v_ref, cos_ref, sin_ref, o_ref, k_scr):
    seq, hd = q_ref.shape
    blk = 256
    cos_t, sin_t = cos_ref[...], sin_ref[...]
    k_f = k_ref[...]
    k_scr[...] = (k_f * cos_t + pltpu.roll(k_f, hd // 2, 1) * sin_t).astype(BF16)
    for i in range(seq // blk):
        rows = slice(i * blk, (i + 1) * blk)
        q_f = q_ref[rows, :]
        q_b = (q_f * cos_t[rows] + pltpu.roll(q_f, hd // 2, 1) * sin_t[rows]).astype(BF16)
        kv = (i + 1) * blk
        s = lax.dot_general(q_b, k_scr[:kv, :], (((1,), (1,)), ((), ())), preferred_element_type=F32) * hd ** -0.5
        r_id = lax.broadcasted_iota(jnp.int32, (blk, kv), 0) + i * blk
        c_id = lax.broadcasted_iota(jnp.int32, (blk, kv), 1)
        s = jnp.where(r_id >= c_id, s, -1e30)
        p = jnp.exp(s - jnp.max(s, axis=1, keepdims=True))
        p = (p * (1.0 / jnp.sum(p, axis=1, keepdims=True))).astype(BF16)
        o_ref[rows, :] = jnp.dot(p, v_ref[:kv, :], preferred_element_type=F32).astype(BF16)


def attention(q, k, v, cos_t, sin_t, head_dim):
    seq, width = q.shape
    heads = width // head_dim
    col = pl.BlockSpec((seq, head_dim), lambda h: (0, h))
    tab = pl.BlockSpec((seq, head_dim), lambda h: (0, 0))
    return pl.pallas_call(
        attn_kernel, grid=(heads,),
        in_specs=[col, col, col, tab, tab], out_specs=col,
        out_shape=jax.ShapeDtypeStruct((seq, width), BF16),
        scratch_shapes=[pltpu.VMEM((seq, head_dim), BF16)],
        cost_estimate=pl.CostEstimate(flops=heads * seq * seq * head_dim * 4, bytes_accessed=12 * seq * width, transcendentals=heads * seq * seq),
        name="attn",
    )(q, k, v, cos_t, sin_t)


def expert_kernel(n_ref, loc_ref, dst_ref, rank_ref, u0_ref, u1_ref, u2_ref, u3_ref, wg_ref, wu_ref, wd_ref, _after, y_hbm, x_scr, h_scr, y_scr, sem):
    e = pl.program_id(0)
    u_refs = (u0_ref, u1_ref, u2_ref, u3_ref)
    half, d = u0_ref.shape
    fe = wg_ref.shape[2]

    for s in range(4):
        n = n_ref[s, e]
        base = loc_ref[s, e]
        rank_row = rank_ref[s, 0]
        for i in range(2):
            @pl.when(n > i * GT)
            def _():
                rid = lax.broadcasted_iota(jnp.int32, (GT, half), 0) + i * GT
                hot = (rank_row == rid).astype(F32).astype(BF16)
                x_scr[pl.ds(pl.multiple_of(base + i * GT, SEG), GT), :] = jnp.dot(hot, u_refs[s][...], preferred_element_type=F32).astype(BF16)

    total = loc_ref[3, e] + lax.shift_right_logical(n_ref[3, e] + (SEG - 1), 4) * SEG

    def copies(fn, ee):
        for s in range(4):
            for i in range(2):
                @pl.when(n_ref[s, ee] > i * OUT)
                def _():
                    fn(pltpu.make_async_copy(
                        y_scr.at[pl.ds(pl.multiple_of(loc_ref[s, ee] + i * OUT, SEG), OUT), :],
                        y_hbm.at[s, pl.ds(pl.multiple_of(dst_ref[s, ee] + i * OUT, SEG), OUT), :], sem))

    @pl.when(e > 0)
    def _():
        copies(lambda c: c.wait(), e - 1)

    def ffn(m0, rows):
        for c in range(fe // 512):
            cols = slice(c * 512, (c + 1) * 512)
            x = x_scr[pl.ds(m0, rows), :]
            g = jnp.dot(x, wg_ref[0, :, cols], preferred_element_type=F32)
            v = jnp.dot(x, wu_ref[0, :, cols], preferred_element_type=F32)
            h_scr[pl.ds(0, rows), cols] = (g * jax.nn.sigmoid(g) * v).astype(BF16)
        for c in range(d // 1024):
            cols = slice(c * 1024, (c + 1) * 1024)
            y_scr[pl.ds(m0, rows), cols] = jnp.dot(h_scr[pl.ds(0, rows), :], wd_ref[0, :, cols], preferred_element_type=F32).astype(BF16)

    for lo, hi in ((256, 320), (320, 384)):
        @pl.when((total > lo) & (total <= hi))
        def _():
            ffn(0, hi)

    @pl.when((total <= 256) | (total > 384))
    def _():
        def body(i, carry):
            ffn(pl.multiple_of(i * 256, 256), 256)
            return carry

        lax.fori_loop(0, lax.shift_right_logical(total + 255, 8), body, 0)

    copies(lambda c: c.start(), e)

    @pl.when(e == pl.num_programs(0) - 1)
    def _():
        copies(lambda c: c.wait(), e)


def run_experts(n, loc, dst, rank_t, u_four, wg, wu, wd, cap_src, after):
    half, d = u_four[0].shape
    n_exp, _, fe = wg.shape
    whole = pl.BlockSpec((half, d), lambda e, *_: (0, 0), pipeline_mode=pl.Buffered(1))
    grid_spec = pltpu.PrefetchScalarGridSpec(
        num_scalar_prefetch=3, grid=(n_exp,),
        in_specs=[
            pl.BlockSpec((4, 1, 1, half), lambda e, *_: (0, e, 0, 0)),
            whole, whole, whole, whole,
            pl.BlockSpec((1, d, fe), lambda e, *_: (e, 0, 0)),
            pl.BlockSpec((1, d, fe), lambda e, *_: (e, 0, 0)),
            pl.BlockSpec((1, fe, d), lambda e, *_: (e, 0, 0)),
            pl.BlockSpec(memory_space=pl.ANY),
        ],
        out_specs=pl.BlockSpec(memory_space=pl.ANY),
        scratch_shapes=[pltpu.VMEM((1024, d), BF16), pltpu.VMEM((384, fe), BF16), pltpu.VMEM((1024, d), BF16), pltpu.SemaphoreType.DMA],
    )
    return pl.pallas_call(
        expert_kernel, grid_spec=grid_spec,
        out_shape=jax.ShapeDtypeStruct((4, cap_src + 256, d), BF16),
        compiler_params=pltpu.CompilerParams(vmem_limit_bytes=VMEM_BIG),
        cost_estimate=pl.CostEstimate(flops=90_000_000_000, bytes_accessed=n_exp * d * fe * 6 + 40_000_000, transcendentals=0),
        name="experts",
    )(n, loc, dst, rank_t, *u_four, wg, wu, wd, after)


def combine_kernel(src, has_init, rows_ref, pos_ref, gate_ref, y_hbm, _after, *rest):
    init_ref = rest[0] if has_init else None
    *o_refs, y_buf, g_scr, sems = rest[1:] if has_init else rest
    half, top_k = pos_ref.shape
    rc, d = o_refs[0].shape
    n_rows = rows_ref[src]
    n_tiles = lax.shift_right_logical(n_rows + (CT - 1), 8)

    def fetch(i, slot):
        return pltpu.make_async_copy(y_hbm.at[src, pl.ds(pl.multiple_of(i * CT, CT), CT), :], y_buf.at[slot], sems.at[slot])

    @pl.when(n_tiles > 0)
    def _():
        fetch(0, 0).start()

    for k, o_ref in enumerate(o_refs):
        o_ref[...] = init_ref[k * rc:(k + 1) * rc, :] if has_init else jnp.zeros_like(o_ref)

    def body(i, carry):
        slot = lax.rem(i, 2)

        @pl.when(i + 1 < n_tiles)
        def _():
            fetch(i + 1, 1 - slot).start()

        rid = lax.broadcasted_iota(jnp.int32, (half, CT), 1) + i * CT
        g = jnp.zeros((half, CT), F32)
        for j in range(top_k):
            g = jnp.where(pos_ref[:, j:j + 1] == rid, gate_ref[:, j:j + 1], g)
        hi = g.astype(BF16)
        left = g - hi.astype(F32)
        mid = left.astype(BF16)
        g_scr[:, :CT] = (left - mid.astype(F32)).astype(BF16)
        g_scr[:, CT:2 * CT] = mid
        g_scr[:, 2 * CT:] = hi
        fetch(i, slot).wait()

        @pl.when(i == n_tiles - 1)
        def _():
            live = lax.broadcasted_iota(jnp.int32, (CT, 1), 0) + i * CT < n_rows
            y_buf[slot] = jnp.where(live, y_buf[slot].astype(F32), 0.0).astype(BF16)

        for c in range(d // 512):
            cols = slice(c * 512, (c + 1) * 512)
            y = y_buf[slot, :, cols]
            part = jnp.dot(g_scr[...], jnp.concatenate([y, y, y], axis=0), preferred_element_type=F32)
            for k, o_ref in enumerate(o_refs):
                o_ref[:, cols] += part[k * rc:(k + 1) * rc]
        return carry

    lax.fori_loop(0, n_tiles, body, 0)


def run_combine(src, rows, pos, gates, y_all, after, init=None, n_out=1):
    d = y_all.shape[2]
    half, top_k = pos.shape[1:]
    full = pl.BlockSpec((half, d), lambda i, r: (0, 0))
    small = pl.BlockSpec((half, top_k), lambda i, r: (0, 0))
    anywhere = pl.BlockSpec(memory_space=pl.ANY)
    extra = [] if init is None else [init]
    grid_spec = pltpu.PrefetchScalarGridSpec(
        num_scalar_prefetch=1, grid=(1,),
        in_specs=[small, small, anywhere, anywhere] + [full for _ in extra],
        out_specs=[pl.BlockSpec((half // n_out, d), lambda i, r: (0, 0))] * n_out,
        scratch_shapes=[pltpu.VMEM((2, CT, d), BF16), pltpu.VMEM((half, 3 * CT), BF16), pltpu.SemaphoreType.DMA((2,))],
    )
    return pl.pallas_call(
        functools.partial(combine_kernel, src, init is not None), grid_spec=grid_spec,
        out_shape=[jax.ShapeDtypeStruct((half // n_out, d), F32)] * n_out,
        compiler_params=pltpu.CompilerParams(vmem_limit_bytes=40 * 1024 * 1024),
        cost_estimate=pl.CostEstimate(flops=12_000_000_000, bytes_accessed=10_000_000, transcendentals=0),
    )(rows, pos[src], gates[src], y_all, after, *extra)


def out_kernel(q_ref, x_ref, gain_ref, ctx_ref, peer_ref, wo_ref, w0_ref, w1_ref, w2_ref, w3_ref, _after, a_ref, n_ref):
    quarter = w0_ref.shape[0]
    o = jnp.dot(ctx_ref[...], wo_ref[...], preferred_element_type=F32)
    p = None
    for r, w in enumerate((w0_ref, w1_ref, w2_ref, w3_ref)):
        cols = pl.ds(pl.multiple_of(q_ref[r] * quarter, quarter), quarter)
        t = jnp.dot(peer_ref[:, cols], w[...], preferred_element_type=F32)
        p = t if p is None else p + t
    after = (x_ref[...].astype(F32) + (o + p)).astype(BF16)
    a_ref[...] = after
    a_f = after.astype(F32)
    inv = lax.rsqrt(jnp.mean(a_f * a_f, axis=1, keepdims=True) + EPS)
    n_ref[...] = (a_f * inv * gain_ref[...].astype(F32)).astype(BF16)


def run_out(quarters, x2, gain, ctx, ctx_peer, w_o, pieces, after):
    seq, d = x2.shape
    width = w_o.shape[0]
    blk = 256
    row = lambda n: pl.BlockSpec((blk, n), lambda i, q: (i, 0))
    const = lambda m, n: pl.BlockSpec((m, n), lambda i, q: (0, 0), pipeline_mode=pl.Buffered(1))
    grid_spec = pltpu.PrefetchScalarGridSpec(
        num_scalar_prefetch=1, grid=(seq // blk,),
        in_specs=[row(d), const(1, d), row(width), row(width), const(width, d)] + [const(width // 4, d)] * 4 + [pl.BlockSpec(memory_space=pl.ANY)],
        out_specs=[row(d), row(d)],
    )
    return pl.pallas_call(
        out_kernel, grid_spec=grid_spec,
        out_shape=[jax.ShapeDtypeStruct((seq, d), BF16)] * 2,
        compiler_params=pltpu.CompilerParams(vmem_limit_bytes=VMEM_BIG),
        cost_estimate=pl.CostEstimate(flops=10_000_000_000, bytes_accessed=24_000_000, transcendentals=0),
        name="out_proj",
    )(quarters, x2, gain.reshape(1, d), ctx, ctx_peer, w_o, *pieces, after)


def ffn_kernel(n_out, has_add, off_ref, x_ref, wg_ref, wu_ref, wd_ref, _after, *rest):
    add_ref = rest[0] if has_add else None
    outs = rest[1:] if has_add else rest
    o_refs, acc = outs[:n_out], outs[n_out]
    i = pl.program_id(0)
    x = x_ref[...]
    g = jnp.dot(x, wg_ref[...], preferred_element_type=F32)
    u = jnp.dot(x, wu_ref[...], preferred_element_type=F32)
    h = (g * jax.nn.sigmoid(g) * u).astype(BF16)
    part = jnp.dot(h, wd_ref[...], preferred_element_type=F32)

    @pl.when(i == 0)
    def _():
        acc[...] = part

    @pl.when(i > 0)
    def _():
        acc[...] += part

    @pl.when(i == pl.num_programs(0) - 1)
    def _():
        rows = acc.shape[0] // n_out
        for k, o_ref in enumerate(o_refs):
            v = acc[k * rows:(k + 1) * rows, :]
            if has_add:
                v = add_ref[k * rows:(k + 1) * rows, :].astype(F32) + v
            o_ref[...] = v


def run_ffn(which, f_norm, wg, wu, wd, after, add=None, n_out=4):
    seq, d = f_norm.shape
    half = seq // 2
    ff = wg.shape[1]
    blk = 512
    extra = [] if add is None else [add]
    mine = pl.BlockSpec((half, d), lambda i, w: (w[0], 0), pipeline_mode=pl.Buffered(1))
    grid_spec = pltpu.PrefetchScalarGridSpec(
        num_scalar_prefetch=1, grid=(ff // blk,),
        in_specs=[mine,
                  pl.BlockSpec((d, blk), lambda i, w: (0, i)), pl.BlockSpec((d, blk), lambda i, w: (0, i)),
                  pl.BlockSpec((blk, d), lambda i, w: (i, 0)), pl.BlockSpec(memory_space=pl.ANY)] + [mine for _ in extra],
        out_specs=[pl.BlockSpec((half // n_out, d), lambda i, w: (0, 0))] * n_out,
        scratch_shapes=[pltpu.VMEM((half, d), F32)],
    )
    return pl.pallas_call(
        functools.partial(ffn_kernel, n_out, add is not None), grid_spec=grid_spec,
        out_shape=[jax.ShapeDtypeStruct((half // n_out, d), F32)] * n_out,
        compiler_params=pltpu.CompilerParams(vmem_limit_bytes=VMEM_BIG),
        cost_estimate=pl.CostEstimate(flops=28_000_000_000, bytes_accessed=60_000_000, transcendentals=0),
        name="ffn",
    )(which.reshape(1), f_norm, wg, wu, wd, after, *extra)


def solution(mesh):
    tok_spec = P(('dp', 'ep'), None, None)
    col_spec = P(None, 'tp', None)
    exp_spec = P('ep', None, None)
    in_specs = (tok_spec, tok_spec, tok_spec, P(None), col_spec, col_spec, col_spec, P('tp', None, None), P(None), P(None, 'tp'), P(None, 'tp'), P('tp', None), P(None), P(None, None), exp_spec, exp_spec, exp_spec)
    n_ep, n_tp = mesh.shape['ep'], mesh.shape['tp']
    assert n_ep == 4 and n_tp == 2

    def over_x(v):
        return lax.ppermute(v, 'ep', [(i, i ^ 2) for i in range(4)])

    def over_core(v):
        return lax.ppermute(v, 'ep', [(i, i ^ 1) for i in range(4)])

    def over_tp(v):
        return lax.ppermute(v, 'tp', [(0, 1), (1, 0)])

    def layer(hidden_in, expert_ids, slot_ids, attn_gain, w_query, w_key, w_value, w_out, ffn_gain, w_gate, w_up, w_down, moe_gain, w_router, exp_gate, exp_up, exp_down):
        seq, d = hidden_in.shape[1:]
        top_k = expert_ids.shape[2]
        n_all = w_router.shape[1]
        n_exp = exp_gate.shape[0]
        half = seq // 2
        my_tp = lax.axis_index('tp')
        my_ep = lax.axis_index('ep')
        x2 = hidden_in.reshape(seq, d)
        ids = expert_ids.reshape(seq, top_k)

        width = w_out.shape[0] * w_out.shape[1]
        w_o = w_out.reshape(width, d)
        quarter = width // 4
        w_q0 = over_tp(lax.dynamic_slice(w_o, (my_ep * quarter, 0), (quarter, d)))

        x_half = lax.dynamic_slice(x2, (my_tp * half, 0), (half, d))
        ids_half = lax.dynamic_slice(ids, (my_tp * half, 0), (half, top_k))
        u_half = rms_norm(x_half, moe_gain)
        u_x = over_x(u_half)
        u_c = over_core(u_half)
        logits = jnp.dot(u_half, w_router, preferred_element_type=F32)
        is_e = ids_half[:, :, None] == jnp.arange(n_all, dtype=jnp.int32)[None, None, :]
        picked = jnp.sum(jnp.where(is_e, logits[:, None, :], 0.0), axis=2)
        gates = jax.nn.softmax(picked, axis=-1)
        meta = jnp.concatenate([ids_half.astype(F32), gates], axis=1)
        meta_x = over_x(meta)
        meta2 = jnp.stack([meta, meta_x])
        meta_all = jnp.concatenate([meta2, over_core(meta2)])
        u_d = over_core(u_x)
        w_q1 = over_x(w_q0)
        w_q2 = over_core(w_q0)
        w_q3 = over_core(w_q1)

        ids_loc = meta_all[:, :, :top_k].astype(jnp.int32) - my_ep * n_exp
        gates_all = meta_all[:, :, top_k:]
        ids_t = jnp.swapaxes(ids_loc, 1, 2)
        e_ids = jnp.arange(n_exp, dtype=jnp.int32)
        sel_t = jnp.any(ids_t[:, None, :, :] == e_ids[None, :, None, None], axis=2)
        before = (jnp.arange(half)[:, None] < jnp.arange(half)[None, :]).astype(BF16)
        rank_f = jnp.dot(sel_t.reshape(-1, half).astype(BF16), before, preferred_element_type=F32).reshape(4, n_exp, half)
        n = jnp.sum(sel_t.astype(jnp.int32), axis=2)
        seg = (n + SEG - 1) // SEG * SEG
        lower4 = jnp.arange(4)[:, None] > jnp.arange(4)[None, :]
        loc = jnp.sum(jnp.where(lower4[:, :, None], seg[None], 0), axis=1)
        lower_e = jnp.arange(n_exp)[:, None] > jnp.arange(n_exp)[None, :]
        dst = jnp.sum(jnp.where(lower_e[None], seg[:, None, :], 0), axis=2)
        rows = jnp.sum(seg, axis=1)
        rank_i = rank_f.astype(jnp.int32)
        rank_t = jnp.where(sel_t, rank_i, -1)[:, :, None, :]
        pos_e = jnp.swapaxes(rank_i + dst[:, :, None], 1, 2)
        hit = ids_loc[..., None] == e_ids
        pos = jnp.sum(jnp.where(hit, pos_e[:, :, None, :] + 1, 0), axis=3) - 1

        x_norm = rms_norm(x2, attn_gain)
        hd = w_query.shape[2]
        q = jnp.dot(x_norm, w_query.reshape(d, width), preferred_element_type=F32)
        k = jnp.dot(x_norm, w_key.reshape(d, width), preferred_element_type=F32)
        v = jnp.dot(x_norm, w_value.reshape(d, width), preferred_element_type=F32).astype(BF16)
        cos_t, sin_t = rope_tables(seq, hd)
        ctx = attention(q, k, v, cos_t, sin_t, hd)
        ctx_peer = over_tp(ctx)

        cap_src = n_exp * (3 * seq * top_k // (2 * n_all))
        y_all = run_experts(n, loc, dst, rank_t, (u_half, u_x, u_c, u_d), exp_gate, exp_up, exp_down, cap_src, ctx)
        m3, = run_combine(3, rows, pos, gates_all, y_all, y_all)
        got3 = over_core(m3)

        quarters = my_ep ^ jnp.arange(4, dtype=jnp.int32)
        after, f_norm = run_out(quarters, x2, ffn_gain, ctx, ctx_peer, w_o, (w_q0, w_q2, w_q1, w_q3), m3)
        f_far = run_ffn(1 - my_tp, f_norm, w_gate, w_up, w_down, after)
        f_got = [over_tp(c) for c in f_far]

        m1 = run_combine(1, rows, pos, gates_all, y_all, f_far[0], init=got3, n_out=CHUNKS)
        m_x = [over_x(c) for c in m1]
        m2, = run_combine(2, rows, pos, gates_all, y_all, m1[0])
        got2 = over_core(m2)
        f_own = run_ffn(my_tp, f_norm, w_gate, w_up, w_down, m2, add=after)
        m0 = run_combine(0, rows, pos, gates_all, y_all, f_own[0], init=got2, n_out=CHUNKS)
        own, peer = [], []
        for c in range(CHUNKS):
            o_c = ((f_own[c] + f_got[c]) + (m0[c] + m_x[c])).astype(BF16)
            own.append(o_c)
            peer.append(over_tp(o_c))
        first = my_tp == 0
        out = jnp.concatenate([jnp.where(first, a, b) for a, b in zip(own, peer)] + [jnp.where(first, b, a) for a, b in zip(own, peer)], axis=0)
        return out.reshape(1, seq, d)

    return jax.shard_map(layer, mesh=mesh, in_specs=in_specs, out_specs=tok_spec, check_vma=False)
```

```python
import functools
import jax
import jax.numpy as jnp
import numpy as np
from jax import lax
from jax.experimental import pallas as pl
from jax.experimental.pallas import tpu as pltpu
from jax.sharding import PartitionSpec as P

EPS = 1e-6
ROPE_BASE = 10000.0
F32 = jnp.float32
BF16 = jnp.bfloat16
SEG = 16
GT = 128
OUT = 96
CHUNKS = 4
CT = 256
VMEM_BIG = 60 * 1024 * 1024


def inv_rms_of(x_f32):
    return lax.rsqrt(jnp.mean(x_f32 * x_f32, axis=-1, keepdims=True) + EPS)


def scaled(x_val, inv, gain):
    return (x_val.astype(F32) * inv * gain.astype(F32)).astype(BF16)


def rope_tables(seq_len, head_dim):
    inv_freq = (np.float32(ROPE_BASE) ** (-np.arange(head_dim // 2, dtype=np.float32) * np.float32(2.0 / head_dim))).astype(np.float32)
    angle = (np.arange(seq_len, dtype=np.float32)[:, None] * inv_freq[None, :]).astype(np.float64)
    cos_tab, sin_tab = np.cos(angle).astype(np.float32), np.sin(angle).astype(np.float32)
    return np.concatenate([cos_tab, cos_tab], axis=1), np.concatenate([-sin_tab, sin_tab], axis=1)


def attn_kernel(q_ref, k_ref, v_ref, cos_ref, sin_ref, o_ref, k_scr):
    seq, hd = cos_ref.shape
    blk = 256
    pair = q_ref.shape[1] // hd
    for h in range(pair):
        hc = slice(h * hd, (h + 1) * hd)
        k_f = k_ref[:, hc]
        k_scr[:, hc] = (k_f * cos_ref[...] + pltpu.roll(k_f, hd // 2, 1) * sin_ref[...]).astype(BF16)
    for i in range(seq // blk):
        rows = slice(i * blk, (i + 1) * blk)
        kv = (i + 1) * blk
        for h in range(pair):
            hc = slice(h * hd, (h + 1) * hd)
            q_f = q_ref[rows, hc]
            q_b = (q_f * cos_ref[rows] + pltpu.roll(q_f, hd // 2, 1) * sin_ref[rows]).astype(BF16)
            s = lax.dot_general(q_b, k_scr[:kv, hc], (((1,), (1,)), ((), ())), preferred_element_type=F32) * hd ** -0.5
            r_id = lax.broadcasted_iota(jnp.int32, (blk, blk), 0)
            c_id = lax.broadcasted_iota(jnp.int32, (blk, blk), 1)
            last = jnp.where(r_id >= c_id, s[:, kv - blk:], -1e30)
            s = last if i == 0 else jnp.concatenate([s[:, :kv - blk], last], axis=1)
            p = jnp.exp(s - jnp.max(s, axis=1, keepdims=True))
            p = (p * (1.0 / jnp.sum(p, axis=1, keepdims=True))).astype(BF16)
            o_ref[rows, hc] = jnp.dot(p, v_ref[:kv, hc], preferred_element_type=F32).astype(BF16)


def attention(q, k, v, cos_t, sin_t, head_dim):
    seq, width = q.shape
    pair = 2
    steps = width // (pair * head_dim)
    col = pl.BlockSpec((seq, pair * head_dim), lambda h: (0, h))
    tab = pl.BlockSpec((seq, head_dim), lambda h: (0, 0))
    return pl.pallas_call(
        attn_kernel, grid=(steps,),
        in_specs=[col, col, col, tab, tab], out_specs=col,
        out_shape=jax.ShapeDtypeStruct((seq, width), BF16),
        scratch_shapes=[pltpu.VMEM((seq, pair * head_dim), BF16)],
        cost_estimate=pl.CostEstimate(flops=width * seq * seq * 4, bytes_accessed=12 * seq * width, transcendentals=0),
        name="attn",
    )(q, k, v, cos_t, sin_t)


def expert_kernel(n_ref, loc_ref, dst_ref, rank_ref, u0_ref, u1_ref, u2_ref, u3_ref, wg_ref, wu_ref, wd_ref, _after, y_hbm, x_scr, h_scr, y_scr, sem):
    e = pl.program_id(0)
    u_refs = (u0_ref, u1_ref, u2_ref, u3_ref)
    half, d = u0_ref.shape
    fe = wg_ref.shape[2]

    for s in range(4):
        n = n_ref[s, e]
        base = loc_ref[s, e]
        rank_row = rank_ref[s, 0]

        def gather(i, carry, s=s, base=base, rank_row=rank_row):
            rid = lax.broadcasted_iota(jnp.int32, (GT, half), 0) + i * GT
            hot = (rank_row == rid).astype(F32).astype(BF16)
            x_scr[pl.ds(pl.multiple_of(base + i * GT, SEG), GT), :] = jnp.dot(hot, u_refs[s][...], preferred_element_type=F32).astype(BF16)
            return carry

        lax.fori_loop(0, lax.shift_right_logical(n + (GT - 1), 7), gather, 0)

    total = loc_ref[3, e] + lax.shift_right_logical(n_ref[3, e] + (SEG - 1), 4) * SEG

    def copies(fn, ee):
        for s in range(4):
            for i in range(2):
                @pl.when(n_ref[s, ee] > i * OUT)
                def _():
                    fn(pltpu.make_async_copy(
                        y_scr.at[pl.ds(pl.multiple_of(loc_ref[s, ee] + i * OUT, SEG), OUT), :],
                        y_hbm.at[s, pl.ds(pl.multiple_of(dst_ref[s, ee] + i * OUT, SEG), OUT), :], sem))

    @pl.when(e > 0)
    def _():
        copies(lambda c: c.wait(), e - 1)

    def ffn(m0, rows):
        for c in range(fe // 512):
            cols = slice(c * 512, (c + 1) * 512)
            x = x_scr[pl.ds(m0, rows), :]
            g = jnp.dot(x, wg_ref[0, :, cols], preferred_element_type=F32)
            v = jnp.dot(x, wu_ref[0, :, cols], preferred_element_type=F32)
            h_scr[pl.ds(0, rows), cols] = (g * jax.nn.sigmoid(g) * v).astype(BF16)
        for c in range(d // 1024):
            cols = slice(c * 1024, (c + 1) * 1024)
            y_scr[pl.ds(m0, rows), cols] = jnp.dot(h_scr[pl.ds(0, rows), :], wd_ref[0, :, cols], preferred_element_type=F32).astype(BF16)

    for lo, hi in ((256, 288), (288, 320), (320, 352), (352, 384)):
        @pl.when((total > lo) & (total <= hi))
        def _():
            ffn(0, hi)

    @pl.when((total <= 256) | (total > 384))
    def _():
        def body(i, carry):
            ffn(pl.multiple_of(i * 256, 256), 256)
            return carry

        lax.fori_loop(0, lax.shift_right_logical(total + 255, 8), body, 0)

    copies(lambda c: c.start(), e)

    @pl.when(e == pl.num_programs(0) - 1)
    def _():
        copies(lambda c: c.wait(), e)


def run_experts(n, loc, dst, rank_t, u_four, wg, wu, wd, cap_src, after):
    half, d = u_four[0].shape
    n_exp, _, fe = wg.shape
    whole = pl.BlockSpec((half, d), lambda e, *_: (0, 0), pipeline_mode=pl.Buffered(1))
    grid_spec = pltpu.PrefetchScalarGridSpec(
        num_scalar_prefetch=3, grid=(n_exp,),
        in_specs=[
            pl.BlockSpec((4, 1, 1, half), lambda e, *_: (0, e, 0, 0)),
            whole, whole, whole, whole,
            pl.BlockSpec((1, d, fe), lambda e, *_: (e, 0, 0)),
            pl.BlockSpec((1, d, fe), lambda e, *_: (e, 0, 0)),
            pl.BlockSpec((1, fe, d), lambda e, *_: (e, 0, 0)),
            pl.BlockSpec(memory_space=pl.ANY),
        ],
        out_specs=pl.BlockSpec(memory_space=pl.ANY),
        scratch_shapes=[pltpu.VMEM((1024, d), BF16), pltpu.VMEM((384, fe), BF16), pltpu.VMEM((1024, d), BF16), pltpu.SemaphoreType.DMA],
    )
    return pl.pallas_call(
        expert_kernel, grid_spec=grid_spec,
        out_shape=jax.ShapeDtypeStruct((4, cap_src + 256, d), BF16),
        compiler_params=pltpu.CompilerParams(vmem_limit_bytes=VMEM_BIG),
        cost_estimate=pl.CostEstimate(flops=90_000_000_000, bytes_accessed=n_exp * d * fe * 6 + 40_000_000, transcendentals=0),
        name="experts",
    )(n, loc, dst, rank_t, *u_four, wg, wu, wd, after)


def combine_kernel(src, has_init, rows_ref, pos_ref, gate_ref, y_hbm, _after, *rest):
    init_ref = rest[0] if has_init else None
    *o_refs, y_buf, g_scr, sems = rest[1:] if has_init else rest
    half, top_k = pos_ref.shape
    rc, d = o_refs[0].shape
    n_rows = rows_ref[src]
    n_tiles = lax.shift_right_logical(n_rows + (CT - 1), 8)

    def fetch(i, slot):
        return pltpu.make_async_copy(y_hbm.at[src, pl.ds(pl.multiple_of(i * CT, CT), CT), :], y_buf.at[slot], sems.at[slot])

    @pl.when(n_tiles > 0)
    def _():
        fetch(0, 0).start()

    for k, o_ref in enumerate(o_refs):
        o_ref[...] = init_ref[k * rc:(k + 1) * rc, :] if has_init else jnp.zeros_like(o_ref)

    def body(i, carry):
        slot = lax.rem(i, 2)

        @pl.when(i + 1 < n_tiles)
        def _():
            fetch(i + 1, 1 - slot).start()

        rid = lax.broadcasted_iota(jnp.int32, (32, CT), 1) + i * CT
        for b in range(half // 32):
            tok = slice(b * 32, (b + 1) * 32)
            pos, gate = pos_ref[tok, :], gate_ref[tok, :]
            g = jnp.zeros((32, CT), F32)
            for j in range(top_k):
                g = jnp.where(pos[:, j:j + 1] == rid, gate[:, j:j + 1], g)
            hi = g.astype(BF16)
            left = g - hi.astype(F32)
            mid = left.astype(BF16)
            g_scr[tok, :CT] = (left - mid.astype(F32)).astype(BF16)
            g_scr[tok, CT:2 * CT] = mid
            g_scr[tok, 2 * CT:] = hi
        fetch(i, slot).wait()

        @pl.when(i == n_tiles - 1)
        def _():
            live = lax.broadcasted_iota(jnp.int32, (CT, 1), 0) + i * CT < n_rows
            y_buf[slot] = jnp.where(live, y_buf[slot].astype(F32), 0.0).astype(BF16)

        for c in range(d // 512):
            cols = slice(c * 512, (c + 1) * 512)
            y = y_buf[slot, :, cols]
            part = jnp.dot(g_scr[...], jnp.concatenate([y, y, y], axis=0), preferred_element_type=F32)
            for k, o_ref in enumerate(o_refs):
                o_ref[:, cols] += part[k * rc:(k + 1) * rc]
        return carry

    lax.fori_loop(0, n_tiles, body, 0)


def run_combine(src, rows, pos, gates, y_all, after, init=None, n_out=1, part=(0, 1)):
    d = y_all.shape[2]
    half, top_k = pos.shape[1] // part[1], pos.shape[2]
    full = pl.BlockSpec((half, d), lambda i, r: (part[0], 0))
    small = pl.BlockSpec((half, top_k), lambda i, r: (part[0], 0))
    anywhere = pl.BlockSpec(memory_space=pl.ANY)
    extra = [] if init is None else [init]
    grid_spec = pltpu.PrefetchScalarGridSpec(
        num_scalar_prefetch=1, grid=(1,),
        in_specs=[small, small, anywhere, anywhere] + [full for _ in extra],
        out_specs=[pl.BlockSpec((half // n_out, d), lambda i, r: (0, 0))] * n_out,
        scratch_shapes=[pltpu.VMEM((2, CT, d), BF16), pltpu.VMEM((half, 3 * CT), BF16), pltpu.SemaphoreType.DMA((2,))],
    )
    return pl.pallas_call(
        functools.partial(combine_kernel, src, init is not None), grid_spec=grid_spec,
        out_shape=[jax.ShapeDtypeStruct((half // n_out, d), F32)] * n_out,
        compiler_params=pltpu.CompilerParams(vmem_limit_bytes=40 * 1024 * 1024),
        cost_estimate=pl.CostEstimate(flops=12_000_000_000, bytes_accessed=10_000_000, transcendentals=0),
    )(rows, pos[src], gates[src], y_all, after, *extra)


def out_kernel(q_ref, x_ref, gain_ref, ctx_ref, peer_ref, wo_ref, w0_ref, w1_ref, w2_ref, w3_ref, _after, a_ref, n_ref):
    quarter = w0_ref.shape[0]
    o = jnp.dot(ctx_ref[...], wo_ref[...], preferred_element_type=F32)
    p = None
    for r, w in enumerate((w0_ref, w1_ref, w2_ref, w3_ref)):
        cols = pl.ds(pl.multiple_of(q_ref[r] * quarter, quarter), quarter)
        t = jnp.dot(peer_ref[:, cols], w[...], preferred_element_type=F32)
        p = t if p is None else p + t
    after = (x_ref[...].astype(F32) + (o + p)).astype(BF16)
    a_ref[...] = after
    a_f = after.astype(F32)
    inv = lax.rsqrt(jnp.mean(a_f * a_f, axis=1, keepdims=True) + EPS)
    n_ref[...] = (a_f * inv * gain_ref[...].astype(F32)).astype(BF16)


def run_out(quarters, x2, gain, ctx, ctx_peer, w_o, pieces, after):
    seq, d = x2.shape
    width = w_o.shape[0]
    blk = 256
    row = lambda n: pl.BlockSpec((blk, n), lambda i, q: (i, 0))
    const = lambda m, n: pl.BlockSpec((m, n), lambda i, q: (0, 0), pipeline_mode=pl.Buffered(1))
    grid_spec = pltpu.PrefetchScalarGridSpec(
        num_scalar_prefetch=1, grid=(seq // blk,),
        in_specs=[row(d), const(1, d), row(width), row(width), const(width, d)] + [const(width // 4, d)] * 4 + [pl.BlockSpec(memory_space=pl.ANY)],
        out_specs=[row(d), row(d)],
    )
    return pl.pallas_call(
        out_kernel, grid_spec=grid_spec,
        out_shape=[jax.ShapeDtypeStruct((seq, d), BF16)] * 2,
        compiler_params=pltpu.CompilerParams(vmem_limit_bytes=VMEM_BIG),
        cost_estimate=pl.CostEstimate(flops=10_000_000_000, bytes_accessed=24_000_000, transcendentals=0),
        name="out_proj",
    )(quarters, x2, gain.reshape(1, d), ctx, ctx_peer, w_o, *pieces, after)


def ffn_kernel(n_out, has_add, off_ref, x_ref, wg_ref, wu_ref, wd_ref, _after, *rest):
    add_ref = rest[0] if has_add else None
    outs = rest[1:] if has_add else rest
    o_refs, acc = outs[:n_out], outs[n_out]
    i = pl.program_id(0)
    x = x_ref[...]
    g = jnp.dot(x, wg_ref[...], preferred_element_type=F32)
    u = jnp.dot(x, wu_ref[...], preferred_element_type=F32)
    h = (g * jax.nn.sigmoid(g) * u).astype(BF16)
    part = jnp.dot(h, wd_ref[...], preferred_element_type=F32)

    @pl.when(i == 0)
    def _():
        acc[...] = part

    @pl.when(i > 0)
    def _():
        acc[...] += part

    @pl.when(i == pl.num_programs(0) - 1)
    def _():
        rows = acc.shape[0] // n_out
        for k, o_ref in enumerate(o_refs):
            v = acc[k * rows:(k + 1) * rows, :]
            if has_add:
                v = add_ref[k * rows:(k + 1) * rows, :].astype(F32) + v
            o_ref[...] = v


def run_ffn(which, half, f_norm, wg, wu, wd, after, add=None, n_out=1):
    d = f_norm.shape[1]
    ff = wg.shape[1]
    blk = 512
    extra = [] if add is None else [add]
    mine = pl.BlockSpec((half, d), lambda i, w: (w[0], 0), pipeline_mode=pl.Buffered(1))
    grid_spec = pltpu.PrefetchScalarGridSpec(
        num_scalar_prefetch=1, grid=(ff // blk,),
        in_specs=[mine,
                  pl.BlockSpec((d, blk), lambda i, w: (0, i)), pl.BlockSpec((d, blk), lambda i, w: (0, i)),
                  pl.BlockSpec((blk, d), lambda i, w: (i, 0)), pl.BlockSpec(memory_space=pl.ANY)] + [mine for _ in extra],
        out_specs=[pl.BlockSpec((half // n_out, d), lambda i, w: (0, 0))] * n_out,
        scratch_shapes=[pltpu.VMEM((half, d), F32)],
    )
    return pl.pallas_call(
        functools.partial(ffn_kernel, n_out, add is not None), grid_spec=grid_spec,
        out_shape=[jax.ShapeDtypeStruct((half // n_out, d), F32)] * n_out,
        compiler_params=pltpu.CompilerParams(vmem_limit_bytes=VMEM_BIG),
        cost_estimate=pl.CostEstimate(flops=half * 56_000_000, bytes_accessed=60_000_000, transcendentals=0),
        name="ffn",
    )(which.reshape(1), f_norm, wg, wu, wd, after, *extra)


def solution(mesh):
    tok_spec = P(('dp', 'ep'), None, None)
    col_spec = P(None, 'tp', None)
    exp_spec = P('ep', None, None)
    in_specs = (tok_spec, tok_spec, tok_spec, P(None), col_spec, col_spec, col_spec, P('tp', None, None), P(None), P(None, 'tp'), P(None, 'tp'), P('tp', None), P(None), P(None, None), exp_spec, exp_spec, exp_spec)
    n_ep, n_tp = mesh.shape['ep'], mesh.shape['tp']
    assert n_ep == 4 and n_tp == 2

    def over_x(v):
        return lax.ppermute(v, 'ep', [(i, i ^ 2) for i in range(4)])

    def over_core(v):
        return lax.ppermute(v, 'ep', [(i, i ^ 1) for i in range(4)])

    def over_tp(v):
        return lax.ppermute(v, 'tp', [(0, 1), (1, 0)])

    def layer(hidden_in, expert_ids, slot_ids, attn_gain, w_query, w_key, w_value, w_out, ffn_gain, w_gate, w_up, w_down, moe_gain, w_router, exp_gate, exp_up, exp_down):
        seq, d = hidden_in.shape[1:]
        top_k = expert_ids.shape[2]
        n_all = w_router.shape[1]
        n_exp = exp_gate.shape[0]
        half = seq // 2
        my_tp = lax.axis_index('tp')
        my_ep = lax.axis_index('ep')
        x2 = hidden_in.reshape(seq, d)
        ids = expert_ids.reshape(seq, top_k)

        width = w_out.shape[0] * w_out.shape[1]
        w_o = w_out.reshape(width, d)
        quarter = width // 4
        w_q0 = over_tp(lax.dynamic_slice(w_o, (my_ep * quarter, 0), (quarter, d)))

        inv_rms = inv_rms_of(x2.astype(F32))
        x_half = lax.dynamic_slice(x2, (my_tp * half, 0), (half, d))
        inv_half = lax.dynamic_slice(inv_rms, (my_tp * half, 0), (half, 1))
        ids_half = lax.dynamic_slice(ids, (my_tp * half, 0), (half, top_k))
        u_half = scaled(x_half, inv_half, moe_gain)
        u_c = over_core(u_half)
        logits = jnp.dot(u_half, w_router, preferred_element_type=F32)
        is_e = ids_half[:, :, None] == jnp.arange(n_all, dtype=jnp.int32)[None, None, :]
        picked = jnp.sum(jnp.where(is_e, logits[:, None, :], 0.0), axis=2)
        gates = jax.nn.softmax(picked, axis=-1)
        meta = jnp.concatenate([ids_half.astype(F32), gates], axis=1)
        meta_x = over_x(meta)
        u_x = over_x(u_half)
        meta2 = jnp.stack([meta, meta_x])
        meta_all = jnp.concatenate([meta2, over_core(meta2)])
        u_d = over_core(u_x)
        w_q1 = over_x(w_q0)
        w_q2 = over_core(w_q0)
        w_q3 = over_core(w_q1)

        ids_loc = meta_all[:, :, :top_k].astype(jnp.int32) - my_ep * n_exp
        gates_all = meta_all[:, :, top_k:]
        ids_t = jnp.swapaxes(ids_loc, 1, 2)
        e_ids = jnp.arange(n_exp, dtype=jnp.int32)
        sel_t = jnp.any(ids_t[:, None, :, :] == e_ids[None, :, None, None], axis=2)
        before = (jnp.arange(half)[:, None] < jnp.arange(half)[None, :]).astype(BF16)
        rank_f = jnp.dot(sel_t.reshape(-1, half).astype(BF16), before, preferred_element_type=F32).reshape(4, n_exp, half)
        n = jnp.sum(sel_t.astype(jnp.int32), axis=2)
        seg = (n + SEG - 1) // SEG * SEG
        lower4 = jnp.arange(4)[:, None] > jnp.arange(4)[None, :]
        loc = jnp.sum(jnp.where(lower4[:, :, None], seg[None], 0), axis=1)
        lower_e = jnp.arange(n_exp)[:, None] > jnp.arange(n_exp)[None, :]
        dst = jnp.sum(jnp.where(lower_e[None], seg[:, None, :], 0), axis=2)
        rows = jnp.sum(seg, axis=1)
        rank_i = rank_f.astype(jnp.int32)
        rank_t = jnp.where(sel_t, rank_i, -1)[:, :, None, :]
        pos_e = jnp.swapaxes(rank_i + dst[:, :, None], 1, 2)
        hit = ids_loc[..., None] == e_ids
        pos = jnp.sum(jnp.where(hit, pos_e[:, :, None, :] + 1, 0), axis=3) - 1

        x_norm = scaled(x2, inv_rms, attn_gain)
        hd = w_query.shape[2]
        q = jnp.dot(x_norm, w_query.reshape(d, width), preferred_element_type=F32)
        k = jnp.dot(x_norm, w_key.reshape(d, width), preferred_element_type=F32)
        v = jnp.dot(x_norm, w_value.reshape(d, width), preferred_element_type=F32).astype(BF16)
        cos_t, sin_t = rope_tables(seq, hd)
        ctx = attention(q, k, v, cos_t, sin_t, hd)
        ctx_peer = over_tp(ctx)

        cap_src = n_exp * (3 * seq * top_k // (2 * n_all))
        y_all = run_experts(n, loc, dst, rank_t, (u_half, u_x, u_c, u_d), exp_gate, exp_up, exp_down, cap_src, ctx)

        quarters = my_ep ^ jnp.arange(4, dtype=jnp.int32)
        after, f_norm = run_out(quarters, x2, ffn_gain, ctx, ctx_peer, w_o, (w_q0, w_q2, w_q1, w_q3), y_all)
        f_far = run_ffn(1 - my_tp, half, f_norm, w_gate, w_up, w_down, after, n_out=2)
        f_got = []
        for c in range(2):
            f_got.append(over_tp(f_far[c]))

        m3, = run_combine(3, rows, pos, gates_all, y_all, f_far[0])
        got3 = over_core(m3)
        m2, = run_combine(2, rows, pos, gates_all, y_all, m3)
        got2 = over_core(m2)
        m1 = run_combine(1, rows, pos, gates_all, y_all, m2, init=got3, n_out=CHUNKS)
        m_x = []
        for c in range(CHUNKS):
            m_x.append(over_x(m1[c]))
        rc = half // CHUNKS
        own, peer = [], []
        tie = m1[0]
        for p in range(2):
            f_own, = run_ffn(2 * my_tp + p, half // 2, f_norm, w_gate, w_up, w_down, tie, add=after)
            m0 = run_combine(0, rows, pos, gates_all, y_all, f_own, init=got2, n_out=CHUNKS // 2, part=(p, 2))
            tie = m0[0]
            for k in range(CHUNKS // 2):
                c = p * (CHUNKS // 2) + k
                sl = slice(k * rc, (k + 1) * rc)
                o_c = ((f_own[sl] + f_got[p][sl]) + (m0[k] + m_x[c])).astype(BF16)
                own.append(o_c)
                peer.append(over_tp(o_c))
        first = my_tp == 0
        out = jnp.concatenate([jnp.where(first, a, b) for a, b in zip(own, peer)] + [jnp.where(first, b, a) for a, b in zip(own, peer)], axis=0)
        return out.reshape(1, seq, d)

    return jax.shard_map(layer, mesh=mesh, in_specs=in_specs, out_specs=tok_spec, check_vma=False)
```

```python
import functools
import jax
import jax.numpy as jnp
import numpy as np
from jax import lax
from jax.experimental import pallas as pl
from jax.experimental.pallas import tpu as pltpu
from jax.sharding import PartitionSpec as P

EPS = 1e-6
ROPE_BASE = 10000.0
F32 = jnp.float32
BF16 = jnp.bfloat16
SEG = 16
GT = 128
OUT = 96
CHUNKS = 4
CT = 256
VMEM_BIG = 60 * 1024 * 1024


def inv_rms_of(x_f32):
    return lax.rsqrt(jnp.mean(x_f32 * x_f32, axis=-1, keepdims=True) + EPS)


def scaled(x_val, inv, gain):
    return (x_val.astype(F32) * inv * gain.astype(F32)).astype(BF16)


def rope_tables(seq_len, head_dim):
    inv_freq = (np.float32(ROPE_BASE) ** (-np.arange(head_dim // 2, dtype=np.float32) * np.float32(2.0 / head_dim))).astype(np.float32)
    angle = (np.arange(seq_len, dtype=np.float32)[:, None] * inv_freq[None, :]).astype(np.float64)
    cos_tab, sin_tab = np.cos(angle).astype(np.float32), np.sin(angle).astype(np.float32)
    return np.concatenate([cos_tab, cos_tab], axis=1), np.concatenate([-sin_tab, sin_tab], axis=1)


def attn_kernel(q_ref, k_ref, v_ref, cos_ref, sin_ref, o_ref, k_scr):
    seq, hd = cos_ref.shape
    blk = 256
    pair = q_ref.shape[1] // hd
    for h in range(pair):
        hc = slice(h * hd, (h + 1) * hd)
        k_f = k_ref[:, hc]
        k_scr[:, hc] = (k_f * cos_ref[...] + pltpu.roll(k_f, hd // 2, 1) * sin_ref[...]).astype(BF16)
    for i in range(seq // blk):
        rows = slice(i * blk, (i + 1) * blk)
        kv = (i + 1) * blk
        for h in range(pair):
            hc = slice(h * hd, (h + 1) * hd)
            q_f = q_ref[rows, hc]
            q_b = (q_f * cos_ref[rows] + pltpu.roll(q_f, hd // 2, 1) * sin_ref[rows]).astype(BF16)
            s = lax.dot_general(q_b, k_scr[:kv, hc], (((1,), (1,)), ((), ())), preferred_element_type=F32) * hd ** -0.5
            r_id = lax.broadcasted_iota(jnp.int32, (blk, blk), 0)
            c_id = lax.broadcasted_iota(jnp.int32, (blk, blk), 1)
            last = jnp.where(r_id >= c_id, s[:, kv - blk:], -1e30)
            s = last if i == 0 else jnp.concatenate([s[:, :kv - blk], last], axis=1)
            p = jnp.exp(s - jnp.max(s, axis=1, keepdims=True))
            p = (p * (1.0 / jnp.sum(p, axis=1, keepdims=True))).astype(BF16)
            o_ref[rows, hc] = jnp.dot(p, v_ref[:kv, hc], preferred_element_type=F32).astype(BF16)


def attention(q, k, v, cos_t, sin_t, head_dim):
    seq, width = q.shape
    pair = 2
    steps = width // (pair * head_dim)
    col = pl.BlockSpec((seq, pair * head_dim), lambda h: (0, h))
    tab = pl.BlockSpec((seq, head_dim), lambda h: (0, 0))
    return pl.pallas_call(
        attn_kernel, grid=(steps,),
        in_specs=[col, col, col, tab, tab], out_specs=col,
        out_shape=jax.ShapeDtypeStruct((seq, width), BF16),
        scratch_shapes=[pltpu.VMEM((seq, pair * head_dim), BF16)],
        cost_estimate=pl.CostEstimate(flops=width * seq * seq * 4, bytes_accessed=12 * seq * width, transcendentals=0),
        name="attn",
    )(q, k, v, cos_t, sin_t)


def expert_kernel(n_ref, loc_ref, dst_ref, rank_ref, u0_ref, u1_ref, u2_ref, u3_ref, wg_ref, wu_ref, wd_ref, _after, y_hbm, x_scr, h_scr, y_scr, sem):
    e = pl.program_id(0)
    u_refs = (u0_ref, u1_ref, u2_ref, u3_ref)
    half, d = u0_ref.shape
    fe = wg_ref.shape[2]

    def gather(s, i):
        rid = lax.broadcasted_iota(jnp.int32, (GT, half), 0) + i * GT
        hot = (rank_ref[s, 0] == rid).astype(F32).astype(BF16)
        x_scr[pl.ds(pl.multiple_of(loc_ref[s, e] + i * GT, SEG), GT), :] = jnp.dot(hot, u_refs[s][...], preferred_element_type=F32).astype(BF16)

    for s in range(4):
        @pl.when(n_ref[s, e] > GT)
        def _():
            gather(s, 1)
    for s in range(4):
        gather(s, 0)

    total = loc_ref[3, e] + lax.shift_right_logical(n_ref[3, e] + (SEG - 1), 4) * SEG

    def copies(fn, ee):
        for s in range(4):
            for i in range(2):
                @pl.when(n_ref[s, ee] > i * OUT)
                def _():
                    fn(pltpu.make_async_copy(
                        y_scr.at[pl.ds(pl.multiple_of(loc_ref[s, ee] + i * OUT, SEG), OUT), :],
                        y_hbm.at[s, pl.ds(pl.multiple_of(dst_ref[s, ee] + i * OUT, SEG), OUT), :], sem))

    @pl.when(e > 0)
    def _():
        copies(lambda c: c.wait(), e - 1)

    def ffn(m0, rows):
        for c in range(fe // 512):
            cols = slice(c * 512, (c + 1) * 512)
            x = x_scr[pl.ds(m0, rows), :]
            g = jnp.dot(x, wg_ref[0, :, cols], preferred_element_type=F32)
            v = jnp.dot(x, wu_ref[0, :, cols], preferred_element_type=F32)
            h_scr[pl.ds(0, rows), cols] = (g * jax.nn.sigmoid(g) * v).astype(BF16)
        for c in range(d // 1024):
            cols = slice(c * 1024, (c + 1) * 1024)
            y_scr[pl.ds(m0, rows), cols] = jnp.dot(h_scr[pl.ds(0, rows), :], wd_ref[0, :, cols], preferred_element_type=F32).astype(BF16)

    for lo, hi in ((256, 288), (288, 320), (320, 352), (352, 384)):
        @pl.when((total > lo) & (total <= hi))
        def _():
            ffn(0, hi)

    @pl.when((total <= 256) | (total > 384))
    def _():
        def body(i, carry):
            ffn(pl.multiple_of(i * 256, 256), 256)
            return carry

        lax.fori_loop(0, lax.shift_right_logical(total + 255, 8), body, 0)

    copies(lambda c: c.start(), e)

    @pl.when(e == pl.num_programs(0) - 1)
    def _():
        copies(lambda c: c.wait(), e)


def run_experts(n, loc, dst, rank_t, u_four, wg, wu, wd, cap_src, after):
    half, d = u_four[0].shape
    n_exp, _, fe = wg.shape
    whole = pl.BlockSpec((half, d), lambda e, *_: (0, 0), pipeline_mode=pl.Buffered(1))
    grid_spec = pltpu.PrefetchScalarGridSpec(
        num_scalar_prefetch=3, grid=(n_exp,),
        in_specs=[
            pl.BlockSpec((4, 1, 1, half), lambda e, *_: (0, e, 0, 0)),
            whole, whole, whole, whole,
            pl.BlockSpec((1, d, fe), lambda e, *_: (e, 0, 0)),
            pl.BlockSpec((1, d, fe), lambda e, *_: (e, 0, 0)),
            pl.BlockSpec((1, fe, d), lambda e, *_: (e, 0, 0)),
            pl.BlockSpec(memory_space=pl.ANY),
        ],
        out_specs=pl.BlockSpec(memory_space=pl.ANY),
        scratch_shapes=[pltpu.VMEM((1024, d), BF16), pltpu.VMEM((384, fe), BF16), pltpu.VMEM((1024, d), BF16), pltpu.SemaphoreType.DMA],
    )
    return pl.pallas_call(
        expert_kernel, grid_spec=grid_spec,
        out_shape=jax.ShapeDtypeStruct((4, cap_src + 256, d), BF16),
        compiler_params=pltpu.CompilerParams(vmem_limit_bytes=VMEM_BIG),
        cost_estimate=pl.CostEstimate(flops=90_000_000_000, bytes_accessed=n_exp * d * fe * 6 + 40_000_000, transcendentals=0),
        name="experts",
    )(n, loc, dst, rank_t, *u_four, wg, wu, wd, after)


def combine_kernel(src, has_init, rows_ref, pos_ref, gate_ref, y_hbm, _after, *rest):
    init_ref = rest[0] if has_init else None
    *o_refs, y_a, y_b, g_a, g_b, sems = rest[1:] if has_init else rest
    half, top_k = pos_ref.shape
    rc, d = o_refs[0].shape
    n_rows = rows_ref[src]
    n_tiles = lax.shift_right_logical(n_rows + (CT - 1), 8)

    def fetch(i, buf, k):
        return pltpu.make_async_copy(y_hbm.at[src, pl.ds(pl.multiple_of(i * CT, CT), CT), :], buf, sems.at[k])

    def start(i, buf, k):
        @pl.when(i < n_tiles)
        def _():
            fetch(i, buf, k).start()

    def arrive(i, buf, k):
        @pl.when(i < n_tiles)
        def _():
            fetch(i, buf, k).wait()

        @pl.when(i >= n_tiles - 1)
        def _():
            live = lax.broadcasted_iota(jnp.int32, (CT, 1), 0) + i * CT < n_rows
            buf[...] = jnp.where(live, buf[...].astype(F32), 0.0).astype(BF16)

    def build(i, g_scr, b):
        rid = lax.broadcasted_iota(jnp.int32, (32, CT), 1) + i * CT
        tok = slice(b * 32, (b + 1) * 32)
        pos, gate = pos_ref[tok, :], gate_ref[tok, :]
        g = jnp.zeros((32, CT), F32)
        for j in range(top_k):
            g = jnp.where(pos[:, j:j + 1] == rid, gate[:, j:j + 1], g)
        hi = g.astype(BF16)
        left = g - hi.astype(F32)
        mid = left.astype(BF16)
        g_scr[tok, :CT] = (left - mid.astype(F32)).astype(BF16)
        g_scr[tok, CT:2 * CT] = mid
        g_scr[tok, 2 * CT:] = hi

    def multiply(g_scr, buf, i_next, g_next):
        n_c = d // 512
        blocks = half // 32
        for c in range(n_c):
            cols = slice(c * 512, (c + 1) * 512)
            y = buf[:, cols]
            part = jnp.dot(g_scr[...], jnp.concatenate([y, y, y], axis=0), preferred_element_type=F32)
            for b in range(c * blocks // n_c, (c + 1) * blocks // n_c):
                build(i_next, g_next, b)
            for k, o_ref in enumerate(o_refs):
                o_ref[:, cols] += part[k * rc:(k + 1) * rc]

    start(0, y_a, 0)
    for b in range(half // 32):
        build(0, g_a, b)
    for k, o_ref in enumerate(o_refs):
        o_ref[...] = init_ref[k * rc:(k + 1) * rc, :] if has_init else jnp.zeros_like(o_ref)

    def body(p, carry):
        i = 2 * p
        start(i + 1, y_b, 1)
        arrive(i, y_a, 0)
        multiply(g_a, y_a, i + 1, g_b)

        @pl.when(i + 1 < n_tiles)
        def _():
            start(i + 2, y_a, 0)
            arrive(i + 1, y_b, 1)
            multiply(g_b, y_b, i + 2, g_a)

        return carry

    lax.fori_loop(0, lax.shift_right_logical(n_tiles + 1, 1), body, 0)


def run_combine(src, rows, pos, gates, y_all, after, init=None, n_out=1, part=(0, 1)):
    d = y_all.shape[2]
    half, top_k = pos.shape[1] // part[1], pos.shape[2]
    full = pl.BlockSpec((half, d), lambda i, r: (part[0], 0))
    small = pl.BlockSpec((half, top_k), lambda i, r: (part[0], 0))
    anywhere = pl.BlockSpec(memory_space=pl.ANY)
    extra = [] if init is None else [init]
    grid_spec = pltpu.PrefetchScalarGridSpec(
        num_scalar_prefetch=1, grid=(1,),
        in_specs=[small, small, anywhere, anywhere] + [full for _ in extra],
        out_specs=[pl.BlockSpec((half // n_out, d), lambda i, r: (0, 0))] * n_out,
        scratch_shapes=[pltpu.VMEM((CT, d), BF16)] * 2 + [pltpu.VMEM((half, 3 * CT), BF16)] * 2 + [pltpu.SemaphoreType.DMA((2,))],
    )
    return pl.pallas_call(
        functools.partial(combine_kernel, src, init is not None), grid_spec=grid_spec,
        out_shape=[jax.ShapeDtypeStruct((half // n_out, d), F32)] * n_out,
        compiler_params=pltpu.CompilerParams(vmem_limit_bytes=40 * 1024 * 1024),
        cost_estimate=pl.CostEstimate(flops=12_000_000_000, bytes_accessed=10_000_000, transcendentals=0),
    )(rows, pos[src], gates[src], y_all, after, *extra)


def out_kernel(q_ref, x_ref, gain_ref, ctx_ref, peer_ref, wo_ref, w0_ref, w1_ref, w2_ref, w3_ref, _after, a_ref, n_ref):
    quarter = w0_ref.shape[0]
    o = jnp.dot(ctx_ref[...], wo_ref[...], preferred_element_type=F32)
    p = None
    for r, w in enumerate((w0_ref, w1_ref, w2_ref, w3_ref)):
        cols = pl.ds(pl.multiple_of(q_ref[r] * quarter, quarter), quarter)
        t = jnp.dot(peer_ref[:, cols], w[...], preferred_element_type=F32)
        p = t if p is None else p + t
    after = (x_ref[...].astype(F32) + (o + p)).astype(BF16)
    a_ref[...] = after
    a_f = after.astype(F32)
    inv = lax.rsqrt(jnp.mean(a_f * a_f, axis=1, keepdims=True) + EPS)
    n_ref[...] = (a_f * inv * gain_ref[...].astype(F32)).astype(BF16)


def run_out(quarters, x2, gain, ctx, ctx_peer, w_o, pieces, after):
    seq, d = x2.shape
    width = w_o.shape[0]
    blk = 256
    row = lambda n: pl.BlockSpec((blk, n), lambda i, q: (i, 0))
    const = lambda m, n: pl.BlockSpec((m, n), lambda i, q: (0, 0), pipeline_mode=pl.Buffered(1))
    grid_spec = pltpu.PrefetchScalarGridSpec(
        num_scalar_prefetch=1, grid=(seq // blk,),
        in_specs=[row(d), const(1, d), row(width), row(width), const(width, d)] + [const(width // 4, d)] * 4 + [pl.BlockSpec(memory_space=pl.ANY)],
        out_specs=[row(d), row(d)],
    )
    return pl.pallas_call(
        out_kernel, grid_spec=grid_spec,
        out_shape=[jax.ShapeDtypeStruct((seq, d), BF16)] * 2,
        compiler_params=pltpu.CompilerParams(vmem_limit_bytes=VMEM_BIG),
        cost_estimate=pl.CostEstimate(flops=10_000_000_000, bytes_accessed=24_000_000, transcendentals=0),
        name="out_proj",
    )(quarters, x2, gain.reshape(1, d), ctx, ctx_peer, w_o, *pieces, after)


def ffn_kernel(n_out, has_add, off_ref, x_ref, wg_ref, wu_ref, wd_ref, _after, *rest):
    add_ref = rest[0] if has_add else None
    outs = rest[1:] if has_add else rest
    o_refs, acc = outs[:n_out], outs[n_out]
    i = pl.program_id(0)
    x = x_ref[...]
    g = jnp.dot(x, wg_ref[...], preferred_element_type=F32)
    u = jnp.dot(x, wu_ref[...], preferred_element_type=F32)
    h = (g * jax.nn.sigmoid(g) * u).astype(BF16)
    part = jnp.dot(h, wd_ref[...], preferred_element_type=F32)

    @pl.when(i == 0)
    def _():
        acc[...] = part

    @pl.when(i > 0)
    def _():
        acc[...] += part

    @pl.when(i == pl.num_programs(0) - 1)
    def _():
        rows = acc.shape[0] // n_out
        for k, o_ref in enumerate(o_refs):
            v = acc[k * rows:(k + 1) * rows, :]
            if has_add:
                v = add_ref[k * rows:(k + 1) * rows, :].astype(F32) + v
            o_ref[...] = v


def run_ffn(which, half, f_norm, wg, wu, wd, after, add=None, n_out=1):
    d = f_norm.shape[1]
    ff = wg.shape[1]
    blk = 512
    extra = [] if add is None else [add]
    mine = pl.BlockSpec((half, d), lambda i, w: (w[0], 0), pipeline_mode=pl.Buffered(1))
    grid_spec = pltpu.PrefetchScalarGridSpec(
        num_scalar_prefetch=1, grid=(ff // blk,),
        in_specs=[mine,
                  pl.BlockSpec((d, blk), lambda i, w: (0, i)), pl.BlockSpec((d, blk), lambda i, w: (0, i)),
                  pl.BlockSpec((blk, d), lambda i, w: (i, 0)), pl.BlockSpec(memory_space=pl.ANY)] + [mine for _ in extra],
        out_specs=[pl.BlockSpec((half // n_out, d), lambda i, w: (0, 0))] * n_out,
        scratch_shapes=[pltpu.VMEM((half, d), F32)],
    )
    return pl.pallas_call(
        functools.partial(ffn_kernel, n_out, add is not None), grid_spec=grid_spec,
        out_shape=[jax.ShapeDtypeStruct((half // n_out, d), F32)] * n_out,
        compiler_params=pltpu.CompilerParams(vmem_limit_bytes=VMEM_BIG),
        cost_estimate=pl.CostEstimate(flops=half * 56_000_000, bytes_accessed=60_000_000, transcendentals=0),
        name="ffn",
    )(which.reshape(1), f_norm, wg, wu, wd, after, *extra)


def final_kernel(f_ref, g_ref, m_ref, x_ref, o_ref):
    o_ref[...] = ((f_ref[...] + g_ref[...]) + (m_ref[...] + x_ref[...])).astype(BF16)


def run_final(f_own, f_got, got_block, m_own, m_got):
    rows, d = f_own.shape
    blk = rows // 2
    here = pl.BlockSpec((blk, d), lambda i: (i, 0))
    there = pl.BlockSpec((blk, d), lambda i: (2 * got_block + i, 0))
    return pl.pallas_call(
        final_kernel, grid=(2,), in_specs=[here, there, here, here], out_specs=here,
        out_shape=jax.ShapeDtypeStruct((rows, d), BF16),
        cost_estimate=pl.CostEstimate(flops=3 * rows * d, bytes_accessed=18 * rows * d, transcendentals=0),
        name="final",
    )(f_own, f_got, m_own, m_got)


def solution(mesh):
    tok_spec = P(('dp', 'ep'), None, None)
    col_spec = P(None, 'tp', None)
    exp_spec = P('ep', None, None)
    in_specs = (tok_spec, tok_spec, tok_spec, P(None), col_spec, col_spec, col_spec, P('tp', None, None), P(None), P(None, 'tp'), P(None, 'tp'), P('tp', None), P(None), P(None, None), exp_spec, exp_spec, exp_spec)
    n_ep, n_tp = mesh.shape['ep'], mesh.shape['tp']
    assert n_ep == 4 and n_tp == 2

    def over_x(v):
        return lax.ppermute(v, 'ep', [(i, i ^ 2) for i in range(4)])

    def over_core(v):
        return lax.ppermute(v, 'ep', [(i, i ^ 1) for i in range(4)])

    def over_tp(v):
        return lax.ppermute(v, 'tp', [(0, 1), (1, 0)])

    def layer(hidden_in, expert_ids, slot_ids, attn_gain, w_query, w_key, w_value, w_out, ffn_gain, w_gate, w_up, w_down, moe_gain, w_router, exp_gate, exp_up, exp_down):
        seq, d = hidden_in.shape[1:]
        top_k = expert_ids.shape[2]
        n_all = w_router.shape[1]
        n_exp = exp_gate.shape[0]
        half = seq // 2
        my_tp = lax.axis_index('tp')
        my_ep = lax.axis_index('ep')
        x2 = hidden_in.reshape(seq, d)
        ids = expert_ids.reshape(seq, top_k)

        width = w_out.shape[0] * w_out.shape[1]
        w_o = w_out.reshape(width, d)
        quarter = width // 4
        w_q0 = over_tp(lax.dynamic_slice(w_o, (my_ep * quarter, 0), (quarter, d)))

        inv_rms = inv_rms_of(x2.astype(F32))
        x_half = lax.dynamic_slice(x2, (my_tp * half, 0), (half, d))
        inv_half = lax.dynamic_slice(inv_rms, (my_tp * half, 0), (half, 1))
        ids_half = lax.dynamic_slice(ids, (my_tp * half, 0), (half, top_k))
        u_half = scaled(x_half, inv_half, moe_gain)
        u_c = over_core(u_half)
        logits = jnp.dot(u_half, w_router, preferred_element_type=F32)
        is_e = ids_half[:, :, None] == jnp.arange(n_all, dtype=jnp.int32)[None, None, :]
        picked = jnp.sum(jnp.where(is_e, logits[:, None, :], 0.0), axis=2)
        gates = jax.nn.softmax(picked, axis=-1)
        meta = jnp.concatenate([ids_half.astype(F32), gates], axis=1)
        meta_x = over_x(meta)
        u_x = over_x(u_half)
        meta2 = jnp.stack([meta, meta_x])
        meta_all = jnp.concatenate([meta2, over_core(meta2)])
        u_d = over_core(u_x)
        w_q1 = over_x(w_q0)
        w_q2 = over_core(w_q0)
        w_q3 = over_core(w_q1)

        ids_loc = meta_all[:, :, :top_k].astype(jnp.int32) - my_ep * n_exp
        gates_all = meta_all[:, :, top_k:]
        ids_t = jnp.swapaxes(ids_loc, 1, 2)
        e_ids = jnp.arange(n_exp, dtype=jnp.int32)
        sel_t = jnp.any(ids_t[:, None, :, :] == e_ids[None, :, None, None], axis=2)
        before = (jnp.arange(half)[:, None] < jnp.arange(half)[None, :]).astype(BF16)
        rank_f = jnp.dot(sel_t.reshape(-1, half).astype(BF16), before, preferred_element_type=F32).reshape(4, n_exp, half)
        n = jnp.sum(sel_t.astype(jnp.int32), axis=2)
        seg = (n + SEG - 1) // SEG * SEG
        lower4 = jnp.arange(4)[:, None] > jnp.arange(4)[None, :]
        loc = jnp.sum(jnp.where(lower4[:, :, None], seg[None], 0), axis=1)
        lower_e = jnp.arange(n_exp)[:, None] > jnp.arange(n_exp)[None, :]
        dst = jnp.sum(jnp.where(lower_e[None], seg[:, None, :], 0), axis=2)
        rows = jnp.sum(seg, axis=1)
        rank_i = rank_f.astype(jnp.int32)
        rank_t = jnp.where(sel_t, rank_i, -1)[:, :, None, :]
        pos_e = jnp.swapaxes(rank_i + dst[:, :, None], 1, 2)
        hit = ids_loc[..., None] == e_ids
        pos = jnp.sum(jnp.where(hit, pos_e[:, :, None, :] + 1, 0), axis=3) - 1

        x_norm = scaled(x2, inv_rms, attn_gain)
        hd = w_query.shape[2]
        q = jnp.dot(x_norm, w_query.reshape(d, width), preferred_element_type=F32)
        k = jnp.dot(x_norm, w_key.reshape(d, width), preferred_element_type=F32)
        v = jnp.dot(x_norm, w_value.reshape(d, width), preferred_element_type=F32).astype(BF16)
        cos_t, sin_t = rope_tables(seq, hd)
        ctx = attention(q, k, v, cos_t, sin_t, hd)
        ctx_peer = over_tp(ctx)

        cap_src = n_exp * (3 * seq * top_k // (2 * n_all))
        y_all = run_experts(n, loc, dst, rank_t, (u_half, u_x, u_c, u_d), exp_gate, exp_up, exp_down, cap_src, ctx)

        quarters = my_ep ^ jnp.arange(4, dtype=jnp.int32)
        after, f_norm = run_out(quarters, x2, ffn_gain, ctx, ctx_peer, w_o, (w_q0, w_q2, w_q1, w_q3), y_all)
        f_far = run_ffn(1 - my_tp, half, f_norm, w_gate, w_up, w_down, after, n_out=2)
        f_got = []
        for c in range(2):
            f_got.append(over_tp(f_far[c]))

        m3, = run_combine(3, rows, pos, gates_all, y_all, f_far[0])
        got3 = over_core(m3)
        m2, = run_combine(2, rows, pos, gates_all, y_all, m3)
        got2 = over_core(m2)
        m1 = run_combine(1, rows, pos, gates_all, y_all, m2, init=got3, n_out=CHUNKS)
        m_x = []
        for c in range(CHUNKS):
            m_x.append(over_x(m1[c]))
        f_own = run_ffn(my_tp, half, f_norm, w_gate, w_up, w_down, m1[0], add=after, n_out=CHUNKS)
        own, peer = [], []
        tie = f_own[0]
        for p in range(2):
            m0 = run_combine(0, rows, pos, gates_all, y_all, tie, init=got2, n_out=CHUNKS // 2, part=(p, 2))
            tie = m0[0]
            for k in range(CHUNKS // 2):
                c = p * (CHUNKS // 2) + k
                o_c = run_final(f_own[c], f_got[p], k, m0[k], m_x[c])
                own.append(o_c)
                peer.append(over_tp(o_c))
        first = my_tp == 0
        out = jnp.concatenate([jnp.where(first, a, b) for a, b in zip(own, peer)] + [jnp.where(first, b, a) for a, b in zip(own, peer)], axis=0)
        return out.reshape(1, seq, d)

    return jax.shard_map(layer, mesh=mesh, in_specs=in_specs, out_specs=tok_spec, check_vma=False)
```

```python
import functools
import jax
import jax.numpy as jnp
import numpy as np
from jax import lax
from jax.experimental import pallas as pl
from jax.experimental.pallas import tpu as pltpu
from jax.sharding import PartitionSpec as P

EPS = 1e-6
ROPE_BASE = 10000.0
F32 = jnp.float32
BF16 = jnp.bfloat16
SEG = 16
GT = 128
OUT = 96
CHUNKS = 4
CT = 256
VMEM_BIG = 60 * 1024 * 1024


def inv_rms_of(x_f32):
    return lax.rsqrt(jnp.mean(x_f32 * x_f32, axis=-1, keepdims=True) + EPS)


def scaled(x_val, inv, gain):
    return (x_val.astype(F32) * inv * gain.astype(F32)).astype(BF16)


def rope_tables(seq_len, head_dim):
    inv_freq = (np.float32(ROPE_BASE) ** (-np.arange(head_dim // 2, dtype=np.float32) * np.float32(2.0 / head_dim))).astype(np.float32)
    angle = (np.arange(seq_len, dtype=np.float32)[:, None] * inv_freq[None, :]).astype(np.float64)
    cos_tab, sin_tab = np.cos(angle).astype(np.float32), np.sin(angle).astype(np.float32)
    return np.concatenate([cos_tab, cos_tab], axis=1), np.concatenate([-sin_tab, sin_tab], axis=1)


def attn_kernel(q_ref, k_ref, v_ref, cos_ref, sin_ref, o_ref, k_scr):
    seq, hd = cos_ref.shape
    blk = 256
    pair = q_ref.shape[1] // hd
    for h in range(pair):
        hc = slice(h * hd, (h + 1) * hd)
        k_f = k_ref[:, hc]
        k_scr[:, hc] = (k_f * cos_ref[...] + pltpu.roll(k_f, hd // 2, 1) * sin_ref[...]).astype(BF16)
    for i in range(seq // blk):
        rows = slice(i * blk, (i + 1) * blk)
        kv = (i + 1) * blk
        for h in range(pair):
            hc = slice(h * hd, (h + 1) * hd)
            q_f = q_ref[rows, hc]
            q_b = (q_f * cos_ref[rows] + pltpu.roll(q_f, hd // 2, 1) * sin_ref[rows]).astype(BF16)
            s = lax.dot_general(q_b, k_scr[:kv, hc], (((1,), (1,)), ((), ())), preferred_element_type=F32) * hd ** -0.5
            r_id = lax.broadcasted_iota(jnp.int32, (blk, blk), 0)
            c_id = lax.broadcasted_iota(jnp.int32, (blk, blk), 1)
            last = jnp.where(r_id >= c_id, s[:, kv - blk:], -1e30)
            s = last if i == 0 else jnp.concatenate([s[:, :kv - blk], last], axis=1)
            p = jnp.exp(s - jnp.max(s, axis=1, keepdims=True))
            p = (p * (1.0 / jnp.sum(p, axis=1, keepdims=True))).astype(BF16)
            o_ref[rows, hc] = jnp.dot(p, v_ref[:kv, hc], preferred_element_type=F32).astype(BF16)


def attention(q, k, v, cos_t, sin_t, head_dim):
    seq, width = q.shape
    pair = 2
    steps = width // (pair * head_dim)
    col = pl.BlockSpec((seq, pair * head_dim), lambda h: (0, h))
    tab = pl.BlockSpec((seq, head_dim), lambda h: (0, 0))
    return pl.pallas_call(
        attn_kernel, grid=(steps,),
        in_specs=[col, col, col, tab, tab], out_specs=col,
        out_shape=jax.ShapeDtypeStruct((seq, width), BF16),
        scratch_shapes=[pltpu.VMEM((seq, pair * head_dim), BF16)],
        cost_estimate=pl.CostEstimate(flops=width * seq * seq * 4, bytes_accessed=12 * seq * width, transcendentals=0),
        name="attn",
    )(q, k, v, cos_t, sin_t)


def expert_kernel(n_ref, loc_ref, dst_ref, rank_ref, u0_ref, u1_ref, u2_ref, u3_ref, wg_ref, wu_ref, wd_ref, _after, y_hbm, x_scr, h_scr, y_scr, sem):
    e = pl.program_id(0)
    u_refs = (u0_ref, u1_ref, u2_ref, u3_ref)
    half, d = u0_ref.shape
    fe = wg_ref.shape[2]

    def gather(s, i):
        rid = lax.broadcasted_iota(jnp.int32, (GT, half), 0) + i * GT
        hot = (rank_ref[s, 0] == rid).astype(F32).astype(BF16)
        x_scr[pl.ds(pl.multiple_of(loc_ref[s, e] + i * GT, SEG), GT), :] = jnp.dot(hot, u_refs[s][...], preferred_element_type=F32).astype(BF16)

    for s in range(4):
        @pl.when(n_ref[s, e] > GT)
        def _():
            gather(s, 1)
    for s in range(4):
        gather(s, 0)

    total = loc_ref[3, e] + lax.shift_right_logical(n_ref[3, e] + (SEG - 1), 4) * SEG

    def copies(fn, ee):
        for s in range(4):
            for i in range(2):
                @pl.when(n_ref[s, ee] > i * OUT)
                def _():
                    fn(pltpu.make_async_copy(
                        y_scr.at[pl.ds(pl.multiple_of(loc_ref[s, ee] + i * OUT, SEG), OUT), :],
                        y_hbm.at[s, pl.ds(pl.multiple_of(dst_ref[s, ee] + i * OUT, SEG), OUT), :], sem))

    @pl.when(e > 0)
    def _():
        copies(lambda c: c.wait(), e - 1)

    def ffn(m0, rows):
        for c in range(fe // 512):
            cols = slice(c * 512, (c + 1) * 512)
            x = x_scr[pl.ds(m0, rows), :]
            g = jnp.dot(x, wg_ref[0, :, cols], preferred_element_type=F32)
            v = jnp.dot(x, wu_ref[0, :, cols], preferred_element_type=F32)
            h_scr[pl.ds(0, rows), cols] = (g * jax.nn.sigmoid(g) * v).astype(BF16)
        for c in range(d // 1024):
            cols = slice(c * 1024, (c + 1) * 1024)
            y_scr[pl.ds(m0, rows), cols] = jnp.dot(h_scr[pl.ds(0, rows), :], wd_ref[0, :, cols], preferred_element_type=F32).astype(BF16)

    for lo, hi in ((256, 288), (288, 320), (320, 352), (352, 384)):
        @pl.when((total > lo) & (total <= hi))
        def _():
            ffn(0, hi)

    @pl.when((total <= 256) | (total > 384))
    def _():
        def body(i, carry):
            ffn(pl.multiple_of(i * 256, 256), 256)
            return carry

        lax.fori_loop(0, lax.shift_right_logical(total + 255, 8), body, 0)

    copies(lambda c: c.start(), e)

    @pl.when(e == pl.num_programs(0) - 1)
    def _():
        copies(lambda c: c.wait(), e)


def run_experts(n, loc, dst, rank_t, u_four, wg, wu, wd, cap_src, after):
    half, d = u_four[0].shape
    n_exp, _, fe = wg.shape
    whole = pl.BlockSpec((half, d), lambda e, *_: (0, 0), pipeline_mode=pl.Buffered(1))
    grid_spec = pltpu.PrefetchScalarGridSpec(
        num_scalar_prefetch=3, grid=(n_exp,),
        in_specs=[
            pl.BlockSpec((4, 1, 1, half), lambda e, *_: (0, e, 0, 0)),
            whole, whole, whole, whole,
            pl.BlockSpec((1, d, fe), lambda e, *_: (e, 0, 0)),
            pl.BlockSpec((1, d, fe), lambda e, *_: (e, 0, 0)),
            pl.BlockSpec((1, fe, d), lambda e, *_: (e, 0, 0)),
            pl.BlockSpec(memory_space=pl.ANY),
        ],
        out_specs=pl.BlockSpec(memory_space=pl.ANY),
        scratch_shapes=[pltpu.VMEM((1024, d), BF16), pltpu.VMEM((384, fe), BF16), pltpu.VMEM((1024, d), BF16), pltpu.SemaphoreType.DMA],
    )
    return pl.pallas_call(
        expert_kernel, grid_spec=grid_spec,
        out_shape=jax.ShapeDtypeStruct((4, cap_src + 256, d), BF16),
        compiler_params=pltpu.CompilerParams(vmem_limit_bytes=VMEM_BIG),
        cost_estimate=pl.CostEstimate(flops=90_000_000_000, bytes_accessed=n_exp * d * fe * 6 + 40_000_000, transcendentals=0),
        name="experts",
    )(n, loc, dst, rank_t, *u_four, wg, wu, wd, after)


def combine_kernel(src, has_init, rows_ref, pos_ref, gate_ref, y_hbm, _after, *rest):
    init_ref = rest[0] if has_init else None
    *o_refs, y_a, y_b, g_a, g_b, sems = rest[1:] if has_init else rest
    half, top_k = pos_ref.shape
    rc, d = o_refs[0].shape
    n_rows = rows_ref[src]
    n_tiles = lax.shift_right_logical(n_rows + (CT - 1), 8)

    def fetch(i, buf, k):
        return pltpu.make_async_copy(y_hbm.at[src, pl.ds(pl.multiple_of(i * CT, CT), CT), :], buf, sems.at[k])

    def start(i, buf, k):
        @pl.when(i < n_tiles)
        def _():
            fetch(i, buf, k).start()

    def arrive(i, buf, k):
        @pl.when(i < n_tiles)
        def _():
            fetch(i, buf, k).wait()

        @pl.when(i >= n_tiles - 1)
        def _():
            live = lax.broadcasted_iota(jnp.int32, (CT, 1), 0) + i * CT < n_rows
            buf[...] = jnp.where(live, buf[...].astype(F32), 0.0).astype(BF16)

    def build(i, g_scr, b):
        rid = lax.broadcasted_iota(jnp.int32, (32, CT), 1) + i * CT
        tok = slice(b * 32, (b + 1) * 32)
        pos, gate = pos_ref[tok, :], gate_ref[tok, :]
        g = jnp.zeros((32, CT), F32)
        for j in range(top_k):
            g = jnp.where(pos[:, j:j + 1] == rid, gate[:, j:j + 1], g)
        hi = g.astype(BF16)
        left = g - hi.astype(F32)
        mid = left.astype(BF16)
        g_scr[tok, :CT] = (left - mid.astype(F32)).astype(BF16)
        g_scr[tok, CT:2 * CT] = mid
        g_scr[tok, 2 * CT:] = hi

    def multiply(g_scr, buf, i_next, g_next):
        n_c = d // 512
        blocks = half // 32
        for c in range(n_c):
            cols = slice(c * 512, (c + 1) * 512)
            y = buf[:, cols]
            part = jnp.dot(g_scr[...], jnp.concatenate([y, y, y], axis=0), preferred_element_type=F32)
            for b in range(c * blocks // n_c, (c + 1) * blocks // n_c):
                build(i_next, g_next, b)
            for k, o_ref in enumerate(o_refs):
                o_ref[:, cols] += part[k * rc:(k + 1) * rc]

    start(0, y_a, 0)
    for b in range(half // 32):
        build(0, g_a, b)
    for k, o_ref in enumerate(o_refs):
        o_ref[...] = init_ref[k * rc:(k + 1) * rc, :] if has_init else jnp.zeros_like(o_ref)

    def body(p, carry):
        i = 2 * p
        start(i + 1, y_b, 1)
        arrive(i, y_a, 0)
        multiply(g_a, y_a, i + 1, g_b)

        @pl.when(i + 1 < n_tiles)
        def _():
            start(i + 2, y_a, 0)
            arrive(i + 1, y_b, 1)
            multiply(g_b, y_b, i + 2, g_a)

        return carry

    lax.fori_loop(0, lax.shift_right_logical(n_tiles + 1, 1), body, 0)


def run_combine(src, rows, pos, gates, y_all, after, init=None, n_out=1, part=(0, 1)):
    d = y_all.shape[2]
    half, top_k = pos.shape[1] // part[1], pos.shape[2]
    small = pl.BlockSpec((half, top_k), lambda i, r: (part[0], 0))
    anywhere = pl.BlockSpec(memory_space=pl.ANY)
    extra = [] if init is None else [init]
    grid_spec = pltpu.PrefetchScalarGridSpec(
        num_scalar_prefetch=1, grid=(1,),
        in_specs=[small, small, anywhere, anywhere] + [pl.BlockSpec((half, d), lambda i, r: (0, 0)) for _ in extra],
        out_specs=[pl.BlockSpec((half // n_out, d), lambda i, r: (0, 0))] * n_out,
        scratch_shapes=[pltpu.VMEM((CT, d), BF16)] * 2 + [pltpu.VMEM((half, 3 * CT), BF16)] * 2 + [pltpu.SemaphoreType.DMA((2,))],
    )
    return pl.pallas_call(
        functools.partial(combine_kernel, src, init is not None), grid_spec=grid_spec,
        out_shape=[jax.ShapeDtypeStruct((half // n_out, d), F32)] * n_out,
        compiler_params=pltpu.CompilerParams(vmem_limit_bytes=40 * 1024 * 1024),
        cost_estimate=pl.CostEstimate(flops=12_000_000_000, bytes_accessed=10_000_000, transcendentals=0),
    )(rows, pos[src], gates[src], y_all, after, *extra)


def out_kernel(q_ref, x_ref, gain_ref, ctx_ref, peer_ref, wo_ref, w0_ref, w1_ref, w2_ref, w3_ref, _after, a_ref, n_ref):
    quarter = w0_ref.shape[0]
    o = jnp.dot(ctx_ref[...], wo_ref[...], preferred_element_type=F32)
    p = None
    for r, w in enumerate((w0_ref, w1_ref, w2_ref, w3_ref)):
        cols = pl.ds(pl.multiple_of(q_ref[r] * quarter, quarter), quarter)
        t = jnp.dot(peer_ref[:, cols], w[...], preferred_element_type=F32)
        p = t if p is None else p + t
    after = (x_ref[...].astype(F32) + (o + p)).astype(BF16)
    a_ref[...] = after
    a_f = after.astype(F32)
    inv = lax.rsqrt(jnp.mean(a_f * a_f, axis=1, keepdims=True) + EPS)
    n_ref[...] = (a_f * inv * gain_ref[...].astype(F32)).astype(BF16)


def run_out(quarters, x2, gain, ctx, ctx_peer, w_o, pieces, after):
    seq, d = x2.shape
    width = w_o.shape[0]
    blk = 256
    row = lambda n: pl.BlockSpec((blk, n), lambda i, q: (i, 0))
    const = lambda m, n: pl.BlockSpec((m, n), lambda i, q: (0, 0), pipeline_mode=pl.Buffered(1))
    grid_spec = pltpu.PrefetchScalarGridSpec(
        num_scalar_prefetch=1, grid=(seq // blk,),
        in_specs=[row(d), const(1, d), row(width), row(width), const(width, d)] + [const(width // 4, d)] * 4 + [pl.BlockSpec(memory_space=pl.ANY)],
        out_specs=[row(d), row(d)],
    )
    return pl.pallas_call(
        out_kernel, grid_spec=grid_spec,
        out_shape=[jax.ShapeDtypeStruct((seq, d), BF16)] * 2,
        compiler_params=pltpu.CompilerParams(vmem_limit_bytes=VMEM_BIG),
        cost_estimate=pl.CostEstimate(flops=10_000_000_000, bytes_accessed=24_000_000, transcendentals=0),
        name="out_proj",
    )(quarters, x2, gain.reshape(1, d), ctx, ctx_peer, w_o, *pieces, after)


def ffn_kernel(n_up, n_add, off_ref, x_ref, wg_ref, wu_ref, wd_ref, _after, *rest):
    adds, (*o_refs, h_scr) = rest[:n_add], rest[n_add:]
    i = pl.program_id(0)
    blk = wg_ref.shape[1]

    @pl.when(i < n_up)
    def _():
        x = x_ref[...]
        g = jnp.dot(x, wg_ref[...], preferred_element_type=F32)
        u = jnp.dot(x, wu_ref[...], preferred_element_type=F32)
        h_scr[:, pl.ds(pl.multiple_of(i * blk, blk), blk)] = (g * jax.nn.sigmoid(g) * u).astype(BF16)

    @pl.when(i >= n_up)
    def _():
        v = jnp.dot(h_scr[...], wd_ref[...], preferred_element_type=F32)
        for r in adds:
            v = r[...].astype(F32) + v
        rows = v.shape[0] // len(o_refs)
        for k, o_ref in enumerate(o_refs):
            o_ref[...] = v[k * rows:(k + 1) * rows]


def run_ffn(which, rows, f_norm, wg, wu, wd, after, adds=(), n_out=1):
    d, ff = wg.shape
    blk, out_blk = 512, 512
    n_up, n_down = ff // blk, d // out_blk
    down = lambda i: jnp.maximum(i - n_up, 0)
    up = lambda i: jnp.minimum(i, n_up - 1)
    add_specs = [
        pl.BlockSpec((rows, out_blk), (lambda i, w: (w[0], down(i))) if at is None else (lambda i, w, at=at: (at, down(i))))
        for _, at in adds]
    grid_spec = pltpu.PrefetchScalarGridSpec(
        num_scalar_prefetch=1, grid=(n_up + n_down,),
        in_specs=[pl.BlockSpec((rows, d), lambda i, w: (w[0], 0), pipeline_mode=pl.Buffered(1)),
                  pl.BlockSpec((d, blk), lambda i, w: (0, up(i))), pl.BlockSpec((d, blk), lambda i, w: (0, up(i))),
                  pl.BlockSpec((ff, out_blk), lambda i, w: (0, down(i))), pl.BlockSpec(memory_space=pl.ANY)] + add_specs,
        out_specs=[pl.BlockSpec((rows // n_out, out_blk), lambda i, w: (0, down(i)))] * n_out,
        scratch_shapes=[pltpu.VMEM((rows, ff), BF16)],
    )
    return pl.pallas_call(
        functools.partial(ffn_kernel, n_up, len(adds)), grid_spec=grid_spec,
        out_shape=[jax.ShapeDtypeStruct((rows // n_out, d), F32)] * n_out,
        compiler_params=pltpu.CompilerParams(vmem_limit_bytes=VMEM_BIG),
        cost_estimate=pl.CostEstimate(flops=rows * 56_000_000, bytes_accessed=60_000_000, transcendentals=0),
        name="ffn",
    )(which.reshape(1), f_norm, wg, wu, wd, after, *[v for v, _ in adds])


def final_kernel(s_ref, g_ref, x_ref, o_ref):
    o_ref[...] = ((s_ref[...] + g_ref[...]) + x_ref[...]).astype(BF16)


def run_final(s_own, f_got, got_block, m_got, m_block):
    rows, d = s_own.shape
    row = lambda b: pl.BlockSpec((rows, d), lambda i, b=b: (b, 0))
    return pl.pallas_call(
        final_kernel, grid=(1,), in_specs=[row(0), row(got_block), row(m_block)], out_specs=row(0),
        out_shape=jax.ShapeDtypeStruct((rows, d), BF16),
        cost_estimate=pl.CostEstimate(flops=3 * rows * d, bytes_accessed=14 * rows * d, transcendentals=0),
        name="final",
    )(s_own, f_got, m_got)


def solution(mesh):
    tok_spec = P(('dp', 'ep'), None, None)
    col_spec = P(None, 'tp', None)
    exp_spec = P('ep', None, None)
    in_specs = (tok_spec, tok_spec, tok_spec, P(None), col_spec, col_spec, col_spec, P('tp', None, None), P(None), P(None, 'tp'), P(None, 'tp'), P('tp', None), P(None), P(None, None), exp_spec, exp_spec, exp_spec)
    n_ep, n_tp = mesh.shape['ep'], mesh.shape['tp']
    assert n_ep == 4 and n_tp == 2

    def over_x(v):
        return lax.ppermute(v, 'ep', [(i, i ^ 2) for i in range(4)])

    def over_core(v):
        return lax.ppermute(v, 'ep', [(i, i ^ 1) for i in range(4)])

    def over_tp(v):
        return lax.ppermute(v, 'tp', [(0, 1), (1, 0)])

    def layer(hidden_in, expert_ids, slot_ids, attn_gain, w_query, w_key, w_value, w_out, ffn_gain, w_gate, w_up, w_down, moe_gain, w_router, exp_gate, exp_up, exp_down):
        seq, d = hidden_in.shape[1:]
        top_k = expert_ids.shape[2]
        n_all = w_router.shape[1]
        n_exp = exp_gate.shape[0]
        half = seq // 2
        my_tp = lax.axis_index('tp')
        my_ep = lax.axis_index('ep')
        x2 = hidden_in.reshape(seq, d)
        ids = expert_ids.reshape(seq, top_k)

        width = w_out.shape[0] * w_out.shape[1]
        w_o = w_out.reshape(width, d)
        quarter = width // 4
        w_q0 = over_tp(lax.dynamic_slice(w_o, (my_ep * quarter, 0), (quarter, d)))

        inv_rms = inv_rms_of(x2.astype(F32))
        x_half = lax.dynamic_slice(x2, (my_tp * half, 0), (half, d))
        inv_half = lax.dynamic_slice(inv_rms, (my_tp * half, 0), (half, 1))
        ids_half = lax.dynamic_slice(ids, (my_tp * half, 0), (half, top_k))
        u_half = scaled(x_half, inv_half, moe_gain)
        u_c = over_core(u_half)
        logits = jnp.dot(u_half, w_router, preferred_element_type=F32)
        is_e = ids_half[:, :, None] == jnp.arange(n_all, dtype=jnp.int32)[None, None, :]
        picked = jnp.sum(jnp.where(is_e, logits[:, None, :], 0.0), axis=2)
        gates = jax.nn.softmax(picked, axis=-1)
        meta = jnp.concatenate([ids_half.astype(F32), gates], axis=1)
        meta_x = over_x(meta)
        u_x = over_x(u_half)
        meta2 = jnp.stack([meta, meta_x])
        meta_c = over_core(meta2)
        meta_all = jnp.concatenate([meta2, meta_c])
        u_d = over_core(u_x)
        w_q1 = over_x(w_q0)
        w_q2 = over_core(w_q0)
        w_q3 = over_core(w_q1)

        ids_loc = meta_all[:, :, :top_k].astype(jnp.int32) - my_ep * n_exp
        gates_all = meta_all[:, :, top_k:]
        ids_t = jnp.swapaxes(ids_loc, 1, 2)
        e_ids = jnp.arange(n_exp, dtype=jnp.int32)
        sel_t = jnp.any(ids_t[:, None, :, :] == e_ids[None, :, None, None], axis=2)
        before = (jnp.arange(half)[:, None] < jnp.arange(half)[None, :]).astype(BF16)
        rank_f = jnp.dot(sel_t.reshape(-1, half).astype(BF16), before, preferred_element_type=F32).reshape(4, n_exp, half)
        n = jnp.sum(sel_t.astype(jnp.int32), axis=2)
        seg = (n + SEG - 1) // SEG * SEG
        lower4 = jnp.arange(4)[:, None] > jnp.arange(4)[None, :]
        loc = jnp.sum(jnp.where(lower4[:, :, None], seg[None], 0), axis=1)
        lower_e = jnp.arange(n_exp)[:, None] > jnp.arange(n_exp)[None, :]
        dst = jnp.sum(jnp.where(lower_e[None], seg[:, None, :], 0), axis=2)
        rows = jnp.sum(seg, axis=1)
        rank_i = rank_f.astype(jnp.int32)
        rank_t = jnp.where(sel_t, rank_i, -1)[:, :, None, :]
        pos_e = jnp.swapaxes(rank_i + dst[:, :, None], 1, 2)
        hit = ids_loc[..., None] == e_ids
        pos = jnp.sum(jnp.where(hit, pos_e[:, :, None, :] + 1, 0), axis=3) - 1

        x_norm = scaled(x2, inv_rms, attn_gain)
        hd = w_query.shape[2]
        q = jnp.dot(x_norm, w_query.reshape(d, width), preferred_element_type=F32)
        k = jnp.dot(x_norm, w_key.reshape(d, width), preferred_element_type=F32)
        v = jnp.dot(x_norm, w_value.reshape(d, width), preferred_element_type=F32).astype(BF16)
        cos_t, sin_t = rope_tables(seq, hd)
        ctx = attention(q, k, v, cos_t, sin_t, hd)
        ctx_peer = over_tp(ctx)

        cap_src = n_exp * (3 * seq * top_k // (2 * n_all))
        y_all = run_experts(n, loc, dst, rank_t, (u_half, u_x, u_c, u_d), exp_gate, exp_up, exp_down, cap_src, ctx)

        quarters = my_ep ^ jnp.arange(4, dtype=jnp.int32)
        after, f_norm = run_out(quarters, x2, ffn_gain, ctx, ctx_peer, w_o, (w_q0, w_q2, w_q1, w_q3), y_all)
        f_far = run_ffn(1 - my_tp, half, f_norm, w_gate, w_up, w_down, after, n_out=2)
        f_got = []
        for c in range(2):
            f_got.append(over_tp(f_far[c]))

        got3, m_x = [], []
        tie = f_far[0]
        for p in range(2):
            m3, = run_combine(3, rows, pos, gates_all, y_all, tie, part=(p, 2))
            tie = m3
            got3.append(over_core(m3))
        for p in range(2):
            m1 = run_combine(1, rows, pos, gates_all, y_all, tie, init=got3[p], n_out=CHUNKS // 2, part=(p, 2))
            tie = m1[0]
            for k in range(CHUNKS // 2):
                m_x.append(over_x(m1[k]))
        m2, = run_combine(2, rows, pos, gates_all, y_all, tie)
        got2 = over_core(m2)
        m0, = run_combine(0, rows, pos, gates_all, y_all, m2)

        own, peer = [], []
        tie = m0
        for p in range(2):
            s_own = run_ffn(2 * my_tp + p, half // 2, f_norm, w_gate, w_up, w_down, tie,
                            adds=((after, None), (m0, p), (got2, p)), n_out=CHUNKS // 2)
            for k in range(CHUNKS // 2):
                c = p * (CHUNKS // 2) + k
                o_c = run_final(s_own[k], f_got[p], k, m_x[c], 0)
                tie = o_c
                own.append(o_c)
                peer.append(over_tp(o_c))
        first = my_tp == 0
        out = jnp.concatenate([jnp.where(first, a, b) for a, b in zip(own, peer)] + [jnp.where(first, b, a) for a, b in zip(own, peer)], axis=0)
        return out.reshape(1, seq, d)

    return jax.shard_map(layer, mesh=mesh, in_specs=in_specs, out_specs=tok_spec, check_vma=False)
```

```python
import functools
import jax
import jax.numpy as jnp
import numpy as np
from jax import lax
from jax.experimental import pallas as pl
from jax.experimental.pallas import tpu as pltpu
from jax.sharding import PartitionSpec as P

EPS = 1e-6
ROPE_BASE = 10000.0
F32 = jnp.float32
BF16 = jnp.bfloat16
SEG = 16
GT = 128
OUT = 96
CHUNKS = 4
CT = 256
VMEM_BIG = 60 * 1024 * 1024


def inv_rms_of(x_f32):
    return lax.rsqrt(jnp.mean(x_f32 * x_f32, axis=-1, keepdims=True) + EPS)


def scaled(x_val, inv, gain):
    return (x_val.astype(F32) * inv * gain.astype(F32)).astype(BF16)


def rope_tables(seq_len, head_dim):
    inv_freq = (np.float32(ROPE_BASE) ** (-np.arange(head_dim // 2, dtype=np.float32) * np.float32(2.0 / head_dim))).astype(np.float32)
    angle = (np.arange(seq_len, dtype=np.float32)[:, None] * inv_freq[None, :]).astype(np.float64)
    cos_tab, sin_tab = np.cos(angle).astype(np.float32), np.sin(angle).astype(np.float32)
    return np.concatenate([cos_tab, cos_tab], axis=1), np.concatenate([-sin_tab, sin_tab], axis=1)


def attn_kernel(q_ref, k_ref, v_ref, cos_ref, sin_ref, o_ref, k_scr, *bufs):
    seq, hd = cos_ref.shape
    blk, strip = 256, 32
    factor = hd ** -0.5 * 1.4426950408889634
    pair = q_ref.shape[1] // hd
    for h in range(pair):
        hc = slice(h * hd, (h + 1) * hd)
        k_f = k_ref[:, hc]
        k_scr[:, hc] = (k_f * cos_ref[...] + pltpu.roll(k_f, hd // 2, 1) * sin_ref[...]).astype(BF16)
    r_id = lax.broadcasted_iota(jnp.int32, (strip, blk), 0)
    c_id = lax.broadcasted_iota(jnp.int32, (strip, blk), 1)
    for i in range(seq // blk):
        rows = slice(i * blk, (i + 1) * blk)
        kv = (i + 1) * blk
        for h in range(pair):
            s_scr, p_scr = bufs[2 * h], bufs[2 * h + 1]
            hc = slice(h * hd, (h + 1) * hd)
            q_f = q_ref[rows, hc]
            q_b = (q_f * cos_ref[rows] + pltpu.roll(q_f, hd // 2, 1) * sin_ref[rows]).astype(BF16)
            s_scr[:, :kv] = lax.dot_general(q_b, k_scr[:kv, hc], (((1,), (1,)), ((), ())), preferred_element_type=F32)
        for h in range(pair):
            s_scr, p_scr = bufs[2 * h], bufs[2 * h + 1]
            for t in range(blk // strip):
                sr = slice(t * strip, (t + 1) * strip)
                last = jnp.where(r_id + t * strip >= c_id, s_scr[sr, kv - blk:kv], -1e30)
                s = last if i == 0 else jnp.concatenate([s_scr[sr, :kv - blk], last], axis=1)
                p = jnp.exp2((s - jnp.max(s, axis=1, keepdims=True)) * factor)
                p_scr[sr, :kv] = (p * (1.0 / jnp.sum(p, axis=1, keepdims=True))).astype(BF16)
        for h in range(pair):
            s_scr, p_scr = bufs[2 * h], bufs[2 * h + 1]
            hc = slice(h * hd, (h + 1) * hd)
            o_ref[rows, hc] = jnp.dot(p_scr[:, :kv], v_ref[:kv, hc], preferred_element_type=F32).astype(BF16)


def attention(q, k, v, cos_t, sin_t, head_dim):
    seq, width = q.shape
    pair = 2
    steps = width // (pair * head_dim)
    col = pl.BlockSpec((seq, pair * head_dim), lambda h: (0, h))
    tab = pl.BlockSpec((seq, head_dim), lambda h: (0, 0))
    return pl.pallas_call(
        attn_kernel, grid=(steps,),
        in_specs=[col, col, col, tab, tab], out_specs=col,
        out_shape=jax.ShapeDtypeStruct((seq, width), BF16),
        scratch_shapes=[pltpu.VMEM((seq, pair * head_dim), BF16)] + [pltpu.VMEM((256, seq), F32), pltpu.VMEM((256, seq), BF16)] * pair,
        cost_estimate=pl.CostEstimate(flops=width * seq * seq * 4, bytes_accessed=12 * seq * width, transcendentals=0),
        name="attn",
    )(q, k, v, cos_t, sin_t)


def expert_kernel(n_ref, loc_ref, dst_ref, rank_ref, u0_ref, u1_ref, u2_ref, u3_ref, wg_ref, wu_ref, wd_ref, _after, y_hbm, x_scr, h_scr, y_scr, sem):
    e = pl.program_id(0)
    u_refs = (u0_ref, u1_ref, u2_ref, u3_ref)
    half, d = u0_ref.shape
    fe = wg_ref.shape[2]

    def gather(s, i):
        rid = lax.broadcasted_iota(jnp.int32, (GT, half), 0) + i * GT
        hot = (rank_ref[s, 0] == rid).astype(F32).astype(BF16)
        x_scr[pl.ds(pl.multiple_of(loc_ref[s, e] + i * GT, SEG), GT), :] = jnp.dot(hot, u_refs[s][...], preferred_element_type=F32).astype(BF16)

    for s in range(4):
        @pl.when(n_ref[s, e] > GT)
        def _():
            gather(s, 1)
    for s in range(4):
        gather(s, 0)

    total = loc_ref[3, e] + lax.shift_right_logical(n_ref[3, e] + (SEG - 1), 4) * SEG

    def copies(fn, ee):
        for s in range(4):
            for i in range(2):
                @pl.when(n_ref[s, ee] > i * OUT)
                def _():
                    fn(pltpu.make_async_copy(
                        y_scr.at[pl.ds(pl.multiple_of(loc_ref[s, ee] + i * OUT, SEG), OUT), :],
                        y_hbm.at[s, pl.ds(pl.multiple_of(dst_ref[s, ee] + i * OUT, SEG), OUT), :], sem))

    @pl.when(e > 0)
    def _():
        copies(lambda c: c.wait(), e - 1)

    def ffn(m0, rows):
        for c in range(fe // 512):
            cols = slice(c * 512, (c + 1) * 512)
            x = x_scr[pl.ds(m0, rows), :]
            g = jnp.dot(x, wg_ref[0, :, cols], preferred_element_type=F32)
            v = jnp.dot(x, wu_ref[0, :, cols], preferred_element_type=F32)
            h_scr[pl.ds(0, rows), cols] = (g * jax.nn.sigmoid(g) * v).astype(BF16)
        for c in range(d // 1024):
            cols = slice(c * 1024, (c + 1) * 1024)
            y_scr[pl.ds(m0, rows), cols] = jnp.dot(h_scr[pl.ds(0, rows), :], wd_ref[0, :, cols], preferred_element_type=F32).astype(BF16)

    for lo, hi in ((256, 288), (288, 320), (320, 352), (352, 384)):
        @pl.when((total > lo) & (total <= hi))
        def _():
            ffn(0, hi)

    @pl.when((total <= 256) | (total > 384))
    def _():
        def body(i, carry):
            ffn(pl.multiple_of(i * 256, 256), 256)
            return carry

        lax.fori_loop(0, lax.shift_right_logical(total + 255, 8), body, 0)

    copies(lambda c: c.start(), e)

    @pl.when(e == pl.num_programs(0) - 1)
    def _():
        copies(lambda c: c.wait(), e)


def run_experts(n, loc, dst, rank_t, u_four, wg, wu, wd, cap_src, after):
    half, d = u_four[0].shape
    n_exp, _, fe = wg.shape
    whole = pl.BlockSpec((half, d), lambda e, *_: (0, 0), pipeline_mode=pl.Buffered(1))
    grid_spec = pltpu.PrefetchScalarGridSpec(
        num_scalar_prefetch=3, grid=(n_exp,),
        in_specs=[
            pl.BlockSpec((4, 1, 1, half), lambda e, *_: (0, e, 0, 0)),
            whole, whole, whole, whole,
            pl.BlockSpec((1, d, fe), lambda e, *_: (e, 0, 0)),
            pl.BlockSpec((1, d, fe), lambda e, *_: (e, 0, 0)),
            pl.BlockSpec((1, fe, d), lambda e, *_: (e, 0, 0)),
            pl.BlockSpec(memory_space=pl.ANY),
        ],
        out_specs=pl.BlockSpec(memory_space=pl.ANY),
        scratch_shapes=[pltpu.VMEM((1024, d), BF16), pltpu.VMEM((384, fe), BF16), pltpu.VMEM((1024, d), BF16), pltpu.SemaphoreType.DMA],
    )
    return pl.pallas_call(
        expert_kernel, grid_spec=grid_spec,
        out_shape=jax.ShapeDtypeStruct((4, cap_src + 256, d), BF16),
        compiler_params=pltpu.CompilerParams(vmem_limit_bytes=VMEM_BIG),
        cost_estimate=pl.CostEstimate(flops=90_000_000_000, bytes_accessed=n_exp * d * fe * 6 + 40_000_000, transcendentals=0),
        name="experts",
    )(n, loc, dst, rank_t, *u_four, wg, wu, wd, after)


def combine_kernel(src, has_init, rows_ref, pos_ref, gate_ref, y_hbm, _after, *rest):
    init_ref = rest[0] if has_init else None
    *o_refs, y_a, y_b, g_a, g_b, sems = rest[1:] if has_init else rest
    half, top_k = pos_ref.shape
    rc, d = o_refs[0].shape
    n_rows = rows_ref[src]
    n_tiles = lax.shift_right_logical(n_rows + (CT - 1), 8)

    def fetch(i, buf, k):
        return pltpu.make_async_copy(y_hbm.at[src, pl.ds(pl.multiple_of(i * CT, CT), CT), :], buf, sems.at[k])

    def start(i, buf, k):
        @pl.when(i < n_tiles)
        def _():
            fetch(i, buf, k).start()

    def arrive(i, buf, k):
        @pl.when(i < n_tiles)
        def _():
            fetch(i, buf, k).wait()

        @pl.when(i >= n_tiles - 1)
        def _():
            live = lax.broadcasted_iota(jnp.int32, (CT, 1), 0) + i * CT < n_rows
            buf[...] = jnp.where(live, buf[...].astype(F32), 0.0).astype(BF16)

    def build(i, g_scr, b):
        rid = lax.broadcasted_iota(jnp.int32, (32, CT), 1) + i * CT
        tok = slice(b * 32, (b + 1) * 32)
        pos, gate = pos_ref[tok, :], gate_ref[tok, :]
        g = jnp.zeros((32, CT), F32)
        for j in range(top_k):
            g = jnp.where(pos[:, j:j + 1] == rid, gate[:, j:j + 1], g)
        hi = g.astype(BF16)
        left = g - hi.astype(F32)
        mid = left.astype(BF16)
        g_scr[tok, :CT] = (left - mid.astype(F32)).astype(BF16)
        g_scr[tok, CT:2 * CT] = mid
        g_scr[tok, 2 * CT:] = hi

    def multiply(g_scr, buf, i_next, g_next):
        n_c = d // 512
        blocks = half // 32
        for c in range(n_c):
            cols = slice(c * 512, (c + 1) * 512)
            y = buf[:, cols]
            part = jnp.dot(g_scr[...], jnp.concatenate([y, y, y], axis=0), preferred_element_type=F32)
            for b in range(c * blocks // n_c, (c + 1) * blocks // n_c):
                build(i_next, g_next, b)
            for k, o_ref in enumerate(o_refs):
                o_ref[:, cols] += part[k * rc:(k + 1) * rc]

    start(0, y_a, 0)
    for b in range(half // 32):
        build(0, g_a, b)
    for k, o_ref in enumerate(o_refs):
        o_ref[...] = init_ref[k * rc:(k + 1) * rc, :] if has_init else jnp.zeros_like(o_ref)

    def body(p, carry):
        i = 2 * p
        start(i + 1, y_b, 1)
        arrive(i, y_a, 0)
        multiply(g_a, y_a, i + 1, g_b)

        @pl.when(i + 1 < n_tiles)
        def _():
            start(i + 2, y_a, 0)
            arrive(i + 1, y_b, 1)
            multiply(g_b, y_b, i + 2, g_a)

        return carry

    lax.fori_loop(0, lax.shift_right_logical(n_tiles + 1, 1), body, 0)


def run_combine(src, rows, pos, gates, y_all, after, init=None, n_out=1, part=(0, 1)):
    d = y_all.shape[2]
    half, top_k = pos.shape[1] // part[1], pos.shape[2]
    small = pl.BlockSpec((half, top_k), lambda i, r: (part[0], 0))
    anywhere = pl.BlockSpec(memory_space=pl.ANY)
    extra = [] if init is None else [init]
    grid_spec = pltpu.PrefetchScalarGridSpec(
        num_scalar_prefetch=1, grid=(1,),
        in_specs=[small, small, anywhere, anywhere] + [pl.BlockSpec((half, d), lambda i, r: (0, 0)) for _ in extra],
        out_specs=[pl.BlockSpec((half // n_out, d), lambda i, r: (0, 0))] * n_out,
        scratch_shapes=[pltpu.VMEM((CT, d), BF16)] * 2 + [pltpu.VMEM((half, 3 * CT), BF16)] * 2 + [pltpu.SemaphoreType.DMA((2,))],
    )
    return pl.pallas_call(
        functools.partial(combine_kernel, src, init is not None), grid_spec=grid_spec,
        out_shape=[jax.ShapeDtypeStruct((half // n_out, d), F32)] * n_out,
        compiler_params=pltpu.CompilerParams(vmem_limit_bytes=40 * 1024 * 1024),
        cost_estimate=pl.CostEstimate(flops=12_000_000_000, bytes_accessed=10_000_000, transcendentals=0),
    )(rows, pos[src], gates[src], y_all, after, *extra)


def out_kernel(q_ref, x_ref, gain_ref, ctx_ref, peer_ref, wo_ref, w0_ref, w1_ref, w2_ref, w3_ref, _after, a_ref, n_ref):
    quarter = w0_ref.shape[0]
    o = jnp.dot(ctx_ref[...], wo_ref[...], preferred_element_type=F32)
    p = None
    for r, w in enumerate((w0_ref, w1_ref, w2_ref, w3_ref)):
        cols = pl.ds(pl.multiple_of(q_ref[r] * quarter, quarter), quarter)
        t = jnp.dot(peer_ref[:, cols], w[...], preferred_element_type=F32)
        p = t if p is None else p + t
    after = (x_ref[...].astype(F32) + (o + p)).astype(BF16)
    a_ref[...] = after
    a_f = after.astype(F32)
    inv = lax.rsqrt(jnp.mean(a_f * a_f, axis=1, keepdims=True) + EPS)
    n_ref[...] = (a_f * inv * gain_ref[...].astype(F32)).astype(BF16)


def run_out(quarters, x2, gain, ctx, ctx_peer, w_o, pieces, after):
    seq, d = x2.shape
    width = w_o.shape[0]
    blk = 256
    row = lambda n: pl.BlockSpec((blk, n), lambda i, q: (i, 0))
    const = lambda m, n: pl.BlockSpec((m, n), lambda i, q: (0, 0), pipeline_mode=pl.Buffered(1))
    grid_spec = pltpu.PrefetchScalarGridSpec(
        num_scalar_prefetch=1, grid=(seq // blk,),
        in_specs=[row(d), const(1, d), row(width), row(width), const(width, d)] + [const(width // 4, d)] * 4 + [pl.BlockSpec(memory_space=pl.ANY)],
        out_specs=[row(d), row(d)],
    )
    return pl.pallas_call(
        out_kernel, grid_spec=grid_spec,
        out_shape=[jax.ShapeDtypeStruct((seq, d), BF16)] * 2,
        compiler_params=pltpu.CompilerParams(vmem_limit_bytes=VMEM_BIG),
        cost_estimate=pl.CostEstimate(flops=10_000_000_000, bytes_accessed=24_000_000, transcendentals=0),
        name="out_proj",
    )(quarters, x2, gain.reshape(1, d), ctx, ctx_peer, w_o, *pieces, after)


def ffn_kernel(n_up, n_add, off_ref, x_ref, wg_ref, wu_ref, wd_ref, _after, *rest):
    adds, (*o_refs, h_scr) = rest[:n_add], rest[n_add:]
    i = pl.program_id(0)
    blk = wg_ref.shape[1]

    @pl.when(i < n_up)
    def _():
        x = x_ref[...]
        g = jnp.dot(x, wg_ref[...], preferred_element_type=F32)
        u = jnp.dot(x, wu_ref[...], preferred_element_type=F32)
        h_scr[:, pl.ds(pl.multiple_of(i * blk, blk), blk)] = (g * jax.nn.sigmoid(g) * u).astype(BF16)

    @pl.when(i >= n_up)
    def _():
        v = jnp.dot(h_scr[...], wd_ref[...], preferred_element_type=F32)
        for r in adds:
            v = r[...].astype(F32) + v
        rows = v.shape[0] // len(o_refs)
        for k, o_ref in enumerate(o_refs):
            o_ref[...] = v[k * rows:(k + 1) * rows]


def run_ffn(which, rows, f_norm, wg, wu, wd, after, adds=(), n_out=1):
    d, ff = wg.shape
    blk, out_blk = 512, 512
    n_up, n_down = ff // blk, d // out_blk
    down = lambda i: jnp.maximum(i - n_up, 0)
    up = lambda i: jnp.minimum(i, n_up - 1)
    add_specs = [
        pl.BlockSpec((rows, out_blk), (lambda i, w: (w[0], down(i))) if at is None else (lambda i, w, at=at: (at, down(i))))
        for _, at in adds]
    grid_spec = pltpu.PrefetchScalarGridSpec(
        num_scalar_prefetch=1, grid=(n_up + n_down,),
        in_specs=[pl.BlockSpec((rows, d), lambda i, w: (w[0], 0), pipeline_mode=pl.Buffered(1)),
                  pl.BlockSpec((d, blk), lambda i, w: (0, up(i))), pl.BlockSpec((d, blk), lambda i, w: (0, up(i))),
                  pl.BlockSpec((ff, out_blk), lambda i, w: (0, down(i))), pl.BlockSpec(memory_space=pl.ANY)] + add_specs,
        out_specs=[pl.BlockSpec((rows // n_out, out_blk), lambda i, w: (0, down(i)))] * n_out,
        scratch_shapes=[pltpu.VMEM((rows, ff), BF16)],
    )
    return pl.pallas_call(
        functools.partial(ffn_kernel, n_up, len(adds)), grid_spec=grid_spec,
        out_shape=[jax.ShapeDtypeStruct((rows // n_out, d), F32)] * n_out,
        compiler_params=pltpu.CompilerParams(vmem_limit_bytes=VMEM_BIG),
        cost_estimate=pl.CostEstimate(flops=rows * 56_000_000, bytes_accessed=60_000_000, transcendentals=0),
        name="ffn",
    )(which.reshape(1), f_norm, wg, wu, wd, after, *[v for v, _ in adds])


def final_kernel(s_ref, g_ref, m_ref, c_ref, x_ref, o_ref):
    o_ref[...] = ((s_ref[...] + g_ref[...]) + ((m_ref[...] + c_ref[...]) + x_ref[...])).astype(BF16)


def run_final(arrays):
    rows, d = arrays[-1][0].shape
    in_specs = [pl.BlockSpec((rows, d), lambda i, b=b: (b, 0)) for _, b in arrays]
    return pl.pallas_call(
        final_kernel, grid=(1,), in_specs=in_specs, out_specs=pl.BlockSpec((rows, d), lambda i: (0, 0)),
        out_shape=jax.ShapeDtypeStruct((rows, d), BF16),
        cost_estimate=pl.CostEstimate(flops=5 * rows * d, bytes_accessed=22 * rows * d, transcendentals=0),
        name="final",
    )(*[v for v, _ in arrays])


def solution(mesh):
    tok_spec = P(('dp', 'ep'), None, None)
    col_spec = P(None, 'tp', None)
    exp_spec = P('ep', None, None)
    in_specs = (tok_spec, tok_spec, tok_spec, P(None), col_spec, col_spec, col_spec, P('tp', None, None), P(None), P(None, 'tp'), P(None, 'tp'), P('tp', None), P(None), P(None, None), exp_spec, exp_spec, exp_spec)
    n_ep, n_tp = mesh.shape['ep'], mesh.shape['tp']
    assert n_ep == 4 and n_tp == 2

    def over_x(v):
        return lax.ppermute(v, 'ep', [(i, i ^ 2) for i in range(4)])

    def over_core(v):
        return lax.ppermute(v, 'ep', [(i, i ^ 1) for i in range(4)])

    def over_tp(v):
        return lax.ppermute(v, 'tp', [(0, 1), (1, 0)])

    def layer(hidden_in, expert_ids, slot_ids, attn_gain, w_query, w_key, w_value, w_out, ffn_gain, w_gate, w_up, w_down, moe_gain, w_router, exp_gate, exp_up, exp_down):
        seq, d = hidden_in.shape[1:]
        top_k = expert_ids.shape[2]
        n_all = w_router.shape[1]
        n_exp = exp_gate.shape[0]
        half = seq // 2
        my_tp = lax.axis_index('tp')
        my_ep = lax.axis_index('ep')
        x2 = hidden_in.reshape(seq, d)
        ids = expert_ids.reshape(seq, top_k)

        width = w_out.shape[0] * w_out.shape[1]
        w_o = w_out.reshape(width, d)
        quarter = width // 4
        w_q0 = over_tp(lax.dynamic_slice(w_o, (my_ep * quarter, 0), (quarter, d)))

        inv_rms = inv_rms_of(x2.astype(F32))
        x_half = lax.dynamic_slice(x2, (my_tp * half, 0), (half, d))
        inv_half = lax.dynamic_slice(inv_rms, (my_tp * half, 0), (half, 1))
        ids_half = lax.dynamic_slice(ids, (my_tp * half, 0), (half, top_k))
        u_half = scaled(x_half, inv_half, moe_gain)
        u_c = over_core(u_half)
        logits = jnp.dot(u_half, w_router, preferred_element_type=F32)
        is_e = ids_half[:, :, None] == jnp.arange(n_all, dtype=jnp.int32)[None, None, :]
        picked = jnp.sum(jnp.where(is_e, logits[:, None, :], 0.0), axis=2)
        gates = jax.nn.softmax(picked, axis=-1)
        meta = jnp.concatenate([ids_half.astype(F32), gates], axis=1)
        meta_x = over_x(meta)
        u_x = over_x(u_half)
        meta2 = jnp.stack([meta, meta_x])
        meta_c = over_core(meta2)
        meta_all = jnp.concatenate([meta2, meta_c])
        u_d = over_core(u_x)
        w_q1 = over_x(w_q0)
        w_q2 = over_core(w_q0)
        w_q3 = over_core(w_q1)

        ids_loc = meta_all[:, :, :top_k].astype(jnp.int32) - my_ep * n_exp
        gates_all = meta_all[:, :, top_k:]
        ids_t = jnp.swapaxes(ids_loc, 1, 2)
        e_ids = jnp.arange(n_exp, dtype=jnp.int32)
        sel_t = jnp.any(ids_t[:, None, :, :] == e_ids[None, :, None, None], axis=2)
        before = (jnp.arange(half)[:, None] < jnp.arange(half)[None, :]).astype(BF16)
        rank_f = jnp.dot(sel_t.reshape(-1, half).astype(BF16), before, preferred_element_type=F32).reshape(4, n_exp, half)
        n = jnp.sum(sel_t.astype(jnp.int32), axis=2)
        seg = (n + SEG - 1) // SEG * SEG
        lower4 = jnp.arange(4)[:, None] > jnp.arange(4)[None, :]
        loc = jnp.sum(jnp.where(lower4[:, :, None], seg[None], 0), axis=1)
        lower_e = jnp.arange(n_exp)[:, None] > jnp.arange(n_exp)[None, :]
        dst = jnp.sum(jnp.where(lower_e[None], seg[:, None, :], 0), axis=2)
        rows = jnp.sum(seg, axis=1)
        rank_i = rank_f.astype(jnp.int32)
        rank_t = jnp.where(sel_t, rank_i, -1)[:, :, None, :]
        pos_e = jnp.swapaxes(rank_i + dst[:, :, None], 1, 2)
        hit = ids_loc[..., None] == e_ids
        pos = jnp.sum(jnp.where(hit, pos_e[:, :, None, :] + 1, 0), axis=3) - 1

        x_norm = scaled(x2, inv_rms, attn_gain)
        hd = w_query.shape[2]
        q = jnp.dot(x_norm, w_query.reshape(d, width), preferred_element_type=F32)
        k = jnp.dot(x_norm, w_key.reshape(d, width), preferred_element_type=F32)
        v = jnp.dot(x_norm, w_value.reshape(d, width), preferred_element_type=F32).astype(BF16)
        cos_t, sin_t = rope_tables(seq, hd)
        ctx = attention(q, k, v, cos_t, sin_t, hd)
        ctx_peer = over_tp(ctx)

        cap_src = n_exp * (3 * seq * top_k // (2 * n_all))
        y_all = run_experts(n, loc, dst, rank_t, (u_half, u_x, u_c, u_d), exp_gate, exp_up, exp_down, cap_src, ctx)

        quarters = my_ep ^ jnp.arange(4, dtype=jnp.int32)
        after, f_norm = run_out(quarters, x2, ffn_gain, ctx, ctx_peer, w_o, (w_q0, w_q2, w_q1, w_q3), y_all)
        f_far = run_ffn(1 - my_tp, half, f_norm, w_gate, w_up, w_down, after, n_out=2)
        f_got = []
        for c in range(2):
            f_got.append(over_tp(f_far[c]))

        got3, m_x = [], []
        tie = f_far[0]
        for p in range(2):
            m3, = run_combine(3, rows, pos, gates_all, y_all, tie, part=(p, 2))
            tie = m3
            got3.append(over_core(m3))
        for p in range(2):
            m1 = run_combine(1, rows, pos, gates_all, y_all, tie, init=got3[p], n_out=CHUNKS // 2, part=(p, 2))
            tie = m1[0]
            for k in range(CHUNKS // 2):
                m_x.append(over_x(m1[k]))

        s_own, = run_ffn(my_tp, half, f_norm, w_gate, w_up, w_down, tie, adds=((after, None),))
        own, peer = [], []
        tie = s_own
        per = CHUNKS // 2
        for p in range(2):
            m2, = run_combine(2, rows, pos, gates_all, y_all, tie, part=(p, 2))
            got2 = over_core(m2)
            m0, = run_combine(0, rows, pos, gates_all, y_all, m2, part=(p, 2))
            tie = m0
            for k in range(per):
                c = p * per + k
                o_c = run_final(((s_own, c), (f_got[p], k), (m0, k), (got2, k), (m_x[c], 0)))
                tie = o_c
                own.append(o_c)
                peer.append(over_tp(o_c))
        first = my_tp == 0
        out = jnp.concatenate([jnp.where(first, a, b) for a, b in zip(own, peer)] + [jnp.where(first, b, a) for a, b in zip(own, peer)], axis=0)
        return out.reshape(1, seq, d)

    return jax.shard_map(layer, mesh=mesh, in_specs=in_specs, out_specs=tok_spec, check_vma=False)
```

```python
import functools
import jax
import jax.numpy as jnp
import numpy as np
from jax import lax
from jax.experimental import pallas as pl
from jax.experimental.pallas import tpu as pltpu
from jax.sharding import PartitionSpec as P

EPS = 1e-6
ROPE_BASE = 10000.0
F32 = jnp.float32
BF16 = jnp.bfloat16
SEG = 16
GT = 128
OUT = 96
CHUNKS = 4
CT = 256
VMEM_BIG = 67_000_000


def inv_rms_of(x_f32):
    return lax.rsqrt(jnp.mean(x_f32 * x_f32, axis=-1, keepdims=True) + EPS)


def scaled(x_val, inv, gain):
    return (x_val.astype(F32) * inv * gain.astype(F32)).astype(BF16)


def rope_tables(seq_len, head_dim):
    inv_freq = (np.float32(ROPE_BASE) ** (-np.arange(head_dim // 2, dtype=np.float32) * np.float32(2.0 / head_dim))).astype(np.float32)
    angle = (np.arange(seq_len, dtype=np.float32)[:, None] * inv_freq[None, :]).astype(np.float64)
    cos_tab, sin_tab = np.cos(angle).astype(np.float32), np.sin(angle).astype(np.float32)
    return np.concatenate([cos_tab, cos_tab], axis=1), np.concatenate([-sin_tab, sin_tab], axis=1)


def attn_kernel(q_ref, k_ref, v_ref, cos_ref, sin_ref, o_ref, k_scr, *bufs):
    seq, hd = cos_ref.shape
    blk, strip = 256, 32
    factor = hd ** -0.5 * 1.4426950408889634
    pair = q_ref.shape[1] // hd
    for h in range(pair):
        hc = slice(h * hd, (h + 1) * hd)
        k_f = k_ref[:, hc]
        k_scr[:, hc] = (k_f * cos_ref[...] + pltpu.roll(k_f, hd // 2, 1) * sin_ref[...]).astype(BF16)
    r_id = lax.broadcasted_iota(jnp.int32, (strip, blk), 0)
    c_id = lax.broadcasted_iota(jnp.int32, (strip, blk), 1)
    for i in range(seq // blk):
        rows = slice(i * blk, (i + 1) * blk)
        kv = (i + 1) * blk
        for h in range(pair):
            s_scr, p_scr = bufs[2 * h], bufs[2 * h + 1]
            hc = slice(h * hd, (h + 1) * hd)
            q_f = q_ref[rows, hc]
            q_b = (q_f * cos_ref[rows] + pltpu.roll(q_f, hd // 2, 1) * sin_ref[rows]).astype(BF16)
            s_scr[:, :kv] = lax.dot_general(q_b, k_scr[:kv, hc], (((1,), (1,)), ((), ())), preferred_element_type=F32)
        for h in range(pair):
            s_scr, p_scr = bufs[2 * h], bufs[2 * h + 1]
            for t in range(blk // strip):
                sr = slice(t * strip, (t + 1) * strip)
                last = jnp.where(r_id + t * strip >= c_id, s_scr[sr, kv - blk:kv], -1e30)
                s = last if i == 0 else jnp.concatenate([s_scr[sr, :kv - blk], last], axis=1)
                p = jnp.exp2((s - jnp.max(s, axis=1, keepdims=True)) * factor)
                p_scr[sr, :kv] = (p * (1.0 / jnp.sum(p, axis=1, keepdims=True))).astype(BF16)
        for h in range(pair):
            s_scr, p_scr = bufs[2 * h], bufs[2 * h + 1]
            hc = slice(h * hd, (h + 1) * hd)
            o_ref[rows, hc] = jnp.dot(p_scr[:, :kv], v_ref[:kv, hc], preferred_element_type=F32).astype(BF16)


def attention(q, k, v, cos_t, sin_t, head_dim):
    seq, width = q.shape
    pair = 2
    steps = width // (pair * head_dim)
    col = pl.BlockSpec((seq, pair * head_dim), lambda h: (0, h))
    tab = pl.BlockSpec((seq, head_dim), lambda h: (0, 0))
    return pl.pallas_call(
        attn_kernel, grid=(steps,),
        in_specs=[col, col, col, tab, tab], out_specs=col,
        out_shape=jax.ShapeDtypeStruct((seq, width), BF16),
        scratch_shapes=[pltpu.VMEM((seq, pair * head_dim), BF16)] + [pltpu.VMEM((256, seq), F32), pltpu.VMEM((256, seq), BF16)] * pair,
        compiler_params=pltpu.CompilerParams(vmem_limit_bytes=VMEM_BIG),
        cost_estimate=pl.CostEstimate(flops=width * seq * seq * 4, bytes_accessed=12 * seq * width, transcendentals=0),
        name="attn",
    )(q, k, v, cos_t, sin_t)


def expert_kernel(n_ref, loc_ref, dst_ref, rank_ref, u0_ref, u1_ref, u2_ref, u3_ref, wg_ref, wu_ref, wd_ref, _after, y_hbm, x_scr, h_scr, y_scr, sem):
    e = pl.program_id(0)
    u_refs = (u0_ref, u1_ref, u2_ref, u3_ref)
    half, d = u0_ref.shape
    fe = wg_ref.shape[2]

    def gather(s, i):
        rid = lax.broadcasted_iota(jnp.int32, (GT, half), 0) + i * GT
        hot = (rank_ref[s, 0] == rid).astype(F32).astype(BF16)
        x_scr[pl.ds(pl.multiple_of(loc_ref[s, e] + i * GT, SEG), GT), :] = jnp.dot(hot, u_refs[s][...], preferred_element_type=F32).astype(BF16)

    for s in range(4):
        @pl.when(n_ref[s, e] > GT)
        def _():
            gather(s, 1)
    for s in range(4):
        gather(s, 0)

    total = loc_ref[3, e] + lax.shift_right_logical(n_ref[3, e] + (SEG - 1), 4) * SEG

    def copies(fn, ee):
        for s in range(4):
            for i in range(2):
                @pl.when(n_ref[s, ee] > i * OUT)
                def _():
                    fn(pltpu.make_async_copy(
                        y_scr.at[pl.ds(pl.multiple_of(loc_ref[s, ee] + i * OUT, SEG), OUT), :],
                        y_hbm.at[s, pl.ds(pl.multiple_of(dst_ref[s, ee] + i * OUT, SEG), OUT), :], sem))

    @pl.when(e > 0)
    def _():
        copies(lambda c: c.wait(), e - 1)

    def ffn(m0, rows):
        for c in range(fe // 512):
            cols = slice(c * 512, (c + 1) * 512)
            x = x_scr[pl.ds(m0, rows), :]
            g = jnp.dot(x, wg_ref[0, :, cols], preferred_element_type=F32)
            v = jnp.dot(x, wu_ref[0, :, cols], preferred_element_type=F32)
            h_scr[pl.ds(0, rows), cols] = (g * jax.nn.sigmoid(g) * v).astype(BF16)
        for c in range(d // 1024):
            cols = slice(c * 1024, (c + 1) * 1024)
            y_scr[pl.ds(m0, rows), cols] = jnp.dot(h_scr[pl.ds(0, rows), :], wd_ref[0, :, cols], preferred_element_type=F32).astype(BF16)

    for lo, hi in ((256, 288), (288, 320), (320, 352), (352, 384)):
        @pl.when((total > lo) & (total <= hi))
        def _():
            ffn(0, hi)

    @pl.when((total <= 256) | (total > 384))
    def _():
        def body(i, carry):
            ffn(pl.multiple_of(i * 256, 256), 256)
            return carry

        lax.fori_loop(0, lax.shift_right_logical(total + 255, 8), body, 0)

    copies(lambda c: c.start(), e)

    @pl.when(e == pl.num_programs(0) - 1)
    def _():
        copies(lambda c: c.wait(), e)


def run_experts(n, loc, dst, rank_t, u_four, wg, wu, wd, cap_src, after):
    half, d = u_four[0].shape
    n_exp, _, fe = wg.shape
    whole = pl.BlockSpec((half, d), lambda e, *_: (0, 0), pipeline_mode=pl.Buffered(1))
    grid_spec = pltpu.PrefetchScalarGridSpec(
        num_scalar_prefetch=3, grid=(n_exp,),
        in_specs=[
            pl.BlockSpec((4, 1, 1, half), lambda e, *_: (0, e, 0, 0)),
            whole, whole, whole, whole,
            pl.BlockSpec((1, d, fe), lambda e, *_: (e, 0, 0)),
            pl.BlockSpec((1, d, fe), lambda e, *_: (e, 0, 0)),
            pl.BlockSpec((1, fe, d), lambda e, *_: (e, 0, 0)),
            pl.BlockSpec(memory_space=pl.ANY),
        ],
        out_specs=pl.BlockSpec(memory_space=pl.ANY),
        scratch_shapes=[pltpu.VMEM((1024, d), BF16), pltpu.VMEM((384, fe), BF16), pltpu.VMEM((1024, d), BF16), pltpu.SemaphoreType.DMA],
    )
    return pl.pallas_call(
        expert_kernel, grid_spec=grid_spec,
        out_shape=jax.ShapeDtypeStruct((4, cap_src + 256, d), BF16),
        compiler_params=pltpu.CompilerParams(vmem_limit_bytes=VMEM_BIG),
        cost_estimate=pl.CostEstimate(flops=90_000_000_000, bytes_accessed=n_exp * d * fe * 6 + 40_000_000, transcendentals=0),
        name="experts",
    )(n, loc, dst, rank_t, *u_four, wg, wu, wd, after)


def combine_kernel(src, has_init, n_adds, rows_ref, pos_ref, gate_ref, y_hbm, _after, *rest):
    init_ref = rest[0] if has_init else None
    adds, rest = rest[has_init:has_init + n_adds], rest[has_init + n_adds:]
    if n_adds:
        out_ref, y_a, y_b, g_a, g_b, sems, acc = rest
        o_refs = [acc]
    else:
        *o_refs, y_a, y_b, g_a, g_b, sems = rest
    half, top_k = pos_ref.shape
    rc, d = o_refs[0].shape
    n_rows = rows_ref[src]
    n_tiles = lax.shift_right_logical(n_rows + (CT - 1), 8)

    def fetch(i, buf, k):
        return pltpu.make_async_copy(y_hbm.at[src, pl.ds(pl.multiple_of(i * CT, CT), CT), :], buf, sems.at[k])

    def start(i, buf, k):
        @pl.when(i < n_tiles)
        def _():
            fetch(i, buf, k).start()

    def arrive(i, buf, k):
        @pl.when(i < n_tiles)
        def _():
            fetch(i, buf, k).wait()

        @pl.when(i >= n_tiles - 1)
        def _():
            live = lax.broadcasted_iota(jnp.int32, (CT, 1), 0) + i * CT < n_rows
            buf[...] = jnp.where(live, buf[...].astype(F32), 0.0).astype(BF16)

    def build(i, g_scr, b):
        rid = lax.broadcasted_iota(jnp.int32, (32, CT), 1) + i * CT
        tok = slice(b * 32, (b + 1) * 32)
        pos, gate = pos_ref[tok, :], gate_ref[tok, :]
        g = jnp.zeros((32, CT), F32)
        for j in range(top_k):
            g = jnp.where(pos[:, j:j + 1] == rid, gate[:, j:j + 1], g)
        hi = g.astype(BF16)
        left = g - hi.astype(F32)
        mid = left.astype(BF16)
        g_scr[tok, :CT] = (left - mid.astype(F32)).astype(BF16)
        g_scr[tok, CT:2 * CT] = mid
        g_scr[tok, 2 * CT:] = hi

    def multiply(g_scr, buf, i_next, g_next):
        n_c = d // 512
        blocks = half // 32
        for c in range(n_c):
            cols = slice(c * 512, (c + 1) * 512)
            y = buf[:, cols]
            part = jnp.dot(g_scr[...], jnp.concatenate([y, y, y], axis=0), preferred_element_type=F32)
            for b in range(c * blocks // n_c, (c + 1) * blocks // n_c):
                build(i_next, g_next, b)
            for k, o_ref in enumerate(o_refs):
                o_ref[:, cols] += part[k * rc:(k + 1) * rc]

    start(0, y_a, 0)
    for b in range(half // 32):
        build(0, g_a, b)
    for k, o_ref in enumerate(o_refs):
        o_ref[...] = init_ref[k * rc:(k + 1) * rc, :] if has_init else jnp.zeros_like(o_ref)

    def body(p, carry):
        i = 2 * p
        start(i + 1, y_b, 1)
        arrive(i, y_a, 0)
        multiply(g_a, y_a, i + 1, g_b)

        @pl.when(i + 1 < n_tiles)
        def _():
            start(i + 2, y_a, 0)
            arrive(i + 1, y_b, 1)
            multiply(g_b, y_b, i + 2, g_a)

        return carry

    lax.fori_loop(0, lax.shift_right_logical(n_tiles + 1, 1), body, 0)

    if n_adds:
        ffn_own, ffn_got, core_got, x_got = adds
        out_ref[...] = ((ffn_own[...] + ffn_got[...]) + ((acc[...] + core_got[...]) + x_got[...])).astype(BF16)


def run_combine(src, rows, pos, gates, y_all, after, init=None, n_out=1, part=(0, 1), adds=()):
    d = y_all.shape[2]
    half, top_k = pos.shape[1] // part[1], pos.shape[2]
    small = pl.BlockSpec((half, top_k), lambda i, r: (part[0], 0))
    anywhere = pl.BlockSpec(memory_space=pl.ANY)
    extra = [] if init is None else [init]
    grid_spec = pltpu.PrefetchScalarGridSpec(
        num_scalar_prefetch=1, grid=(1,),
        in_specs=[small, small, anywhere, anywhere] + [pl.BlockSpec((half, d), lambda i, r: (0, 0)) for _ in extra]
        + [pl.BlockSpec((half, d), lambda i, r, b=b: (b, 0)) for _, b in adds],
        out_specs=[pl.BlockSpec((half // n_out, d), lambda i, r: (0, 0))] * n_out,
        scratch_shapes=[pltpu.VMEM((CT, d), BF16)] * 2 + [pltpu.VMEM((half, 3 * CT), BF16)] * 2 + [pltpu.SemaphoreType.DMA((2,))]
        + ([pltpu.VMEM((half, d), F32)] if adds else []),
    )
    return pl.pallas_call(
        functools.partial(combine_kernel, src, int(init is not None), len(adds)), grid_spec=grid_spec,
        out_shape=[jax.ShapeDtypeStruct((half // n_out, d), BF16 if adds else F32)] * n_out,
        compiler_params=pltpu.CompilerParams(vmem_limit_bytes=VMEM_BIG),
        cost_estimate=pl.CostEstimate(flops=12_000_000_000, bytes_accessed=10_000_000, transcendentals=0),
    )(rows, pos[src], gates[src], y_all, after, *extra, *[v for v, _ in adds])


def out_kernel(q_ref, x_ref, gain_ref, ctx_ref, peer_ref, wo_ref, w0_ref, w1_ref, w2_ref, w3_ref, _after, a_ref, n_ref):
    quarter = w0_ref.shape[0]
    o = jnp.dot(ctx_ref[...], wo_ref[...], preferred_element_type=F32)
    p = None
    for r, w in enumerate((w0_ref, w1_ref, w2_ref, w3_ref)):
        cols = pl.ds(pl.multiple_of(q_ref[r] * quarter, quarter), quarter)
        t = jnp.dot(peer_ref[:, cols], w[...], preferred_element_type=F32)
        p = t if p is None else p + t
    after = (x_ref[...].astype(F32) + (o + p)).astype(BF16)
    a_ref[...] = after
    a_f = after.astype(F32)
    inv = lax.rsqrt(jnp.mean(a_f * a_f, axis=1, keepdims=True) + EPS)
    n_ref[...] = (a_f * inv * gain_ref[...].astype(F32)).astype(BF16)


def run_out(quarters, x2, gain, ctx, ctx_peer, w_o, pieces, after):
    seq, d = x2.shape
    width = w_o.shape[0]
    blk = 256
    row = lambda n: pl.BlockSpec((blk, n), lambda i, q: (i, 0))
    const = lambda m, n: pl.BlockSpec((m, n), lambda i, q: (0, 0), pipeline_mode=pl.Buffered(1))
    grid_spec = pltpu.PrefetchScalarGridSpec(
        num_scalar_prefetch=1, grid=(seq // blk,),
        in_specs=[row(d), const(1, d), row(width), row(width), const(width, d)] + [const(width // 4, d)] * 4 + [pl.BlockSpec(memory_space=pl.ANY)],
        out_specs=[row(d), row(d)],
    )
    return pl.pallas_call(
        out_kernel, grid_spec=grid_spec,
        out_shape=[jax.ShapeDtypeStruct((seq, d), BF16)] * 2,
        compiler_params=pltpu.CompilerParams(vmem_limit_bytes=VMEM_BIG),
        cost_estimate=pl.CostEstimate(flops=10_000_000_000, bytes_accessed=24_000_000, transcendentals=0),
        name="out_proj",
    )(quarters, x2, gain.reshape(1, d), ctx, ctx_peer, w_o, *pieces, after)


def ffn_kernel(n_up, n_add, off_ref, x_ref, wg_ref, wu_ref, wd_ref, _after, *rest):
    adds, (*o_refs, h_scr) = rest[:n_add], rest[n_add:]
    i = pl.program_id(0)
    blk = wg_ref.shape[1]

    @pl.when(i < n_up)
    def _():
        x = x_ref[...]
        g = jnp.dot(x, wg_ref[...], preferred_element_type=F32)
        u = jnp.dot(x, wu_ref[...], preferred_element_type=F32)
        h_scr[:, pl.ds(pl.multiple_of(i * blk, blk), blk)] = (g * jax.nn.sigmoid(g) * u).astype(BF16)

    @pl.when(i >= n_up)
    def _():
        v = jnp.dot(h_scr[...], wd_ref[...], preferred_element_type=F32)
        for r in adds:
            v = r[...].astype(F32) + v
        rows = v.shape[0] // len(o_refs)
        for k, o_ref in enumerate(o_refs):
            o_ref[...] = v[k * rows:(k + 1) * rows]


def run_ffn(which, rows, f_norm, wg, wu, wd, after, adds=(), n_out=1):
    d, ff = wg.shape
    blk, out_blk = 512, 512
    n_up, n_down = ff // blk, d // out_blk
    down = lambda i: jnp.maximum(i - n_up, 0)
    up = lambda i: jnp.minimum(i, n_up - 1)
    add_specs = [
        pl.BlockSpec((rows, out_blk), (lambda i, w: (w[0], down(i))) if at is None else (lambda i, w, at=at: (at, down(i))))
        for _, at in adds]
    grid_spec = pltpu.PrefetchScalarGridSpec(
        num_scalar_prefetch=1, grid=(n_up + n_down,),
        in_specs=[pl.BlockSpec((rows, d), lambda i, w: (w[0], 0), pipeline_mode=pl.Buffered(1)),
                  pl.BlockSpec((d, blk), lambda i, w: (0, up(i))), pl.BlockSpec((d, blk), lambda i, w: (0, up(i))),
                  pl.BlockSpec((ff, out_blk), lambda i, w: (0, down(i))), pl.BlockSpec(memory_space=pl.ANY)] + add_specs,
        out_specs=[pl.BlockSpec((rows // n_out, out_blk), lambda i, w: (0, down(i)))] * n_out,
        scratch_shapes=[pltpu.VMEM((rows, ff), BF16)],
    )
    return pl.pallas_call(
        functools.partial(ffn_kernel, n_up, len(adds)), grid_spec=grid_spec,
        out_shape=[jax.ShapeDtypeStruct((rows // n_out, d), F32)] * n_out,
        compiler_params=pltpu.CompilerParams(vmem_limit_bytes=VMEM_BIG),
        cost_estimate=pl.CostEstimate(flops=rows * 56_000_000, bytes_accessed=60_000_000, transcendentals=0),
        name="ffn",
    )(which.reshape(1), f_norm, wg, wu, wd, after, *[v for v, _ in adds])


def place_kernel(n, _dest, *refs):
    i = pl.program_id(0)
    for k in range(n):
        @pl.when(i == k)
        def _():
            refs[-1][...] = refs[k][...]


def run_place(dest, pieces, seq, buf=None):
    rows, d = pieces[0].shape
    n = len(pieces)
    extra = [] if buf is None else [buf]
    grid_spec = pltpu.PrefetchScalarGridSpec(
        num_scalar_prefetch=1, grid=(n,),
        in_specs=[pl.BlockSpec((rows, d), lambda i, t: (0, 0), pipeline_mode=pl.Buffered(1))] * n + [pl.BlockSpec(memory_space=pl.ANY) for _ in extra],
        out_specs=pl.BlockSpec((rows, d), lambda i, t: (t[i], 0)),
    )
    return pl.pallas_call(
        functools.partial(place_kernel, n), grid_spec=grid_spec,
        out_shape=jax.ShapeDtypeStruct((seq, d), BF16),
        input_output_aliases={n + 1: 0} if extra else {},
        compiler_params=pltpu.CompilerParams(vmem_limit_bytes=VMEM_BIG),
        cost_estimate=pl.CostEstimate(flops=n * rows * d, bytes_accessed=4 * n * rows * d, transcendentals=0),
        name="place",
    )(dest, *pieces, *extra)


def solution(mesh):
    tok_spec = P(('dp', 'ep'), None, None)
    col_spec = P(None, 'tp', None)
    exp_spec = P('ep', None, None)
    in_specs = (tok_spec, tok_spec, tok_spec, P(None), col_spec, col_spec, col_spec, P('tp', None, None), P(None), P(None, 'tp'), P(None, 'tp'), P('tp', None), P(None), P(None, None), exp_spec, exp_spec, exp_spec)
    n_ep, n_tp = mesh.shape['ep'], mesh.shape['tp']
    assert n_ep == 4 and n_tp == 2

    def over_x(v):
        return lax.ppermute(v, 'ep', [(i, i ^ 2) for i in range(4)])

    def over_core(v):
        return lax.ppermute(v, 'ep', [(i, i ^ 1) for i in range(4)])

    def over_tp(v):
        return lax.ppermute(v, 'tp', [(0, 1), (1, 0)])

    def layer(hidden_in, expert_ids, slot_ids, attn_gain, w_query, w_key, w_value, w_out, ffn_gain, w_gate, w_up, w_down, moe_gain, w_router, exp_gate, exp_up, exp_down):
        seq, d = hidden_in.shape[1:]
        top_k = expert_ids.shape[2]
        n_all = w_router.shape[1]
        n_exp = exp_gate.shape[0]
        half = seq // 2
        my_tp = lax.axis_index('tp')
        my_ep = lax.axis_index('ep')
        x2 = hidden_in.reshape(seq, d)
        ids = expert_ids.reshape(seq, top_k)

        width = w_out.shape[0] * w_out.shape[1]
        w_o = w_out.reshape(width, d)
        quarter = width // 4
        w_q0 = over_tp(lax.dynamic_slice(w_o, (my_ep * quarter, 0), (quarter, d)))

        inv_rms = inv_rms_of(x2.astype(F32))
        x_half = lax.dynamic_slice(x2, (my_tp * half, 0), (half, d))
        inv_half = lax.dynamic_slice(inv_rms, (my_tp * half, 0), (half, 1))
        ids_half = lax.dynamic_slice(ids, (my_tp * half, 0), (half, top_k))
        u_half = scaled(x_half, inv_half, moe_gain)
        u_c = over_core(u_half)
        logits = jnp.dot(u_half, w_router, preferred_element_type=F32)
        is_e = ids_half[:, :, None] == jnp.arange(n_all, dtype=jnp.int32)[None, None, :]
        picked = jnp.sum(jnp.where(is_e, logits[:, None, :], 0.0), axis=2)
        gates = jax.nn.softmax(picked, axis=-1)
        meta = jnp.concatenate([ids_half.astype(F32), gates], axis=1)
        meta_x = over_x(meta)
        u_x = over_x(u_half)
        meta2 = jnp.stack([meta, meta_x])
        meta_c = over_core(meta2)
        meta_all = jnp.concatenate([meta2, meta_c])
        u_d = over_core(u_x)
        w_q1 = over_x(w_q0)
        w_q2 = over_core(w_q0)
        w_q3 = over_core(w_q1)

        ids_loc = meta_all[:, :, :top_k].astype(jnp.int32) - my_ep * n_exp
        gates_all = meta_all[:, :, top_k:]
        ids_t = jnp.swapaxes(ids_loc, 1, 2)
        e_ids = jnp.arange(n_exp, dtype=jnp.int32)
        sel_t = jnp.any(ids_t[:, None, :, :] == e_ids[None, :, None, None], axis=2)
        before = (jnp.arange(half)[:, None] < jnp.arange(half)[None, :]).astype(BF16)
        rank_f = jnp.dot(sel_t.reshape(-1, half).astype(BF16), before, preferred_element_type=F32).reshape(4, n_exp, half)
        n = jnp.sum(sel_t.astype(jnp.int32), axis=2)
        seg = (n + SEG - 1) // SEG * SEG
        lower4 = jnp.arange(4)[:, None] > jnp.arange(4)[None, :]
        loc = jnp.sum(jnp.where(lower4[:, :, None], seg[None], 0), axis=1)
        lower_e = jnp.arange(n_exp)[:, None] > jnp.arange(n_exp)[None, :]
        dst = jnp.sum(jnp.where(lower_e[None], seg[:, None, :], 0), axis=2)
        rows = jnp.sum(seg, axis=1)
        rank_i = rank_f.astype(jnp.int32)
        rank_t = jnp.where(sel_t, rank_i, -1)[:, :, None, :]
        pos_e = jnp.swapaxes(rank_i + dst[:, :, None], 1, 2)
        hit = ids_loc[..., None] == e_ids
        pos = jnp.sum(jnp.where(hit, pos_e[:, :, None, :] + 1, 0), axis=3) - 1

        x_norm = scaled(x2, inv_rms, attn_gain)
        hd = w_query.shape[2]
        q = jnp.dot(x_norm, w_query.reshape(d, width), preferred_element_type=F32)
        k = jnp.dot(x_norm, w_key.reshape(d, width), preferred_element_type=F32)
        v = jnp.dot(x_norm, w_value.reshape(d, width), preferred_element_type=F32).astype(BF16)
        cos_t, sin_t = rope_tables(seq, hd)
        ctx = attention(q, k, v, cos_t, sin_t, hd)
        ctx_peer = over_tp(ctx)

        cap_src = n_exp * (3 * seq * top_k // (2 * n_all))
        y_all = run_experts(n, loc, dst, rank_t, (u_half, u_x, u_c, u_d), exp_gate, exp_up, exp_down, cap_src, ctx)

        quarters = my_ep ^ jnp.arange(4, dtype=jnp.int32)
        after, f_norm = run_out(quarters, x2, ffn_gain, ctx, ctx_peer, w_o, (w_q0, w_q2, w_q1, w_q3), y_all)
        f_far = run_ffn(1 - my_tp, half, f_norm, w_gate, w_up, w_down, after, n_out=2)
        f_got = []
        for c in range(2):
            f_got.append(over_tp(f_far[c]))

        got3, m_x = [], []
        tie = f_far[0]
        for p in range(2):
            m3, = run_combine(3, rows, pos, gates_all, y_all, tie, part=(p, 2))
            tie = m3
            got3.append(over_core(m3))
        for p in range(2):
            m1 = run_combine(1, rows, pos, gates_all, y_all, tie, init=got3[p], n_out=CHUNKS // 2, part=(p, 2))
            tie = m1[0]
            for k in range(CHUNKS // 2):
                m_x.append(over_x(m1[k]))

        s_own, = run_ffn(my_tp, half, f_norm, w_gate, w_up, w_down, tie, adds=((after, None),))
        own, peer, got2 = [], [], []
        tie = s_own
        per = CHUNKS // 2
        for p in range(2):
            tie, = run_combine(2, rows, pos, gates_all, y_all, tie, part=(p, 2))
            got2.append(over_core(tie))
        for c in range(CHUNKS):
            p, k = c // per, c % per
            tie, = run_combine(0, rows, pos, gates_all, y_all, tie, part=(c, CHUNKS),
                               adds=((s_own, c), (f_got[p], k), (got2[p], k), (m_x[c], 0)))
            own.append(tie)
            peer.append(over_tp(tie))
        mine, other = my_tp * CHUNKS, (1 - my_tp) * CHUNKS
        dest = jnp.stack([mine + c for c in range(CHUNKS)] + [other + c for c in range(CHUNKS)]).astype(jnp.int32)
        out = run_place(dest[:-1], own + peer[:-1], seq)
        out = run_place(dest[-1:], peer[-1:], seq, out)
        return out.reshape(1, seq, d)

    return jax.shard_map(layer, mesh=mesh, in_specs=in_specs, out_specs=tok_spec, check_vma=False)
```

```python
import functools
import jax
import jax.numpy as jnp
import numpy as np
from jax import lax
from jax.experimental import pallas as pl
from jax.experimental.pallas import tpu as pltpu
from jax.sharding import PartitionSpec as P

EPS = 1e-6
ROPE_BASE = 10000.0
F32 = jnp.float32
BF16 = jnp.bfloat16
SEG = 16
GT = 128
OUT = 96
CHUNKS = 2
CT = 256
VMEM_BIG = 60 * 1024 * 1024


def inv_rms_of(x_f32):
    return lax.rsqrt(jnp.mean(x_f32 * x_f32, axis=-1, keepdims=True) + EPS)


def scaled(x_val, inv, gain):
    return (x_val.astype(F32) * inv * gain.astype(F32)).astype(BF16)


def rope_tables(seq_len, head_dim):
    inv_freq = (np.float32(ROPE_BASE) ** (-np.arange(head_dim // 2, dtype=np.float32) * np.float32(2.0 / head_dim))).astype(np.float32)
    angle = (np.arange(seq_len, dtype=np.float32)[:, None] * inv_freq[None, :]).astype(np.float64)
    cos_tab, sin_tab = np.cos(angle).astype(np.float32), np.sin(angle).astype(np.float32)
    return np.concatenate([cos_tab, cos_tab], axis=1), np.concatenate([-sin_tab, sin_tab], axis=1)


def attn_kernel(q_ref, k_ref, v_ref, cos_ref, sin_ref, o_ref, k_scr, *bufs):
    seq, hd = cos_ref.shape
    blk, strip = 256, 32
    factor = hd ** -0.5 * 1.4426950408889634
    pair = q_ref.shape[1] // hd
    for h in range(pair):
        hc = slice(h * hd, (h + 1) * hd)
        k_f = k_ref[:, hc]
        k_scr[:, hc] = (k_f * cos_ref[...] + pltpu.roll(k_f, hd // 2, 1) * sin_ref[...]).astype(BF16)
    r_id = lax.broadcasted_iota(jnp.int32, (strip, blk), 0)
    c_id = lax.broadcasted_iota(jnp.int32, (strip, blk), 1)
    for i in range(seq // blk):
        rows = slice(i * blk, (i + 1) * blk)
        kv = (i + 1) * blk
        for h in range(pair):
            s_scr, p_scr = bufs[2 * h], bufs[2 * h + 1]
            hc = slice(h * hd, (h + 1) * hd)
            q_f = q_ref[rows, hc]
            q_b = (q_f * cos_ref[rows] + pltpu.roll(q_f, hd // 2, 1) * sin_ref[rows]).astype(BF16)
            s_scr[:, :kv] = lax.dot_general(q_b, k_scr[:kv, hc], (((1,), (1,)), ((), ())), preferred_element_type=F32)
        for h in range(pair):
            s_scr, p_scr = bufs[2 * h], bufs[2 * h + 1]
            for t in range(blk // strip):
                sr = slice(t * strip, (t + 1) * strip)
                last = jnp.where(r_id + t * strip >= c_id, s_scr[sr, kv - blk:kv], -1e30)
                s = last if i == 0 else jnp.concatenate([s_scr[sr, :kv - blk], last], axis=1)
                p = jnp.exp2((s - jnp.max(s, axis=1, keepdims=True)) * factor)
                p_scr[sr, :kv] = (p * (1.0 / jnp.sum(p, axis=1, keepdims=True))).astype(BF16)
        for h in range(pair):
            s_scr, p_scr = bufs[2 * h], bufs[2 * h + 1]
            hc = slice(h * hd, (h + 1) * hd)
            o_ref[rows, hc] = jnp.dot(p_scr[:, :kv], v_ref[:kv, hc], preferred_element_type=F32).astype(BF16)


def attention(q, k, v, cos_t, sin_t, head_dim):
    seq, width = q.shape
    pair = 2
    steps = width // (pair * head_dim)
    col = pl.BlockSpec((seq, pair * head_dim), lambda h: (0, h))
    tab = pl.BlockSpec((seq, head_dim), lambda h: (0, 0))
    return pl.pallas_call(
        attn_kernel, grid=(steps,),
        in_specs=[col, col, col, tab, tab], out_specs=col,
        out_shape=jax.ShapeDtypeStruct((seq, width), BF16),
        scratch_shapes=[pltpu.VMEM((seq, pair * head_dim), BF16)] + [pltpu.VMEM((256, seq), F32), pltpu.VMEM((256, seq), BF16)] * pair,
        cost_estimate=pl.CostEstimate(flops=width * seq * seq * 4, bytes_accessed=12 * seq * width, transcendentals=0),
        name="attn",
    )(q, k, v, cos_t, sin_t)


def expert_kernel(n_ref, loc_ref, dst_ref, rank_ref, u0_ref, u1_ref, u2_ref, u3_ref, wg_ref, wu_ref, wd_ref, _after, y_hbm, x_scr, h_scr, y_scr, sem):
    e = pl.program_id(0)
    u_refs = (u0_ref, u1_ref, u2_ref, u3_ref)
    half, d = u0_ref.shape
    fe = wg_ref.shape[2]

    def gather(s, i):
        rid = lax.broadcasted_iota(jnp.int32, (GT, half), 0) + i * GT
        hot = (rank_ref[s, 0] == rid).astype(F32).astype(BF16)
        x_scr[pl.ds(pl.multiple_of(loc_ref[s, e] + i * GT, SEG), GT), :] = jnp.dot(hot, u_refs[s][...], preferred_element_type=F32).astype(BF16)

    for s in range(4):
        @pl.when(n_ref[s, e] > GT)
        def _():
            gather(s, 1)
    for s in range(4):
        gather(s, 0)

    total = loc_ref[3, e] + lax.shift_right_logical(n_ref[3, e] + (SEG - 1), 4) * SEG

    def copies(fn, ee):
        for s in range(4):
            for i in range(2):
                @pl.when(n_ref[s, ee] > i * OUT)
                def _():
                    fn(pltpu.make_async_copy(
                        y_scr.at[pl.ds(pl.multiple_of(loc_ref[s, ee] + i * OUT, SEG), OUT), :],
                        y_hbm.at[s, pl.ds(pl.multiple_of(dst_ref[s, ee] + i * OUT, SEG), OUT), :], sem))

    @pl.when(e > 0)
    def _():
        copies(lambda c: c.wait(), e - 1)

    def ffn(m0, rows):
        for c in range(fe // 512):
            cols = slice(c * 512, (c + 1) * 512)
            x = x_scr[pl.ds(m0, rows), :]
            g = jnp.dot(x, wg_ref[0, :, cols], preferred_element_type=F32)
            v = jnp.dot(x, wu_ref[0, :, cols], preferred_element_type=F32)
            h_scr[pl.ds(0, rows), cols] = (g * jax.nn.sigmoid(g) * v).astype(BF16)
        for c in range(d // 1024):
            cols = slice(c * 1024, (c + 1) * 1024)
            y_scr[pl.ds(m0, rows), cols] = jnp.dot(h_scr[pl.ds(0, rows), :], wd_ref[0, :, cols], preferred_element_type=F32).astype(BF16)

    for lo, hi in ((256, 288), (288, 320), (320, 352), (352, 384)):
        @pl.when((total > lo) & (total <= hi))
        def _():
            ffn(0, hi)

    @pl.when((total <= 256) | (total > 384))
    def _():
        def body(i, carry):
            ffn(pl.multiple_of(i * 256, 256), 256)
            return carry

        lax.fori_loop(0, lax.shift_right_logical(total + 255, 8), body, 0)

    copies(lambda c: c.start(), e)

    @pl.when(e == pl.num_programs(0) - 1)
    def _():
        copies(lambda c: c.wait(), e)


def run_experts(n, loc, dst, rank_t, u_four, wg, wu, wd, cap_src, after):
    half, d = u_four[0].shape
    n_exp, _, fe = wg.shape
    whole = pl.BlockSpec((half, d), lambda e, *_: (0, 0), pipeline_mode=pl.Buffered(1))
    grid_spec = pltpu.PrefetchScalarGridSpec(
        num_scalar_prefetch=3, grid=(n_exp,),
        in_specs=[
            pl.BlockSpec((4, 1, 1, half), lambda e, *_: (0, e, 0, 0)),
            whole, whole, whole, whole,
            pl.BlockSpec((1, d, fe), lambda e, *_: (e, 0, 0)),
            pl.BlockSpec((1, d, fe), lambda e, *_: (e, 0, 0)),
            pl.BlockSpec((1, fe, d), lambda e, *_: (e, 0, 0)),
            pl.BlockSpec(memory_space=pl.ANY),
        ],
        out_specs=pl.BlockSpec(memory_space=pl.ANY),
        scratch_shapes=[pltpu.VMEM((1024, d), BF16), pltpu.VMEM((384, fe), BF16), pltpu.VMEM((1024, d), BF16), pltpu.SemaphoreType.DMA],
    )
    return pl.pallas_call(
        expert_kernel, grid_spec=grid_spec,
        out_shape=jax.ShapeDtypeStruct((4, cap_src + 256, d), BF16),
        compiler_params=pltpu.CompilerParams(vmem_limit_bytes=VMEM_BIG),
        cost_estimate=pl.CostEstimate(flops=90_000_000_000, bytes_accessed=n_exp * d * fe * 6 + 40_000_000, transcendentals=0),
        name="experts",
    )(n, loc, dst, rank_t, *u_four, wg, wu, wd, after)


def combine_kernel(src, has_init, n_adds, rows_ref, pos_ref, gate_ref, y_hbm, _after, *rest):
    init_ref = rest[0] if has_init else None
    adds, rest = rest[has_init:has_init + n_adds], rest[has_init + n_adds:]
    if n_adds:
        out_ref, y_a, y_b, g_a, g_b, sems, acc = rest
        o_refs = [acc]
    else:
        *o_refs, y_a, y_b, g_a, g_b, sems = rest
    half, top_k = pos_ref.shape
    rc, d = o_refs[0].shape
    n_rows = rows_ref[src]
    n_tiles = lax.shift_right_logical(n_rows + (CT - 1), 8)

    def fetch(i, buf, k):
        return pltpu.make_async_copy(y_hbm.at[src, pl.ds(pl.multiple_of(i * CT, CT), CT), :], buf, sems.at[k])

    def start(i, buf, k):
        @pl.when(i < n_tiles)
        def _():
            fetch(i, buf, k).start()

    def arrive(i, buf, k):
        @pl.when(i < n_tiles)
        def _():
            fetch(i, buf, k).wait()

        @pl.when(i >= n_tiles - 1)
        def _():
            live = lax.broadcasted_iota(jnp.int32, (CT, 1), 0) + i * CT < n_rows
            buf[...] = jnp.where(live, buf[...].astype(F32), 0.0).astype(BF16)

    def build(i, g_scr, b):
        rid = lax.broadcasted_iota(jnp.int32, (32, CT), 1) + i * CT
        tok = slice(b * 32, (b + 1) * 32)
        pos, gate = pos_ref[tok, :], gate_ref[tok, :]
        g = jnp.zeros((32, CT), F32)
        for j in range(top_k):
            g = jnp.where(pos[:, j:j + 1] == rid, gate[:, j:j + 1], g)
        hi = g.astype(BF16)
        left = g - hi.astype(F32)
        mid = left.astype(BF16)
        g_scr[tok, :CT] = (left - mid.astype(F32)).astype(BF16)
        g_scr[tok, CT:2 * CT] = mid
        g_scr[tok, 2 * CT:] = hi

    def multiply(g_scr, buf, i_next, g_next):
        n_c = d // 512
        blocks = half // 32
        for c in range(n_c):
            cols = slice(c * 512, (c + 1) * 512)
            y = buf[:, cols]
            part = jnp.dot(g_scr[...], jnp.concatenate([y, y, y], axis=0), preferred_element_type=F32)
            for b in range(c * blocks // n_c, (c + 1) * blocks // n_c):
                build(i_next, g_next, b)
            for k, o_ref in enumerate(o_refs):
                o_ref[:, cols] += part[k * rc:(k + 1) * rc]

    start(0, y_a, 0)
    for b in range(half // 32):
        build(0, g_a, b)
    for k, o_ref in enumerate(o_refs):
        o_ref[...] = init_ref[k * rc:(k + 1) * rc, :] if has_init else jnp.zeros_like(o_ref)

    def body(p, carry):
        i = 2 * p
        start(i + 1, y_b, 1)
        arrive(i, y_a, 0)
        multiply(g_a, y_a, i + 1, g_b)

        @pl.when(i + 1 < n_tiles)
        def _():
            start(i + 2, y_a, 0)
            arrive(i + 1, y_b, 1)
            multiply(g_b, y_b, i + 2, g_a)

        return carry

    lax.fori_loop(0, lax.shift_right_logical(n_tiles + 1, 1), body, 0)

    if n_adds:
        ffn_own, ffn_got, core_got, x_got = adds
        out_ref[...] = ((ffn_own[...] + ffn_got[...]) + ((acc[...] + core_got[...]) + x_got[...])).astype(BF16)


def run_combine(src, rows, pos, gates, y_all, after, init=None, n_out=1, part=(0, 1), adds=()):
    d = y_all.shape[2]
    half, top_k = pos.shape[1] // part[1], pos.shape[2]
    small = pl.BlockSpec((half, top_k), lambda i, r: (part[0], 0))
    anywhere = pl.BlockSpec(memory_space=pl.ANY)
    extra = [] if init is None else [init]
    grid_spec = pltpu.PrefetchScalarGridSpec(
        num_scalar_prefetch=1, grid=(1,),
        in_specs=[small, small, anywhere, anywhere] + [pl.BlockSpec((half, d), lambda i, r: (0, 0)) for _ in extra]
        + [pl.BlockSpec((half, d), lambda i, r, b=b: (b, 0)) for _, b in adds],
        out_specs=[pl.BlockSpec((half // n_out, d), lambda i, r: (0, 0))] * n_out,
        scratch_shapes=[pltpu.VMEM((CT, d), BF16)] * 2 + [pltpu.VMEM((half, 3 * CT), BF16)] * 2 + [pltpu.SemaphoreType.DMA((2,))]
        + ([pltpu.VMEM((half, d), F32)] if adds else []),
    )
    return pl.pallas_call(
        functools.partial(combine_kernel, src, int(init is not None), len(adds)), grid_spec=grid_spec,
        out_shape=[jax.ShapeDtypeStruct((half // n_out, d), BF16 if adds else F32)] * n_out,
        compiler_params=pltpu.CompilerParams(vmem_limit_bytes=VMEM_BIG if adds else 40 * 1024 * 1024),
        cost_estimate=pl.CostEstimate(flops=12_000_000_000, bytes_accessed=10_000_000, transcendentals=0),
    )(rows, pos[src], gates[src], y_all, after, *extra, *[v for v, _ in adds])


def out_kernel(q_ref, x_ref, gain_ref, ctx_ref, peer_ref, wo_ref, w0_ref, w1_ref, w2_ref, w3_ref, _after, a_ref, n_ref):
    quarter = w0_ref.shape[0]
    o = jnp.dot(ctx_ref[...], wo_ref[...], preferred_element_type=F32)
    p = None
    for r, w in enumerate((w0_ref, w1_ref, w2_ref, w3_ref)):
        cols = pl.ds(pl.multiple_of(q_ref[r] * quarter, quarter), quarter)
        t = jnp.dot(peer_ref[:, cols], w[...], preferred_element_type=F32)
        p = t if p is None else p + t
    after = (x_ref[...].astype(F32) + (o + p)).astype(BF16)
    a_ref[...] = after
    a_f = after.astype(F32)
    inv = lax.rsqrt(jnp.mean(a_f * a_f, axis=1, keepdims=True) + EPS)
    n_ref[...] = (a_f * inv * gain_ref[...].astype(F32)).astype(BF16)


def run_out(quarters, x2, gain, ctx, ctx_peer, w_o, pieces, after):
    seq, d = x2.shape
    width = w_o.shape[0]
    blk = 256
    row = lambda n: pl.BlockSpec((blk, n), lambda i, q: (i, 0))
    const = lambda m, n: pl.BlockSpec((m, n), lambda i, q: (0, 0), pipeline_mode=pl.Buffered(1))
    grid_spec = pltpu.PrefetchScalarGridSpec(
        num_scalar_prefetch=1, grid=(seq // blk,),
        in_specs=[row(d), const(1, d), row(width), row(width), const(width, d)] + [const(width // 4, d)] * 4 + [pl.BlockSpec(memory_space=pl.ANY)],
        out_specs=[row(d), row(d)],
    )
    return pl.pallas_call(
        out_kernel, grid_spec=grid_spec,
        out_shape=[jax.ShapeDtypeStruct((seq, d), BF16)] * 2,
        compiler_params=pltpu.CompilerParams(vmem_limit_bytes=VMEM_BIG),
        cost_estimate=pl.CostEstimate(flops=10_000_000_000, bytes_accessed=24_000_000, transcendentals=0),
        name="out_proj",
    )(quarters, x2, gain.reshape(1, d), ctx, ctx_peer, w_o, *pieces, after)


def ffn_kernel(n_up, n_add, off_ref, x_ref, wg_ref, wu_ref, wd_ref, _after, *rest):
    adds, (*o_refs, h_scr) = rest[:n_add], rest[n_add:]
    i = pl.program_id(0)
    blk = wg_ref.shape[1]

    @pl.when(i < n_up)
    def _():
        x = x_ref[...]
        g = jnp.dot(x, wg_ref[...], preferred_element_type=F32)
        u = jnp.dot(x, wu_ref[...], preferred_element_type=F32)
        h_scr[:, pl.ds(pl.multiple_of(i * blk, blk), blk)] = (g * jax.nn.sigmoid(g) * u).astype(BF16)

    @pl.when(i >= n_up)
    def _():
        v = jnp.dot(h_scr[...], wd_ref[...], preferred_element_type=F32)
        for r in adds:
            v = r[...].astype(F32) + v
        rows = v.shape[0] // len(o_refs)
        for k, o_ref in enumerate(o_refs):
            o_ref[...] = v[k * rows:(k + 1) * rows]


def run_ffn(which, rows, f_norm, wg, wu, wd, after, adds=(), n_out=1):
    d, ff = wg.shape
    blk, out_blk = 512, 512
    n_up, n_down = ff // blk, d // out_blk
    down = lambda i: jnp.maximum(i - n_up, 0)
    up = lambda i: jnp.minimum(i, n_up - 1)
    add_specs = [
        pl.BlockSpec((rows, out_blk), (lambda i, w: (w[0], down(i))) if at is None else (lambda i, w, at=at: (at, down(i))))
        for _, at in adds]
    grid_spec = pltpu.PrefetchScalarGridSpec(
        num_scalar_prefetch=1, grid=(n_up + n_down,),
        in_specs=[pl.BlockSpec((rows, d), lambda i, w: (w[0], 0), pipeline_mode=pl.Buffered(1)),
                  pl.BlockSpec((d, blk), lambda i, w: (0, up(i))), pl.BlockSpec((d, blk), lambda i, w: (0, up(i))),
                  pl.BlockSpec((ff, out_blk), lambda i, w: (0, down(i))), pl.BlockSpec(memory_space=pl.ANY)] + add_specs,
        out_specs=[pl.BlockSpec((rows // n_out, out_blk), lambda i, w: (0, down(i)))] * n_out,
        scratch_shapes=[pltpu.VMEM((rows, ff), BF16)],
    )
    return pl.pallas_call(
        functools.partial(ffn_kernel, n_up, len(adds)), grid_spec=grid_spec,
        out_shape=[jax.ShapeDtypeStruct((rows // n_out, d), F32)] * n_out,
        compiler_params=pltpu.CompilerParams(vmem_limit_bytes=VMEM_BIG),
        cost_estimate=pl.CostEstimate(flops=rows * 56_000_000, bytes_accessed=60_000_000, transcendentals=0),
        name="ffn",
    )(which.reshape(1), f_norm, wg, wu, wd, after, *[v for v, _ in adds])


def place_kernel(n, _dest, *refs):
    i = pl.program_id(0)
    for k in range(n):
        @pl.when(i == k)
        def _():
            refs[-1][...] = refs[k][...]


def run_place(dest, pieces, seq, buf=None):
    rows, d = pieces[0].shape
    n = len(pieces)
    extra = [] if buf is None else [buf]
    grid_spec = pltpu.PrefetchScalarGridSpec(
        num_scalar_prefetch=1, grid=(n,),
        in_specs=[pl.BlockSpec((rows, d), lambda i, t: (0, 0), pipeline_mode=pl.Buffered(1))] * n + [pl.BlockSpec(memory_space=pl.ANY) for _ in extra],
        out_specs=pl.BlockSpec((rows, d), lambda i, t: (t[i], 0)),
    )
    return pl.pallas_call(
        functools.partial(place_kernel, n), grid_spec=grid_spec,
        out_shape=jax.ShapeDtypeStruct((seq, d), BF16),
        input_output_aliases={n + 1: 0} if extra else {},
        compiler_params=pltpu.CompilerParams(vmem_limit_bytes=VMEM_BIG),
        cost_estimate=pl.CostEstimate(flops=n * rows * d, bytes_accessed=4 * n * rows * d, transcendentals=0),
        name="place",
    )(dest, *pieces, *extra)


def solution(mesh):
    tok_spec = P(('dp', 'ep'), None, None)
    col_spec = P(None, 'tp', None)
    exp_spec = P('ep', None, None)
    in_specs = (tok_spec, tok_spec, tok_spec, P(None), col_spec, col_spec, col_spec, P('tp', None, None), P(None), P(None, 'tp'), P(None, 'tp'), P('tp', None), P(None), P(None, None), exp_spec, exp_spec, exp_spec)
    n_ep, n_tp = mesh.shape['ep'], mesh.shape['tp']
    assert n_ep == 4 and n_tp == 2

    def over_x(v):
        return lax.ppermute(v, 'ep', [(i, i ^ 2) for i in range(4)])

    def over_core(v):
        return lax.ppermute(v, 'ep', [(i, i ^ 1) for i in range(4)])

    def over_tp(v):
        return lax.ppermute(v, 'tp', [(0, 1), (1, 0)])

    def layer(hidden_in, expert_ids, slot_ids, attn_gain, w_query, w_key, w_value, w_out, ffn_gain, w_gate, w_up, w_down, moe_gain, w_router, exp_gate, exp_up, exp_down):
        seq, d = hidden_in.shape[1:]
        top_k = expert_ids.shape[2]
        n_all = w_router.shape[1]
        n_exp = exp_gate.shape[0]
        half = seq // 2
        my_tp = lax.axis_index('tp')
        my_ep = lax.axis_index('ep')
        x2 = hidden_in.reshape(seq, d)
        ids = expert_ids.reshape(seq, top_k)

        width = w_out.shape[0] * w_out.shape[1]
        w_o = w_out.reshape(width, d)
        quarter = width // 4
        w_q0 = over_tp(lax.dynamic_slice(w_o, (my_ep * quarter, 0), (quarter, d)))

        inv_rms = inv_rms_of(x2.astype(F32))
        x_half = lax.dynamic_slice(x2, (my_tp * half, 0), (half, d))
        inv_half = lax.dynamic_slice(inv_rms, (my_tp * half, 0), (half, 1))
        ids_half = lax.dynamic_slice(ids, (my_tp * half, 0), (half, top_k))
        u_half = scaled(x_half, inv_half, moe_gain)
        u_c = over_core(u_half)
        logits = jnp.dot(u_half, w_router, preferred_element_type=F32)
        is_e = ids_half[:, :, None] == jnp.arange(n_all, dtype=jnp.int32)[None, None, :]
        picked = jnp.sum(jnp.where(is_e, logits[:, None, :], 0.0), axis=2)
        gates = jax.nn.softmax(picked, axis=-1)
        meta = jnp.concatenate([ids_half.astype(F32), gates], axis=1)
        meta_x = over_x(meta)
        u_x = over_x(u_half)
        meta2 = jnp.stack([meta, meta_x])
        meta_c = over_core(meta2)
        meta_all = jnp.concatenate([meta2, meta_c])
        u_d = over_core(u_x)
        w_q1 = over_x(w_q0)
        w_q2 = over_core(w_q0)
        w_q3 = over_core(w_q1)

        ids_loc = meta_all[:, :, :top_k].astype(jnp.int32) - my_ep * n_exp
        gates_all = meta_all[:, :, top_k:]
        ids_t = jnp.swapaxes(ids_loc, 1, 2)
        e_ids = jnp.arange(n_exp, dtype=jnp.int32)
        sel_t = jnp.any(ids_t[:, None, :, :] == e_ids[None, :, None, None], axis=2)
        before = (jnp.arange(half)[:, None] < jnp.arange(half)[None, :]).astype(BF16)
        rank_f = jnp.dot(sel_t.reshape(-1, half).astype(BF16), before, preferred_element_type=F32).reshape(4, n_exp, half)
        n = jnp.sum(sel_t.astype(jnp.int32), axis=2)
        seg = (n + SEG - 1) // SEG * SEG
        lower4 = jnp.arange(4)[:, None] > jnp.arange(4)[None, :]
        loc = jnp.sum(jnp.where(lower4[:, :, None], seg[None], 0), axis=1)
        lower_e = jnp.arange(n_exp)[:, None] > jnp.arange(n_exp)[None, :]
        dst = jnp.sum(jnp.where(lower_e[None], seg[:, None, :], 0), axis=2)
        rows = jnp.sum(seg, axis=1)
        rank_i = rank_f.astype(jnp.int32)
        rank_t = jnp.where(sel_t, rank_i, -1)[:, :, None, :]
        pos_e = jnp.swapaxes(rank_i + dst[:, :, None], 1, 2)
        hit = ids_loc[..., None] == e_ids
        pos = jnp.sum(jnp.where(hit, pos_e[:, :, None, :] + 1, 0), axis=3) - 1

        x_norm = scaled(x2, inv_rms, attn_gain)
        hd = w_query.shape[2]
        q = jnp.dot(x_norm, w_query.reshape(d, width), preferred_element_type=F32)
        k = jnp.dot(x_norm, w_key.reshape(d, width), preferred_element_type=F32)
        v = jnp.dot(x_norm, w_value.reshape(d, width), preferred_element_type=F32).astype(BF16)
        cos_t, sin_t = rope_tables(seq, hd)
        ctx = attention(q, k, v, cos_t, sin_t, hd)
        ctx_peer = over_tp(ctx)

        cap_src = n_exp * (3 * seq * top_k // (2 * n_all))
        y_all = run_experts(n, loc, dst, rank_t, (u_half, u_x, u_c, u_d), exp_gate, exp_up, exp_down, cap_src, ctx)

        quarters = my_ep ^ jnp.arange(4, dtype=jnp.int32)
        after, f_norm = run_out(quarters, x2, ffn_gain, ctx, ctx_peer, w_o, (w_q0, w_q2, w_q1, w_q3), y_all)
        f_far = run_ffn(1 - my_tp, half, f_norm, w_gate, w_up, w_down, after, n_out=2)
        f_got = []
        for c in range(2):
            f_got.append(over_tp(f_far[c]))

        got3, m_x = [], []
        tie = f_far[0]
        for p in range(2):
            m3, = run_combine(3, rows, pos, gates_all, y_all, tie, part=(p, 2))
            tie = m3
            got3.append(over_core(m3))
        for p in range(2):
            m1 = run_combine(1, rows, pos, gates_all, y_all, tie, init=got3[p], n_out=CHUNKS // 2, part=(p, 2))
            tie = m1[0]
            for k in range(CHUNKS // 2):
                m_x.append(over_x(m1[k]))

        m2, = run_combine(2, rows, pos, gates_all, y_all, tie)
        got2 = over_core(m2)

        s_own, = run_ffn(my_tp, half, f_norm, w_gate, w_up, w_down, m2, adds=((after, None),))
        own, peer = [], []
        tie = s_own
        for c in range(CHUNKS):
            tie, = run_combine(0, rows, pos, gates_all, y_all, tie, part=(c, CHUNKS),
                               adds=((s_own, c), (f_got[c], 0), (got2, c), (m_x[c], 0)))
            own.append(tie)
            peer.append(over_tp(tie))
        mine, other = my_tp * CHUNKS, (1 - my_tp) * CHUNKS
        dest = jnp.stack([mine + c for c in range(CHUNKS)] + [other + c for c in range(CHUNKS)]).astype(jnp.int32)
        out = run_place(dest[:-1], own + peer[:-1], seq)
        out = run_place(dest[-1:], peer[-1:], seq, out)
        return out.reshape(1, seq, d)

    return jax.shard_map(layer, mesh=mesh, in_specs=in_specs, out_specs=tok_spec, check_vma=False)
```
